32 devices in a mesh: expert: 4 (over x, core), shard: 8 (over z, y).
Axes of the slice: x: 2, y: 2, z: 4, core: 2. Of those that a mesh axis runs over, the one named last changes fastest.
Arguments:
- hidden_in: float32 [8192, 1024], P(('expert', 'shard')), may hold values from -6 to 6
- cotangent: float32 [8192, 1024], P(('expert', 'shard')), may hold values from -6 to 6
- doc_lengths: int32 [4, 4], replicated, may hold values from 1 to 1280, 2048 in all within a row
- routes: int32 [2, 8192, 8], P(None, ('expert', 'shard')), may hold values from 0 to 15, all different within a row; in each aligned block of 256 rows (0 to 255, 256 to 511, ..., all dimensions but the last counted through in order) at most 160 rows name the same one
- gains: float32 [2, 2, 1024], P(None, None, 'shard'), may hold values from 0.5 to 1.5
- gains_first: float32 [2, 2, 1024], P(None, None, 'shard'), may hold values from -149.34096 to 149.34096
- gains_second: float32 [2, 2, 1024], P(None, None, 'shard'), may hold values from 5406.72 to 21299.2
- w_qkv: float32 [2, 1024, 2048], P(None, 'shard'), may hold values from -0.1875 to 0.1875
- w_qkv_first: float32 [2, 1024, 2048], P(None, 'shard'), may hold values from -90.96222 to 90.96222
- w_qkv_second: float32 [2, 1024, 2048], P(None, 'shard'), may hold values from 1945.6 to 7782.4
- w_out: float32 [2, 1024, 1024], P(None, 'shard'), may hold values from -1.5 to 1.5
- w_out_first: float32 [2, 1024, 1024], P(None, 'shard'), may hold values from -9.96 to 9.96
- w_out_second: float32 [2, 1024, 1024], P(None, 'shard'), may hold values from 24 to 96
- router: float32 [2, 1024, 16], P(None, 'shard'), may hold values from -0.1875 to 0.1875
- router_first: float32 [2, 1024, 16], P(None, 'shard'), may hold values from -192 to 192
- router_second: float32 [2, 1024, 16], P(None, 'shard'), may hold values from 9216 to 36864
- w_in: float32 [2, 16, 1024, 1024], P(None, 'expert', 'shard'), may hold values from -0.1875 to 0.1875
- w_in_first: float32 [2, 16, 1024, 1024], P(None, 'expert', 'shard'), may hold values from -12.48 to 12.48
- w_in_second: float32 [2, 16, 1024, 1024], P(None, 'expert', 'shard'), may hold values from 35.84 to 143.36
- w_down: float32 [2, 16, 512, 1024], P(None, 'expert', 'shard'), may hold values from -0.75 to 0.75
- w_down_first: float32 [2, 16, 512, 1024], P(None, 'expert', 'shard'), may hold values from -3.36 to 3.36
- w_down_second: float32 [2, 16, 512, 1024], P(None, 'expert', 'shard'), may hold values from 2.56 to 10.24
Outputs:
- hidden_out: float32 [8192, 1024], P(('expert', 'shard'))
- input_grad: float32 [8192, 1024], P(('expert', 'shard'))
- gains_grad: float32 [2, 2, 1024], P(None, None, 'shard')
- gains_first_new: float32 [2, 2, 1024], P(None, None, 'shard')
- gains_second_new: float32 [2, 2, 1024], P(None, None, 'shard')
- gains_step: float32 [2, 2, 1024], P(None, None, 'shard')
- w_qkv_grad: float32 [2, 1024, 2048], P(None, 'shard')
- w_qkv_first_new: float32 [2, 1024, 2048], P(None, 'shard')
- w_qkv_second_new: float32 [2, 1024, 2048], P(None, 'shard')
- w_qkv_step: float32 [2, 1024, 2048], P(None, 'shard')
- w_out_grad: float32 [2, 1024, 1024], P(None, 'shard')
- w_out_first_new: float32 [2, 1024, 1024], P(None, 'shard')
- w_out_second_new: float32 [2, 1024, 1024], P(None, 'shard')
- w_out_step: float32 [2, 1024, 1024], P(None, 'shard')
- router_grad: float32 [2, 1024, 16], P(None, 'shard')
- router_first_new: float32 [2, 1024, 16], P(None, 'shard')
- router_second_new: float32 [2, 1024, 16], P(None, 'shard')
- router_step: float32 [2, 1024, 16], P(None, 'shard')
- w_in_grad: float32 [2, 16, 1024, 1024], P(None, 'expert', 'shard')
- w_in_first_new: float32 [2, 16, 1024, 1024], P(None, 'expert', 'shard')
- w_in_second_new: float32 [2, 16, 1024, 1024], P(None, 'expert', 'shard')
- w_in_step: float32 [2, 16, 1024, 1024], P(None, 'expert', 'shard')
- w_down_grad: float32 [2, 16, 512, 1024], P(None, 'expert', 'shard')
- w_down_first_new: float32 [2, 16, 512, 1024], P(None, 'expert', 'shard')
- w_down_second_new: float32 [2, 16, 512, 1024], P(None, 'expert', 'shard')
- w_down_step: float32 [2, 16, 512, 1024], P(None, 'expert', 'shard')
The draws below stay inside these ranges and needn't reach their ends.
Inputs may be any that keep to these rules, and one draw needn't show every extreme that they name: `routes`: each row names 8 different experts; within the 256 tokens of one device, in each layer, no expert is named by more than 160 rows, a bound that some block reaches. `doc_lengths`: each row sums to 2048; its longest document has exactly 1280 tokens.
All inputs are finite; a program needn't handle non-finite values.
Results may differ from the reference program's by a relative error of at most 0.03.
Values may be sent and summed in bfloat16 or wider, within the bound.
A program may use at most 384 MiB of HBM per device.

```python
import math
import jax
import jax.numpy as jnp
import numpy as np
from jax import lax

D = 1024
HEADS = 16
KV_HEADS = 8
HEAD = 64
FFE = 512
TOP = 8
LAYERS = 2
WINDOW = 1024
DOCS = 4
TOK_DEV = 256
EXPERTS = 16
SEQ = 2048
DOC_MOST = 1280
TOKENS = 8192
NSEQ = 4
CAP = 160


def level_of(own_key, shape, cuts, low, largest):
    def one(axis_at, shards_of):
        heights = jax.random.uniform(jax.random.fold_in(jax.random.fold_in(own_key, 6), axis_at), (shards_of,), jnp.float32, low / len(cuts), largest / len(cuts))
        return jnp.repeat(jnp.exp(heights), shape[axis_at] // shards_of).reshape((-1,) + (1,) * (len(shape) - axis_at - 1))

    level = one(*cuts[0])
    for cut in cuts[1:]:
        level = level * one(*cut)
    return level


def profile(amount, total, bound, skew):
    weights = [(1 << 20) // math.isqrt(standing ** skew) + 1 for standing in range(2, amount + 1)]
    spare, counts = total - bound - (amount - 1), [1] * (amount - 1)
    while spare > 0:
        free = [i for i in range(amount - 1) if counts[i] < bound]
        whole, budget = sum([weights[i] for i in free]), spare
        for i in free:
            extra = min(bound - counts[i], max(1, budget * weights[i] // whole), spare)
            counts[i] = counts[i] + extra
            spare = spare - extra
    return np.array([bound] + counts)


def uneven_parts(rng, count, total, limit, slope):
    if count == 2:
        one = jax.random.randint(rng, (), max(1, total - limit), min(limit, total - 1) + 1)
        return jnp.stack([one, total - one])
    sizes = jnp.asarray(profile(count, total, limit, slope), jnp.int32)
    twos = (count - 1) // 2
    source_of, taker = sizes[1:1 + 2 * twos:2], sizes[2:2 + 2 * twos:2]
    slack = jnp.minimum(source_of - 1, limit - taker)
    passed = jax.random.randint(jax.random.fold_in(rng, 1), (twos,), 0, 1 << 20) % (slack + 1)
    sizes = sizes.at[1:1 + 2 * twos:2].set(source_of - passed).at[2:2 + 2 * twos:2].set(taker + passed)
    return sizes[jax.random.permutation(jax.random.fold_in(rng, 2), count)]


def shared_out(stream_key, own, number, rows, amount, top, reach, lean):
    ranking = jax.random.permutation(stream_key, amount)
    crowded, common = portions_of(amount, rows * top, reach, lean, True), portions_of(amount, rows * top, reach, lean, False)
    places = jnp.arange(amount)

    def named(tallies, turn):
        used = int((tallies > 0).sum())
        fixed = max(1, used // 4)
        shifted = fixed + (places - fixed + turn * (used - fixed)) % max(1, amount - fixed)
        return jnp.zeros((amount,), jnp.int32).at[ranking[jnp.where(places < fixed, places, shifted)]].set(jnp.asarray(tallies, jnp.int32))

    tallies = jnp.where(number % 4 == 0, named(crowded, number // 4), named(common, number - number // 4 - 1))
    mixed = jax.random.permutation(jax.random.fold_in(own, 3), amount)
    giver, receiver = mixed[0:amount // 2 * 2:2], mixed[1:amount // 2 * 2:2]
    slack = jnp.minimum(tallies[giver] - 1, reach - tallies[receiver]) // 2
    slack = jnp.where((giver == ranking[0]) | (receiver == ranking[0]) | (tallies[receiver] == 0), 0, jnp.maximum(slack, 0))
    shifted = jax.random.randint(jax.random.fold_in(own, 4), (amount // 2,), 0, 1 << 20) % (slack + 1)
    tallies = tallies.at[giver].add(-shifted).at[receiver].add(shifted)
    labels = jnp.searchsorted(jnp.cumsum(tallies), jnp.arange(rows * top), side="right").astype(jnp.int32)
    listing = labels.reshape(top, rows).T
    listing = listing[jax.random.permutation(jax.random.fold_in(own, 1), rows)]
    turn = jax.random.randint(jax.random.fold_in(own, 2), (rows, 1), 0, top)
    return jnp.take_along_axis(listing, (jnp.arange(top)[None, :] + turn) % top, axis=1)


def portions_of(amount, total, limit, lean, full):
    loads = [(1 << 20) // math.isqrt(rank ** lean) + 1 for rank in range(1, amount + 1)]
    largest = limit if full else min(limit, max(-(-total // amount), total * loads[0] // sum(loads)))
    least = 1 if total - largest >= amount - 1 else 0
    holding, surplus = [largest] + [least] * (amount - 1), total - largest - least * (amount - 1)
    while surplus > 0:
        movable = [i for i in range(1, amount) if holding[i] < largest] or [i for i in range(1, amount) if holding[i] < limit]
        mass, budget = sum([loads[i] for i in movable]), surplus
        for i in movable:
            extra = min(limit - holding[i], max(1, budget * loads[i] // mass), surplus)
            holding[i] = holding[i] + extra
            surplus = surplus - extra
    return np.array(holding)


def bell_draw(own_key, shape, deviation, bound, pieces=(), kind=jnp.bfloat16):
    array = jax.random.normal(own_key, shape, jnp.float32) * deviation
    if len(pieces) > 0:
        array = level_of(own_key, shape, pieces, -0.22, 0.18) * array
    return jnp.clip(array, min=-bound, max=bound).astype(kind)


def setup_inputs(seed: int = 0) -> dict:
    key_list = jax.random.split(jax.random.key(seed), 23)
    hidden_in = bell_draw(key_list[0], (TOKENS, D), 1.0, 6.0, ((0, 32),), jnp.float32)
    cotangent = bell_draw(key_list[1], (TOKENS, D), 1.0, 6.0, ((0, 32),), jnp.float32)
    doc_lengths = jax.vmap(lambda own: uneven_parts(own, DOCS, SEQ, DOC_MOST, 1))(jax.random.split(key_list[2], NSEQ)).reshape((NSEQ, DOCS)).astype(jnp.int32)
    routes_keys = jax.random.split(jax.random.fold_in(key_list[3], 1), LAYERS * TOKENS // TOK_DEV)
    routes_turns = jax.random.permutation(jax.random.fold_in(key_list[3], 3), LAYERS * TOKENS // TOK_DEV)
    routes = jax.vmap(lambda own, number: shared_out(jax.random.fold_in(key_list[3], 2), own, number, TOK_DEV, EXPERTS, TOP, CAP, 1))(routes_keys, routes_turns).reshape((LAYERS, TOKENS, TOP))
    gains = jnp.clip(1.0 + 0.1 * jax.random.normal(key_list[4], (LAYERS, 2, D), jnp.float32), 0.5, 1.5)
    gains_first = bell_draw(key_list[5], (LAYERS, 2, D), (0.55 * TOKENS ** 0.5), 149.34096, ((2, 8),), jnp.float32)
    gains_second = jnp.clip(jnp.exp(math.log(21299.2) - 1.3710268 * jax.random.uniform(key_list[6], (LAYERS, 2, D), jnp.float32) ** level_of(key_list[6], (LAYERS, 2, D), ((2, 8),), -0.2, 0.2)), 5406.72, 21299.2)
    w_qkv = bell_draw(key_list[7], (LAYERS, D, (HEADS + 2 * KV_HEADS) * HEAD), D ** -0.5, 0.1875, ((1, 8),), jnp.float32)
    w_qkv_first = bell_draw(key_list[8], (LAYERS, D, (HEADS + 2 * KV_HEADS) * HEAD), (0.67 * (2 * D * TOKENS // (KV_HEADS * WINDOW)) ** 0.5), 90.96222, ((1, 8),), jnp.float32)
    w_qkv_second = jnp.clip(jnp.exp(math.log(7782.4) - 1.3862944 * jax.random.uniform(key_list[9], (LAYERS, D, (HEADS + 2 * KV_HEADS) * HEAD), jnp.float32) ** level_of(key_list[9], (LAYERS, D, (HEADS + 2 * KV_HEADS) * HEAD), ((1, 8),), -0.2, 0.2)), 1945.6, 7782.4)
    w_out = bell_draw(key_list[10], (LAYERS, HEADS * HEAD, D), HEADS ** -0.5, 1.5, ((1, 8),), jnp.float32)
    w_out_first = bell_draw(key_list[11], (LAYERS, HEADS * HEAD, D), (0.83 * (2 * TOKENS // WINDOW) ** 0.5), 9.96, ((1, 8),), jnp.float32)
    w_out_second = jnp.clip(jnp.exp(math.log(96.0) - 1.3862944 * jax.random.uniform(key_list[12], (LAYERS, HEADS * HEAD, D), jnp.float32) ** level_of(key_list[12], (LAYERS, HEADS * HEAD, D), ((1, 8),), -0.2, 0.2)), 24.0, 96.0)
    router = bell_draw(key_list[13], (LAYERS, D, EXPERTS), D ** -0.5, 0.1875, ((1, 8),), jnp.float32)
    router_first = bell_draw(key_list[14], (LAYERS, D, EXPERTS), (0.2 * (25 * TOKENS * TOP // EXPERTS) ** 0.5), 192.0, ((1, 8),), jnp.float32)
    router_second = jnp.clip(jnp.exp(math.log(36864.0) - 1.3862944 * jax.random.uniform(key_list[15], (LAYERS, D, EXPERTS), jnp.float32) ** level_of(key_list[15], (LAYERS, D, EXPERTS), ((1, 8),), -0.2, 0.2)), 9216.0, 36864.0)
    w_in = bell_draw(key_list[16], (LAYERS, EXPERTS, D, 2 * FFE), D ** -0.5, 0.1875, ((1, 4), (2, 8)), jnp.float32)
    w_in_first = bell_draw(key_list[17], (LAYERS, EXPERTS, D, 2 * FFE), (0.26 * (TOKENS * TOP // (16 * EXPERTS)) ** 0.5), 12.48, ((1, 4), (2, 8)), jnp.float32)
    w_in_second = jnp.clip(jnp.exp(math.log(143.36) - 1.3862944 * jax.random.uniform(key_list[18], (LAYERS, EXPERTS, D, 2 * FFE), jnp.float32) ** level_of(key_list[18], (LAYERS, EXPERTS, D, 2 * FFE), ((1, 4), (2, 8)), -0.2, 0.2)), 35.84, 143.36)
    w_down = bell_draw(key_list[19], (LAYERS, EXPERTS, FFE, D), (FFE // 8) ** -0.5, 0.75, ((1, 4), (2, 8)), jnp.float32)
    w_down_first = bell_draw(key_list[20], (LAYERS, EXPERTS, FFE, D), (0.28 * (TOKENS // (4 * TOP * EXPERTS)) ** 0.5), 3.36, ((1, 4), (2, 8)), jnp.float32)
    w_down_second = jnp.clip(jnp.exp(math.log(10.24) - 1.3862944 * jax.random.uniform(key_list[21], (LAYERS, EXPERTS, FFE, D), jnp.float32) ** level_of(key_list[21], (LAYERS, EXPERTS, FFE, D), ((1, 4), (2, 8)), -0.2, 0.2)), 2.56, 10.24)
    return dict(hidden_in=hidden_in, cotangent=cotangent, doc_lengths=doc_lengths, routes=routes, gains=gains, gains_first=gains_first, gains_second=gains_second, w_qkv=w_qkv, w_qkv_first=w_qkv_first, w_qkv_second=w_qkv_second, w_out=w_out, w_out_first=w_out_first, w_out_second=w_out_second, router=router, router_first=router_first, router_second=router_second, w_in=w_in, w_in_first=w_in_first, w_in_second=w_in_second, w_down=w_down, w_down_first=w_down_first, w_down_second=w_down_second)


@jax.custom_vjp
def low(v):
    return lax.optimization_barrier(v.astype(jnp.bfloat16)).astype(jnp.float32)

@jax.custom_vjp
def low_back(v):
    return v

def low_keep(v):
    return (low(v), None)

def low_pass(kept, grad):
    return (grad,)

def back_keep(v):
    return (v, None)

def back_low(kept, grad):
    return (low(grad),)
low.defvjp(low_keep, low_pass)
low_back.defvjp(back_keep, back_low)
norm_eps = 1e-05
masked_score = -1e+30
beta_one = 0.9
beta_two = 0.95
adam_eps = 1e-08
learn_rate = 0.05
decay_rate = 0.1
adam_step = 10.0
highest = lax.Precision.HIGHEST

def matmul(left_side, right_side):
    return jnp.dot(left_side, right_side, precision=highest, preferred_element_type=jnp.float32)

def rms_scale(values, gain_row):
    return values * lax.rsqrt(lax.optimization_barrier(jnp.mean(values * values, axis=-1, keepdims=True)) + norm_eps) * gain_row

def attend_sequence(seq_pair):
    qkv_seq, lengths_row = seq_pair
    seq_len = qkv_seq.shape[0]
    q_width = HEADS * HEAD
    kv_width = KV_HEADS * HEAD
    queries = qkv_seq[:, :q_width].reshape(seq_len, KV_HEADS, HEADS // KV_HEADS, HEAD)
    keys_all = qkv_seq[:, q_width:q_width + kv_width].reshape(seq_len, KV_HEADS, HEAD)
    values_all = qkv_seq[:, q_width + kv_width:].reshape(seq_len, KV_HEADS, HEAD)
    places = jnp.arange(seq_len, dtype=jnp.int32)
    doc_ends = jnp.cumsum(lengths_row)
    doc_ids = lax.optimization_barrier(jnp.sum((places[:, None] >= doc_ends[None, :]).astype(jnp.int32), axis=1))
    distance = places[:, None] - places[None, :]
    allowed = (doc_ids[:, None] == doc_ids[None, :]) & (distance >= 0) & (distance < WINDOW)
    scores = low_back(jnp.einsum('tngd,snd->ngts', queries, keys_all, precision=highest) * HEAD ** (-0.5))
    scores = jnp.where(allowed, scores, masked_score)
    probs = jax.nn.softmax(scores, axis=-1)
    attended = jnp.einsum('ngts,snd->tngd', low(probs), values_all, precision=highest)
    return attended.reshape(seq_len, q_width)

def slot_tables(layer_routes):
    blocks = TOKENS // TOK_DEV
    flat_routes = layer_routes.reshape(blocks, TOK_DEV * TOP)
    route_hits = (flat_routes[:, :, None] == jnp.arange(EXPERTS, dtype=jnp.int32)[None, None, :]).astype(jnp.int32)
    slot_index = lax.optimization_barrier(jnp.sum((jnp.cumsum(route_hits, axis=1) - 1) * route_hits, axis=2))
    assigns = jnp.arange(TOKENS * TOP, dtype=jnp.int32).reshape(blocks, TOK_DEV * TOP)
    block_ids = jnp.broadcast_to(jnp.arange(blocks, dtype=jnp.int32)[:, None], flat_routes.shape)
    token_table = jnp.full((blocks, EXPERTS, CAP), TOKENS, jnp.int32).at[block_ids, flat_routes, slot_index].set(assigns // TOP)
    assign_table = jnp.full((blocks, EXPERTS, CAP), TOKENS * TOP, jnp.int32).at[block_ids, flat_routes, slot_index].set(assigns)
    return (token_table, assign_table)

def expert_mix(normed_two, weights, token_table, assign_table, w_in_low, w_down_low):
    padded = jnp.concatenate([normed_two, jnp.zeros((1, D), jnp.float32)], 0)
    weight_pad = jnp.concatenate([weights.reshape(-1), jnp.zeros((1,), jnp.float32)], 0)
    token_lists = jnp.transpose(token_table, (1, 0, 2)).reshape(EXPERTS, -1)
    assign_lists = jnp.transpose(assign_table, (1, 0, 2)).reshape(EXPERTS, -1)

    def one_expert(summed, inputs):
        token_ids, assign_ids, w_in_one, w_down_one = inputs
        slot_rows = low_back(padded[token_ids])
        gate_up = low_back(matmul(slot_rows, w_in_one))
        hidden = low(jax.nn.silu(gate_up[:, :FFE]) * gate_up[:, FFE:])
        result = low_back(low(matmul(hidden, w_down_one)))
        return (summed.at[token_ids].add(result * weight_pad[assign_ids][:, None]), None)
    summed, unused = lax.scan(jax.checkpoint(one_expert), jnp.zeros((TOKENS + 1, D), jnp.float32), (token_lists, assign_lists, w_in_low, w_down_low))
    return summed[:TOKENS]

def adam_update(weight, gradient, first_moment, second_moment):
    new_first = beta_one * first_moment + (1.0 - beta_one) * gradient
    new_second = beta_two * second_moment + (1.0 - beta_two) * gradient * gradient
    corr_first = new_first / (1.0 - beta_one ** adam_step)
    corr_second = new_second / (1.0 - beta_two ** adam_step)
    weight_step = -learn_rate * (corr_first / (jnp.sqrt(corr_second) + adam_eps) + decay_rate * weight)
    return (new_first, new_second, weight_step)

def reference(hidden_in, cotangent, doc_lengths, routes, gains, gains_first, gains_second, w_qkv, w_qkv_first, w_qkv_second, w_out, w_out_first, w_out_second, router, router_first, router_second, w_in, w_in_first, w_in_second, w_down, w_down_first, w_down_second):
    tables = [slot_tables(routes[layer_no]) for layer_no in range(LAYERS)]

    def forward(stream, gain_all, qkv_all, out_all, router_all, w_in_all, w_down_all):
        for layer_no in range(LAYERS):
            gain_low = low(gain_all[layer_no])
            normed_one = low(rms_scale(stream, gain_low[0]))
            qkv_rows = low_back(low(matmul(normed_one, low(qkv_all[layer_no]))))
            attended = lax.map(jax.checkpoint(attend_sequence), (qkv_rows.reshape(TOKENS // SEQ, SEQ, -1), doc_lengths))
            attended = low_back(low(attended.reshape(TOKENS, HEADS * HEAD)))
            mixed = stream + low_back(matmul(attended, low(out_all[layer_no])))
            normed_two = low(rms_scale(mixed, gain_low[1]))
            logits = low_back(matmul(normed_two, low(router_all[layer_no])))
            weights = jax.nn.softmax(jnp.take_along_axis(logits, routes[layer_no], axis=1), axis=-1)
            stream = mixed + expert_mix(normed_two, weights, tables[layer_no][0], tables[layer_no][1], low(w_in_all[layer_no]), low(w_down_all[layer_no]))
        return stream
    hidden_out, pullback = jax.vjp(forward, hidden_in, gains, w_qkv, w_out, router, w_in, w_down)
    input_grad, gains_grad, w_qkv_grad, w_out_grad, router_grad, w_in_grad, w_down_grad = pullback(cotangent)
    gains_first_new, gains_second_new, gains_step = adam_update(gains, gains_grad, gains_first, gains_second)
    w_qkv_first_new, w_qkv_second_new, w_qkv_step = adam_update(w_qkv, w_qkv_grad, w_qkv_first, w_qkv_second)
    w_out_first_new, w_out_second_new, w_out_step = adam_update(w_out, w_out_grad, w_out_first, w_out_second)
    router_first_new, router_second_new, router_step = adam_update(router, router_grad, router_first, router_second)
    w_in_first_new, w_in_second_new, w_in_step = adam_update(w_in, w_in_grad, w_in_first, w_in_second)
    w_down_first_new, w_down_second_new, w_down_step = adam_update(w_down, w_down_grad, w_down_first, w_down_second)
    return (hidden_out, input_grad, gains_grad, gains_first_new, gains_second_new, gains_step, w_qkv_grad, w_qkv_first_new, w_qkv_second_new, w_qkv_step, w_out_grad, w_out_first_new, w_out_second_new, w_out_step, router_grad, router_first_new, router_second_new, router_step, w_in_grad, w_in_first_new, w_in_second_new, w_in_step, w_down_grad, w_down_first_new, w_down_second_new, w_down_step)
```

```python
import functools

import jax
import jax.numpy as jnp
from jax import lax
from jax.experimental import pallas as pl
from jax.experimental.pallas import tpu as pltpu
from jax.sharding import PartitionSpec as P

HEADS = 16
KV_HEADS = 8
HEAD = 64
TOP = 8
LAYERS = 2
WINDOW = 1024
SPAN = 8

norm_eps = 1e-05
masked_score = -1e30
beta_one = 0.9
beta_two = 0.95
adam_eps = 1e-08
learn_rate = 0.05
decay_rate = 0.1
adam_step = 10.0

F32 = jnp.float32
BF16 = jnp.bfloat16
MESH = pl.DeviceIdType.MESH
VMEM_LIMIT = 60 * 1024 * 1024


def rms_scale(values, gain_row):
    return (
        values * lax.rsqrt(jnp.mean(values * values, axis=-1, keepdims=True) + norm_eps) * gain_row
    )


def inner_rows(left_side, right_side):
    return lax.dot_general(
        left_side, right_side, (((0,), (0,)), ((), ())), preferred_element_type=F32
    )


def outer_cols(left_side, right_side):
    return lax.dot_general(
        left_side, right_side, (((1,), (1,)), ((), ())), preferred_element_type=F32
    )


def adam_update(weight, gradient, first_moment, second_moment):
    new_first = beta_one * first_moment + (1.0 - beta_one) * gradient
    new_second = beta_two * second_moment + (1.0 - beta_two) * gradient * gradient
    corr_first = new_first / (1.0 - beta_one**adam_step)
    corr_second = new_second / (1.0 - beta_two**adam_step)
    weight_step = -learn_rate * (
        corr_first / (jnp.sqrt(corr_second) + adam_eps) + decay_rate * weight
    )
    return [gradient, new_first, new_second, weight_step]


def greet(axis, count):
    me = lax.axis_index(axis)
    barrier = pltpu.get_barrier_semaphore()
    for d in range(1, count):
        pl.semaphore_signal(
            barrier, inc=1, device_id={axis: lax.rem(me + d, count)}, device_id_type=MESH
        )
    pl.semaphore_wait(barrier, count - 1)
    return me


def spread_kernel(count, x_ref, o_ref, send_sem, recv_sem):
    me = greet("expert", count)
    copies = []
    for d in range(1, count):
        copy = pltpu.make_async_remote_copy(
            src_ref=x_ref,
            dst_ref=o_ref.at[me],
            send_sem=send_sem.at[d - 1],
            recv_sem=recv_sem.at[d - 1],
            device_id={"expert": lax.rem(me + d, count)},
            device_id_type=MESH,
        )
        copy.start()
        copies.append(copy)
    o_ref[me] = x_ref[...]
    for copy in copies:
        copy.wait()


def spread(rows, count):
    return pl.pallas_call(
        functools.partial(spread_kernel, count),
        out_shape=jax.ShapeDtypeStruct((count,) + rows.shape, rows.dtype),
        in_specs=[pl.BlockSpec(memory_space=pltpu.VMEM)],
        out_specs=pl.BlockSpec(memory_space=pltpu.VMEM),
        scratch_shapes=[
            pltpu.SemaphoreType.DMA((count - 1,)),
            pltpu.SemaphoreType.DMA((count - 1,)),
        ],
        compiler_params=pltpu.CompilerParams(
            collective_id=1, has_side_effects=True, vmem_limit_bytes=VMEM_LIMIT
        ),
        name="spread",
    )(rows)


def collect_kernel(count, p_ref, o_ref, held, send_sem, recv_sem):
    me = greet("expert", count)
    copies = []
    for d in range(1, count):
        peer = lax.rem(me + d, count)
        copy = pltpu.make_async_remote_copy(
            src_ref=p_ref.at[peer],
            dst_ref=held.at[d - 1],
            send_sem=send_sem.at[d - 1],
            recv_sem=recv_sem.at[d - 1],
            device_id={"expert": peer},
            device_id_type=MESH,
        )
        copy.start()
        copies.append(copy)
    total = p_ref[me].astype(F32)
    for d, copy in enumerate(copies):
        copy.wait()
        total = total + held[d].astype(F32)
    o_ref[...] = total


def collect(parts):
    count, rows, width = parts.shape
    return pl.pallas_call(
        functools.partial(collect_kernel, count),
        out_shape=jax.ShapeDtypeStruct((rows, width), F32),
        in_specs=[pl.BlockSpec(memory_space=pltpu.VMEM)],
        out_specs=pl.BlockSpec(memory_space=pltpu.VMEM),
        scratch_shapes=[
            pltpu.VMEM((count - 1, rows, width), parts.dtype),
            pltpu.SemaphoreType.DMA((count - 1,)),
            pltpu.SemaphoreType.DMA((count - 1,)),
        ],
        compiler_params=pltpu.CompilerParams(
            collective_id=2, has_side_effects=True, vmem_limit_bytes=VMEM_LIMIT
        ),
        name="collect",
    )(parts)


def ring_shard(place, count):
    back = lax.div(place, count // 2)
    return (1 - back) * 2 * place + back * (2 * (count - 1 - place) + 1)


def ring_place(shard, count):
    odd, pair = lax.rem(shard, 2), lax.div(shard, 2)
    return (1 - odd) * pair + odd * (count - 1 - pair)


def signal(barrier, where):
    pl.semaphore_signal(barrier, inc=1, device_id=where, device_id_type=MESH)


def gather_dense_kernel(
    n, rows, x_ref, o_ref, ring_send, ring_recv, pair_send, pair_recv, own_sem
):
    e, s = lax.axis_index("expert"), lax.axis_index("shard")
    core = lax.rem(e, 2)
    partner = e + 1 - 2 * core
    p = ring_place(s, n)
    ways = (ring_shard(lax.rem(p + 1, n), n), ring_shard(lax.rem(p + n - 1, n), n))
    barrier = pltpu.get_barrier_semaphore()
    signal(barrier, {"expert": partner})
    signal(barrier, {"shard": ways[0]})
    signal(barrier, {"shard": ways[1]})
    pl.semaphore_wait(barrier, 3)
    quarter = rows // 4

    def part(side, way):
        return pl.ds(pl.multiple_of(side * 2 * quarter + way * quarter, quarter), quarter)

    def block(way, k):
        return ring_shard(lax.rem(p + (n - k if way == 0 else k), n), n)

    def ring_copy(way, k, src):
        return pltpu.make_async_remote_copy(
            src_ref=src,
            dst_ref=o_ref.at[block(way, k), part(core, way)],
            send_sem=ring_send.at[way, k],
            recv_sem=ring_recv.at[way, k],
            device_id={"shard": ways[way]},
            device_id_type=MESH,
        )

    def pair_copy(way, k, side):
        there = o_ref.at[block(way, k), part(side, way)]
        return pltpu.make_async_remote_copy(
            src_ref=there,
            dst_ref=there,
            send_sem=pair_send.at[way, k - 1],
            recv_sem=pair_recv.at[way, k - 1],
            device_id={"expert": partner},
            device_id_type=MESH,
        )

    for way in range(2):
        ring_copy(way, 0, x_ref.at[part(core, way)]).start()
    own = pltpu.make_async_copy(x_ref, o_ref.at[s], own_sem)
    own.start()

    def step(k, carry):
        for way in range(2):
            came = o_ref.at[block(way, k), part(core, way)]
            pltpu.make_async_remote_copy(
                src_ref=came,
                dst_ref=came,
                send_sem=ring_send.at[way, k - 1],
                recv_sem=ring_recv.at[way, k - 1],
                device_id={"shard": ways[way]},
                device_id_type=MESH,
            ).wait_recv()

            @pl.when(k < n - 1)
            def _():
                ring_copy(way, k, came).start()

            pair_copy(way, k, core).start()
        return carry

    lax.fori_loop(1, n, step, 0)

    def finish(k, carry):
        for way in range(2):
            ring_copy(way, k - 1, x_ref.at[part(core, way)]).wait_send()
            pair_copy(way, k, core).wait_send()
            pair_copy(way, k, 1 - core).wait_recv()
        return carry

    lax.fori_loop(1, n, finish, 0)
    own.wait()


def gather_dense(piece, n):
    rows, columns = piece.shape
    dma = pltpu.SemaphoreType.DMA
    return pl.pallas_call(
        functools.partial(gather_dense_kernel, n, rows),
        out_shape=jax.ShapeDtypeStruct((n, rows, columns), piece.dtype),
        in_specs=[pl.BlockSpec(memory_space=pltpu.VMEM)],
        out_specs=pl.BlockSpec(memory_space=pl.ANY),
        scratch_shapes=[
            dma((2, n - 1)), dma((2, n - 1)), dma((2, n - 1)), dma((2, n - 1)), dma,
        ],
        compiler_params=pltpu.CompilerParams(
            collective_id=3, has_side_effects=True, vmem_limit_bytes=VMEM_LIMIT
        ),
        name="gather_dense",
    )(piece)


def reduce_dense_kernel(
    n, owners, rows, g_ref, o_ref, paired, came, going, crossed, last_in,
    pair_send, pair_recv, ring_send, ring_recv, cross_send, cross_recv, last_send, last_recv,
):
    e, s = lax.axis_index("expert"), lax.axis_index("shard")
    core, x = lax.rem(e, 2), lax.div(e, 2)
    partner = e + 1 - 2 * core
    columns = owners // 2
    p = ring_place(s, n)
    ways = (ring_shard(lax.rem(p + 1, n), n), ring_shard(lax.rem(p + n - 1, n), n))
    barrier = pltpu.get_barrier_semaphore()
    signal(barrier, {"expert": partner})
    signal(barrier, {"shard": ways[0]})
    signal(barrier, {"shard": ways[1]})
    for d in range(1, columns):
        signal(barrier, {"expert": lax.rem(e + 2 * d, owners)})
    pl.semaphore_wait(barrier, 3 + columns - 1)
    half, quarter = rows // 2, rows // 4

    def mine(way):
        return pl.ds(pl.multiple_of(core * half + way * quarter, quarter), quarter)

    def block(way, k):
        return ring_shard(lax.rem(p + (2 * n - 1 - k if way == 0 else k + 1), n), n)

    def pair_copy(k):
        b = block(0, k)
        return pltpu.make_async_remote_copy(
            src_ref=g_ref.at[b, pl.ds(pl.multiple_of((1 - core) * half, half), half)],
            dst_ref=paired.at[b],
            send_sem=pair_send.at[b],
            recv_sem=pair_recv.at[b],
            device_id={"expert": partner},
            device_id_type=MESH,
        )

    def ring_copy(way, k):
        return pltpu.make_async_remote_copy(
            src_ref=going.at[way, k],
            dst_ref=came.at[way, k],
            send_sem=ring_send.at[way, k],
            recv_sem=ring_recv.at[way, k],
            device_id={"shard": ways[way]},
            device_id_type=MESH,
        )

    def own(way, b):
        return g_ref[b, mine(way), :].astype(F32) + paired[
            b, way * quarter : (way + 1) * quarter, :
        ].astype(F32)

    order = []
    for k in range(n):
        for place in (k, n - 2 - k):
            place = place % n
            if place not in order:
                order.append(place)
    for k in order:
        pair_copy(k).start()
    for k in order:
        pair_copy(k).wait_recv()
    for way in range(2):
        going[way, 0] = own(way, block(way, 0)).astype(BF16)
        ring_copy(way, 0).start()

    def step(k, carry):
        for way in range(2):
            ring_copy(way, k - 1).wait_recv()
            going[way, k] = (
                came[way, k - 1].astype(F32) + own(way, block(way, k))
            ).astype(BF16)
            ring_copy(way, k).start()
        return carry

    lax.fori_loop(1, n - 1, step, 0)
    for way in range(2):
        ring_copy(way, n - 2).wait_recv()
        crossed[x, way * quarter : (way + 1) * quarter, :] = (
            came[way, n - 2].astype(F32) + own(way, s)
        ).astype(BF16)

    def cross_copy(d):
        return pltpu.make_async_remote_copy(
            src_ref=crossed.at[x],
            dst_ref=crossed.at[x],
            send_sem=cross_send.at[d - 1],
            recv_sem=cross_recv.at[d - 1],
            device_id={"expert": lax.rem(e + 2 * d, owners)},
            device_id_type=MESH,
        )

    for d in range(1, columns):
        cross_copy(d).start()
    for d in range(1, columns):
        cross_copy(d).wait()
    total = crossed[0].astype(F32)
    for d in range(1, columns):
        total = total + crossed[d].astype(F32)
    here = pl.ds(pl.multiple_of(core * half, half), half)
    o_ref[here, :] = total.astype(BF16)
    last = pltpu.make_async_remote_copy(
        src_ref=o_ref.at[here],
        dst_ref=last_in,
        send_sem=last_send,
        recv_sem=last_recv,
        device_id={"expert": partner},
        device_id_type=MESH,
    )
    last.start()
    for k in order:
        pair_copy(k).wait_send()

    def finish(k, carry):
        for way in range(2):
            ring_copy(way, k).wait_send()
        return carry

    lax.fori_loop(0, n - 1, finish, 0)
    last.wait()
    o_ref[pl.ds(pl.multiple_of((1 - core) * half, half), half), :] = last_in[...]


def reduce_dense(grads, n, owners):
    rows, columns = grads.shape[1:]
    dma = pltpu.SemaphoreType.DMA
    across = owners // 2
    return pl.pallas_call(
        functools.partial(reduce_dense_kernel, n, owners, rows),
        out_shape=jax.ShapeDtypeStruct((rows, columns), BF16),
        in_specs=[pl.BlockSpec(memory_space=pltpu.VMEM)],
        out_specs=pl.BlockSpec(memory_space=pltpu.VMEM),
        scratch_shapes=[
            pltpu.VMEM((n, rows // 2, columns), BF16),
            pltpu.VMEM((2, n - 1, rows // 4, columns), BF16),
            pltpu.VMEM((2, n - 1, rows // 4, columns), BF16),
            pltpu.VMEM((across, rows // 2, columns), BF16),
            pltpu.VMEM((rows // 2, columns), BF16),
            dma((n,)), dma((n,)), dma((2, n - 1)), dma((2, n - 1)),
            dma((across - 1,)), dma((across - 1,)), dma, dma,
        ],
        compiler_params=pltpu.CompilerParams(
            collective_id=4, has_side_effects=True, vmem_limit_bytes=VMEM_LIMIT
        ),
        name="reduce_dense",
    )(grads)


def halo_links(n, s):
    odd = lax.rem(s, 2)
    return odd, s + 1 - 2 * odd, s + 2 < n, s >= 2


def halo_barrier(s, odd, mate, ahead, behind, sends_back):
    barrier = pltpu.get_barrier_semaphore()
    even = odd == 0
    to_ahead, to_behind = (ahead, behind) if not sends_back else (behind, ahead)
    step = -2 if not sends_back else 2
    mate_copies = (odd == 1) | behind if not sends_back else even | behind
    to_mate = even | behind if not sends_back else (odd == 1) | behind

    @pl.when(to_behind)
    def _():
        signal(barrier, {"shard": s + step})

    @pl.when(mate_copies)
    def _():
        signal(barrier, {"shard": mate})

    @pl.when(to_ahead & to_mate)
    def _():
        pl.semaphore_wait(barrier, 2)

    @pl.when(to_ahead != to_mate)
    def _():
        pl.semaphore_wait(barrier, 1)


def halo_kernel(n, rows, cuts, kv_ref, o_ref, sends, recvs, own_sem):
    s = lax.axis_index("shard")
    odd, mate, ahead, behind = halo_links(n, s)
    even = odd == 0
    size = rows // cuts

    def copy(kind, cut, src, slot, where):
        return pltpu.make_async_remote_copy(
            src_ref=src.at[pl.ds(cut * size, size)],
            dst_ref=o_ref.at[slot, pl.ds(cut * size, size)],
            send_sem=sends.at[kind, cut],
            recv_sem=recvs.at[kind, cut],
            device_id={"shard": where},
            device_id_type=MESH,
        )

    halo_barrier(s, odd, mate, ahead, behind, False)
    from_odd = (o_ref.at[2], o_ref.at[0])
    from_even = (kv_ref, o_ref.at[2])
    for cut in range(cuts):

        @pl.when(ahead)
        def _():
            copy(0, cut, kv_ref, 2, s + 2).start()

        @pl.when(even)
        def _():
            copy(2, cut, kv_ref, 3, mate).start()

    o_ref[4] = kv_ref[...]
    for slot in range(4):

        @pl.when(s < 4 - slot)
        def _():
            o_ref[slot] = jnp.zeros_like(o_ref[slot])

    for cut in range(cuts):

        @pl.when(behind)
        def _():
            copy(0, cut, kv_ref, 2, s).wait_recv()

        @pl.when(behind & ahead)
        def _():
            copy(1, cut, o_ref.at[2], 0, s + 2).start()

        @pl.when(behind & (odd == 1))
        def _():
            copy(2, cut, from_odd[0], 3, mate).start()

        @pl.when(behind & even)
        def _():
            copy(3, cut, from_even[1], 1, mate).start()

    for cut in range(cuts):

        @pl.when(s >= 4)
        def _():
            copy(1, cut, o_ref.at[2], 0, s).wait_recv()

        @pl.when((s >= 4) & (odd == 1))
        def _():
            copy(3, cut, from_odd[1], 1, mate).start()

    for cut in range(cuts):

        @pl.when(s >= 1)
        def _():
            copy(2, cut, kv_ref, 3, mate).wait_recv()

        @pl.when(s >= 3)
        def _():
            copy(3, cut, kv_ref, 1, mate).wait_recv()

        @pl.when(ahead)
        def _():
            copy(0, cut, kv_ref, 2, s).wait_send()

        @pl.when(behind & ahead)
        def _():
            copy(1, cut, kv_ref, 0, s).wait_send()

        @pl.when(even | behind)
        def _():
            copy(2, cut, kv_ref, 3, mate).wait_send()

        @pl.when((even & behind) | ((odd == 1) & (s >= 4)))
        def _():
            copy(3, cut, kv_ref, 1, mate).wait_send()


def halo(kv, n, slots):
    rows, columns = kv.shape
    dma = pltpu.SemaphoreType.DMA
    cuts = 2
    return pl.pallas_call(
        functools.partial(halo_kernel, n, rows, cuts),
        out_shape=jax.ShapeDtypeStruct((slots, rows, columns), kv.dtype),
        in_specs=[pl.BlockSpec(memory_space=pltpu.VMEM)],
        out_specs=pl.BlockSpec(memory_space=pltpu.VMEM),
        scratch_shapes=[dma((4, cuts)), dma((4, cuts)), dma],
        compiler_params=pltpu.CompilerParams(
            collective_id=5, has_side_effects=True, vmem_limit_bytes=VMEM_LIMIT
        ),
        name="halo",
    )(kv)


def halo_back_kernel(n, rows, cuts, g_ref, o_ref, own, came, sends, recvs):
    s = lax.axis_index("shard")
    odd, mate, ahead, behind = halo_links(n, s)
    even = odd == 0
    size = rows // cuts

    def copy(kind, cut, src, where):
        return pltpu.make_async_remote_copy(
            src_ref=src.at[pl.ds(cut * size, size)],
            dst_ref=came.at[kind, pl.ds(cut * size, size)],
            send_sem=sends.at[kind, cut],
            recv_sem=recvs.at[kind, cut],
            device_id={"shard": where},
            device_id_type=MESH,
        )

    def there(ref, cut, value=None):
        here = pl.ds(cut * size, size)
        return ref[here, :].astype(F32)

    halo_barrier(s, odd, mate, ahead, behind, True)
    for cut in range(cuts):

        @pl.when(s >= 3)
        def _():
            copy(3, cut, g_ref.at[1], mate).start()

        @pl.when(s >= 1)
        def _():
            copy(2, cut, g_ref.at[3], mate).start()

    for cut in range(cuts):
        here = pl.ds(cut * size, size)

        @pl.when((odd == 1) & (s >= 4))
        def _():
            copy(3, cut, g_ref.at[1], mate).wait_recv()
            own[0, here, :] = (there(g_ref.at[0], cut) + there(came.at[3], cut)).astype(BF16)

        @pl.when((odd == 1) & (s >= 4))
        def _():
            copy(1, cut, own.at[0], s - 2).start()

        @pl.when(even & (s >= 4))
        def _():
            copy(1, cut, g_ref.at[0], s - 2).start()

    for cut in range(cuts):
        here = pl.ds(cut * size, size)

        @pl.when((odd == 1) & behind)
        def _():
            copy(2, cut, g_ref.at[3], mate).wait_recv()
            own[1, here, :] = (there(g_ref.at[2], cut) + there(came.at[2], cut)).astype(BF16)

        @pl.when(even & behind)
        def _():
            copy(3, cut, g_ref.at[1], mate).wait_recv()
            own[1, here, :] = (there(g_ref.at[2], cut) + there(came.at[3], cut)).astype(BF16)

        @pl.when(behind & ahead)
        def _():
            copy(1, cut, g_ref.at[0], s).wait_recv()
            own[1, here, :] = (there(own.at[1], cut) + there(came.at[1], cut)).astype(BF16)

        @pl.when(behind)
        def _():
            copy(0, cut, own.at[1], s - 2).start()

    for cut in range(cuts):
        here = pl.ds(cut * size, size)
        o_ref[here, :] = there(g_ref.at[4], cut)

        @pl.when(even)
        def _():
            copy(2, cut, g_ref.at[3], mate).wait_recv()
            o_ref[here, :] += there(came.at[2], cut)

        @pl.when(ahead)
        def _():
            copy(0, cut, own.at[1], s).wait_recv()
            o_ref[here, :] += there(came.at[0], cut)

        @pl.when(s >= 3)
        def _():
            copy(3, cut, g_ref.at[1], mate).wait_send()

        @pl.when(s >= 1)
        def _():
            copy(2, cut, g_ref.at[3], mate).wait_send()

        @pl.when(s >= 4)
        def _():
            copy(1, cut, g_ref.at[0], mate).wait_send()

        @pl.when(behind)
        def _():
            copy(0, cut, own.at[1], mate).wait_send()


def halo_back(grads, n):
    slots, rows, columns = grads.shape
    dma = pltpu.SemaphoreType.DMA
    cuts = 2
    return pl.pallas_call(
        functools.partial(halo_back_kernel, n, rows, cuts),
        out_shape=jax.ShapeDtypeStruct((rows, columns), F32),
        in_specs=[pl.BlockSpec(memory_space=pltpu.VMEM)],
        out_specs=pl.BlockSpec(memory_space=pltpu.VMEM),
        scratch_shapes=[
            pltpu.VMEM((3, rows, columns), BF16),
            pltpu.VMEM((4, rows, columns), BF16),
            dma((4, cuts)),
            dma((4, cuts)),
        ],
        compiler_params=pltpu.CompilerParams(
            collective_id=6, has_side_effects=True, vmem_limit_bytes=VMEM_LIMIT
        ),
        name="halo_back",
    )(grads)


def column_of(extra, index, experts_total):
    lanes = lax.broadcasted_iota(jnp.int32, extra.shape, 1)
    hit = (lanes == index) | (lanes == index + experts_total)
    return jnp.sum(jnp.where(hit, extra.astype(F32), 0.0), axis=1, keepdims=True)


def ffn_forward_kernel(
    tile, width, in_rows, experts_total, first_ref, x_ref, w_ref, part_ref, gate_up_ref, acc
):
    e = pl.program_id(0)
    w_in = w_ref[:, 0, :in_rows, :].reshape(width, w_ref.shape[-1])
    w_down = w_ref[:, 0, in_rows:, :].reshape(-1, width)
    half = w_in.shape[1] // 2
    index = first_ref[0] + e
    count = x_ref.shape[0] // tile
    for t in range(count):
        rows = pl.ds(t * tile, tile)
        gate_up = jnp.dot(x_ref[rows, :width], w_in, preferred_element_type=F32)
        gate, up = gate_up[:, :half], gate_up[:, half:]
        gate_up_ref[0, rows, :] = gate_up.astype(BF16)
        weight = column_of(x_ref[rows, width:], index, experts_total)
        hidden = (gate * jax.nn.sigmoid(gate) * up * weight).astype(BF16)
        out = jnp.dot(hidden, w_down, preferred_element_type=F32)

        @pl.when(e == 0)
        def _():
            acc[rows, :] = out

        @pl.when(e > 0)
        def _():
            acc[rows, :] += out

        @pl.when(e == pl.num_programs(0) - 1)
        def _():
            part_ref[rows, :] = acc[rows, :].astype(BF16)


def ffn_forward(first, x_all, w_all, experts_total, in_rows):
    shards, local, piece, inner = w_all.shape
    tokens, wide = x_all.shape
    width = in_rows * shards
    return pl.pallas_call(
        functools.partial(ffn_forward_kernel, 256, width, in_rows, experts_total),
        grid_spec=pltpu.PrefetchScalarGridSpec(
            num_scalar_prefetch=1,
            grid=(local,),
            in_specs=[
                pl.BlockSpec((tokens, wide), lambda e, f: (0, 0)),
                pl.BlockSpec((shards, 1, piece, inner), lambda e, f: (0, e, 0, 0)),
            ],
            out_specs=[
                pl.BlockSpec((tokens, width), lambda e, f: (0, 0)),
                pl.BlockSpec((1, tokens, inner), lambda e, f: (e, 0, 0)),
            ],
            scratch_shapes=[pltpu.VMEM((tokens, width), F32)],
        ),
        out_shape=[
            jax.ShapeDtypeStruct((tokens, width), BF16),
            jax.ShapeDtypeStruct((local, tokens, inner), BF16),
        ],
        compiler_params=pltpu.CompilerParams(vmem_limit_bytes=VMEM_LIMIT),
        cost_estimate=pl.CostEstimate(
            flops=2 * local * tokens * width * (inner + inner // 2),
            bytes_accessed=2 * (w_all.size + local * tokens * inner + 2 * tokens * wide),
            transcendentals=0,
        ),
        name="ffn_forward",
    )(first, x_all, w_all)


def ffn_backward_kernel(
    tile,
    width,
    in_rows,
    experts_total,
    first_ref,
    x_ref,
    g_ref,
    gate_up_ref,
    w_ref,
    router_ref,
    part_ref,
    grad_ref,
    router_grad_ref,
    acc,
    d_gate_up,
    hidden_all,
    d_logits,
):
    e = pl.program_id(0)
    inner = w_ref.shape[-1]
    w_in = w_ref[:, 0, :in_rows, :].reshape(width, inner)
    w_down = w_ref[:, 0, in_rows:, :].reshape(-1, width)
    half = inner // 2
    index = first_ref[0] + e
    tokens = x_ref.shape[0]
    last = pl.num_programs(0) - 1
    for t in range(tokens // tile):
        rows = pl.ds(t * tile, tile)
        d_plain = outer_cols(g_ref[rows, :width], w_down)
        gate = gate_up_ref[0, rows, :half].astype(F32)
        up = gate_up_ref[0, rows, half:].astype(F32)
        weight = column_of(x_ref[rows, width:], index, experts_total)
        mean_d = column_of(g_ref[rows, width:], 0, 1)
        sig = jax.nn.sigmoid(gate)
        silu = gate * sig
        hidden = silu * up
        d_weight = jnp.sum(hidden * d_plain, axis=1, keepdims=True)
        d_hidden = d_plain * weight
        hidden_all[rows, :] = (hidden * weight).astype(BF16)
        d_gate_up[rows, :half] = (d_hidden * up * sig * (1.0 + gate * (1.0 - sig))).astype(BF16)
        d_gate_up[rows, half:] = (d_hidden * silu).astype(BF16)
        lanes = lax.broadcasted_iota(jnp.int32, (tile, d_logits.shape[1]), 1)
        d_logit = jnp.where(lanes == e, weight * (d_weight - mean_d), 0.0).astype(BF16)
        out = outer_cols(d_gate_up[rows, :], w_in)

        @pl.when(e == 0)
        def _():
            acc[rows, :] = out
            d_logits[rows, :] = d_logit

        @pl.when(e > 0)
        def _():
            acc[rows, :] += out
            d_logits[rows, :] += d_logit

    x = x_ref[:, :width]
    grad_ref[:, 0, :in_rows, :] = (
        inner_rows(x, d_gate_up[...]).astype(BF16).reshape(-1, in_rows, inner)
    )
    grad_ref[:, 0, in_rows:, :] = (
        inner_rows(hidden_all[...], g_ref[:, :width])
        .astype(BF16)
        .reshape(-1, w_ref.shape[2] - in_rows, width)
    )

    @pl.when(e == last)
    def _():
        for t in range(tokens // tile):
            rows = pl.ds(t * tile, tile)
            out = acc[rows, :] + jnp.dot(
                d_logits[rows, :], router_ref[...], preferred_element_type=F32
            )
            part_ref[rows, :] = out.astype(BF16)
        router_grad_ref[...] = inner_rows(x, d_logits[...])


def ffn_backward(first, x_all, g_all, gate_up, w_all, router_rows, experts_total, in_rows):
    shards, local, piece, inner = w_all.shape
    tokens, wide = x_all.shape
    width = in_rows * shards
    lanes = router_rows.shape[0]
    return pl.pallas_call(
        functools.partial(ffn_backward_kernel, 256, width, in_rows, experts_total),
        grid_spec=pltpu.PrefetchScalarGridSpec(
            num_scalar_prefetch=1,
            grid=(local,),
            in_specs=[
                pl.BlockSpec((tokens, wide), lambda e, f: (0, 0)),
                pl.BlockSpec((tokens, g_all.shape[1]), lambda e, f: (0, 0)),
                pl.BlockSpec((1, tokens, inner), lambda e, f: (e, 0, 0)),
                pl.BlockSpec((shards, 1, piece, inner), lambda e, f: (0, e, 0, 0)),
                pl.BlockSpec((lanes, width), lambda e, f: (0, 0)),
            ],
            out_specs=[
                pl.BlockSpec((tokens, width), lambda e, f: (0, 0)),
                pl.BlockSpec((shards, 1, piece, inner), lambda e, f: (0, e, 0, 0)),
                pl.BlockSpec((width, lanes), lambda e, f: (0, 0)),
            ],
            scratch_shapes=[
                pltpu.VMEM((tokens, width), F32),
                pltpu.VMEM((tokens, inner), BF16),
                pltpu.VMEM((tokens, inner // 2), BF16),
                pltpu.VMEM((tokens, lanes), BF16),
            ],
        ),
        out_shape=[
            jax.ShapeDtypeStruct((tokens, width), BF16),
            jax.ShapeDtypeStruct(w_all.shape, BF16),
            jax.ShapeDtypeStruct((width, lanes), F32),
        ],
        compiler_params=pltpu.CompilerParams(vmem_limit_bytes=VMEM_LIMIT),
        cost_estimate=pl.CostEstimate(
            flops=4 * local * tokens * width * (inner + inner // 2),
            bytes_accessed=2 * (2 * w_all.size + local * tokens * inner + 4 * tokens * wide),
            transcendentals=0,
        ),
        name="ffn_backward",
    )(first, x_all, g_all, gate_up, w_all, router_rows)


def on_device(
    hidden_in,
    cotangent,
    doc_lengths,
    routes,
    gains,
    gains_first,
    gains_second,
    w_qkv,
    w_qkv_first,
    w_qkv_second,
    w_out,
    w_out_first,
    w_out_second,
    router,
    router_first,
    router_second,
    w_in,
    w_in_first,
    w_in_second,
    w_down,
    w_down_first,
    w_down_second,
):
    tok_rows, width = hidden_in.shape
    owners = lax.axis_size("expert")
    shards = lax.axis_size("shard")
    local_experts = w_in.shape[1]
    in_rows = w_in.shape[2]
    experts_total = local_experts * owners
    seq_len = tok_rows * SPAN
    hop_count = min(-(-WINDOW // tok_rows), SPAN - 1)
    key_count = (hop_count + 1) * tok_rows
    q_width = HEADS * HEAD
    kv_width = KV_HEADS * HEAD
    qkv_width = q_width + 2 * kv_width
    groups = HEADS // KV_HEADS
    score_scale = HEAD ** (-0.5)
    extra = -(-2 * experts_total // 128) * 128
    my_owner = lax.axis_index("expert")
    first_expert = my_owner * local_experts
    first_array = first_expert.astype(jnp.int32).reshape(1)
    row_start = (my_owner * shards + lax.axis_index("shard")) * tok_rows
    my_seq = row_start // seq_len
    doc_ends = jnp.cumsum(lax.dynamic_slice_in_dim(doc_lengths, my_seq, 1, 0)[0])
    query_rows = row_start + jnp.arange(tok_rows, dtype=jnp.int32)
    key_rows = row_start - hop_count * tok_rows + jnp.arange(key_count, dtype=jnp.int32)
    query_docs = jnp.sum(
        (query_rows[:, None] % seq_len >= doc_ends[None, :]).astype(jnp.int32), axis=1
    )
    key_docs = jnp.sum((key_rows[:, None] % seq_len >= doc_ends[None, :]).astype(jnp.int32), axis=1)
    distance = query_rows[:, None] - key_rows[None, :]
    allowed = (
        (query_rows[:, None] // seq_len == key_rows[None, :] // seq_len)
        & (query_docs[:, None] == key_docs[None, :])
        & (distance >= 0)
        & (distance < WINDOW)
    )
    expert_ids = jnp.arange(experts_total, dtype=jnp.int32)
    side = 128

    def dense_piece():
        rows = w_qkv.shape[1]
        parts = []
        for layer_no in range(LAYERS):
            parts += [w_qkv[layer_no].astype(BF16), w_out[layer_no].astype(BF16)]
        for layer_no in range(LAYERS):
            parts += [router[layer_no].astype(BF16), gains[layer_no].T.astype(BF16)]
        parts.append(jnp.zeros((rows, side - LAYERS * (experts_total + 2)), BF16))
        return jnp.concatenate(parts, 1)

    def expert_piece(layer_no):
        return jnp.concatenate(
            [w_in[layer_no].astype(BF16), w_down[layer_no].astype(BF16)], 1
        )

    layer_columns = qkv_width + width
    dense = gather_dense(dense_piece(), shards).reshape(width, -1)
    expert_full = []
    for layer_no in range(LAYERS):
        expert_full.append(lax.all_gather(expert_piece(layer_no), "shard", axis=0, tiled=False))

    kept_layers = []
    stream = hidden_in
    for layer_no in range(LAYERS):
        at = layer_no * layer_columns
        w_qkv_full = dense[:, at : at + qkv_width]
        w_out_full = dense[:, at + qkv_width : at + layer_columns]
        at = LAYERS * layer_columns + layer_no * (experts_total + 2)
        small = dense[:, at : at + experts_total + 2]
        router_full = small[:, :experts_total]
        gain_pair = small[:, experts_total : experts_total + 2].astype(F32).T
        normed_one = rms_scale(stream, gain_pair[0]).astype(BF16)
        qkv_rows = jnp.dot(normed_one, w_qkv_full, preferred_element_type=F32).astype(BF16)
        queries = qkv_rows[:, :q_width].reshape(tok_rows, KV_HEADS, groups, HEAD)
        ext = halo(qkv_rows[:, q_width:], shards, hop_count + 1).reshape(key_count, 2 * kv_width)
        ext_keys = ext[:, :kv_width].reshape(key_count, KV_HEADS, HEAD)
        ext_values = ext[:, kv_width:].reshape(key_count, KV_HEADS, HEAD)
        scores = (
            jnp.einsum("tngd,snd->ngts", queries, ext_keys, preferred_element_type=F32)
            * score_scale
        )
        masked = jnp.where(allowed, scores, masked_score)
        row_top = jnp.max(masked, axis=-1, keepdims=True)
        log_total = row_top + jnp.log(jnp.sum(jnp.exp(masked - row_top), axis=-1, keepdims=True))
        prob_rows = jnp.exp(masked - log_total).astype(BF16)
        attended = (
            jnp.einsum("ngts,snd->tngd", prob_rows, ext_values, preferred_element_type=F32)
            .astype(BF16)
            .reshape(tok_rows, q_width)
        )
        mixed = stream + jnp.dot(attended, w_out_full, preferred_element_type=F32)
        normed_two = rms_scale(mixed, gain_pair[1]).astype(BF16)
        logits = jnp.dot(normed_two, router_full, preferred_element_type=F32)
        named = jnp.any(routes[layer_no][:, :, None] == expert_ids[None, None, :], axis=1)
        top_logit = jnp.max(jnp.where(named, logits, -jnp.inf), axis=1, keepdims=True)
        powers = jnp.where(named, jnp.exp(jnp.where(named, logits - top_logit, 0.0)), 0.0)
        weights = powers / jnp.sum(powers, axis=1, keepdims=True)
        high = weights.astype(BF16)
        low = (weights - high.astype(F32)).astype(BF16)
        wide_rows = jnp.concatenate(
            [normed_two, high, low, jnp.zeros((tok_rows, extra - 2 * experts_total), BF16)], 1
        )
        x_all = spread(wide_rows, owners).reshape(owners * tok_rows, width + extra)
        partial, gate_up = ffn_forward(
            first_array, x_all, expert_full[layer_no], experts_total, in_rows
        )
        moe_out = collect(partial.reshape(owners, tok_rows, width))
        kept_layers.append(
            (
                stream, normed_one, queries, ext_keys, ext_values, log_total, attended, mixed,
                x_all, gate_up, moe_out, w_qkv_full, w_out_full, router_full, gain_pair,
            )
        )
        stream = mixed + moe_out
    grad_stream = cotangent
    collected = [None] * LAYERS
    dense_parts = [None] * LAYERS
    small_parts = [None] * LAYERS
    for layer_no in reversed(range(LAYERS)):
        (
            layer_input, normed_one, queries, ext_keys, ext_values, log_total, attended, mixed,
            x_all, gate_up, moe_out, w_qkv_full, w_out_full, router_full, gain_pair,
        ) = kept_layers[layer_no]
        mean_d = jnp.sum(grad_stream * moe_out, axis=1, keepdims=True)
        high = mean_d.astype(BF16)
        low = (mean_d - high.astype(F32)).astype(BF16)
        wide_rows = jnp.concatenate(
            [grad_stream.astype(BF16), high, low, jnp.zeros((tok_rows, extra - 2), BF16)], 1
        )
        g_all = spread(wide_rows, owners).reshape(owners * tok_rows, width + extra)
        router_rows = jnp.concatenate(
            [
                lax.dynamic_slice_in_dim(router_full, first_expert, local_experts, 1).T,
                jnp.zeros((side - local_experts, width), BF16),
            ],
            0,
        )
        d_partial, d_experts, d_router_local = ffn_backward(
            first_array, x_all, g_all, gate_up, expert_full[layer_no], router_rows,
            experts_total, in_rows,
        )
        d_experts = lax.psum_scatter(d_experts, "shard", scatter_dimension=0, tiled=True)[0]
        d_normed_two = collect(d_partial.reshape(owners, tok_rows, width))
        _, norm_back = jax.vjp(rms_scale, mixed, gain_pair[1])
        d_mixed_norm, d_gain_two = norm_back(d_normed_two)
        grad_mixed = grad_stream + d_mixed_norm
        d_att = grad_mixed.astype(BF16)
        d_w_out = inner_rows(attended, d_att)
        d_attended = (
            outer_cols(d_att, w_out_full).astype(BF16).reshape(tok_rows, KV_HEADS, groups, HEAD)
        )
        scores = (
            jnp.einsum("tngd,snd->ngts", queries, ext_keys, preferred_element_type=F32)
            * score_scale
        )
        prob_rows = jnp.exp(jnp.where(allowed, scores, masked_score) - log_total)
        d_probs = jnp.einsum("tngd,snd->ngts", d_attended, ext_values, preferred_element_type=F32)
        d_scores = (
            prob_rows * (d_probs - jnp.sum(prob_rows * d_probs, axis=-1, keepdims=True))
        ).astype(BF16)
        d_queries = (
            jnp.einsum("ngts,snd->tngd", d_scores, ext_keys, preferred_element_type=F32)
            * score_scale
        )
        d_keys = (
            jnp.einsum("ngts,tngd->snd", d_scores, queries, preferred_element_type=F32)
            * score_scale
        )
        d_values = jnp.einsum(
            "ngts,tngd->snd", prob_rows.astype(BF16), d_attended, preferred_element_type=F32
        )
        blocks = jnp.concatenate(
            [d_keys.reshape(key_count, kv_width), d_values.reshape(key_count, kv_width)], 1
        ).reshape(hop_count + 1, tok_rows, 2 * kv_width)
        carried = halo_back(blocks.astype(BF16), shards)
        d_qkv = jnp.concatenate([d_queries.reshape(tok_rows, q_width), carried], 1).astype(BF16)
        d_w_qkv = inner_rows(normed_one, d_qkv)
        d_normed_one = outer_cols(d_qkv, w_qkv_full)
        _, norm_back = jax.vjp(rms_scale, layer_input, gain_pair[0])
        d_input_norm, d_gain_one = norm_back(d_normed_one)
        grad_stream = grad_mixed + d_input_norm
        lanes = jnp.arange(experts_total, dtype=jnp.int32)
        d_router = jnp.where(
            (lanes >= first_expert) & (lanes < first_expert + local_experts),
            jnp.tile(d_router_local[:, :local_experts], (1, owners)),
            0.0,
        )
        dense_parts[layer_no] = [d_w_qkv.astype(BF16), d_w_out.astype(BF16)]
        small_parts[layer_no] = [
            d_router.astype(BF16),
            jnp.stack([d_gain_one, d_gain_two], 1).astype(BF16),
        ]
        collected[layer_no] = (
            d_experts[:, :in_rows, :].astype(F32),
            d_experts[:, in_rows:, :].astype(F32),
        )
    parts = sum(dense_parts, []) + sum(small_parts, [])
    parts.append(jnp.zeros((width, side - LAYERS * (experts_total + 2)), BF16))
    d_dense = jnp.concatenate(parts, 1).reshape(shards, width // shards, -1)
    d_dense = reduce_dense(d_dense, shards, owners).astype(F32)
    for layer_no in range(LAYERS):
        at = layer_no * layer_columns
        d_main = d_dense[:, at : at + layer_columns]
        at = LAYERS * layer_columns + layer_no * (experts_total + 2)
        small = d_dense[:, at : at + experts_total + 2]
        collected[layer_no] = (
            small[:, experts_total:].T,
            d_main[:, :qkv_width],
            d_main[:, qkv_width:],
            small[:, :experts_total],
        ) + collected[layer_no]
    stacked = [
        jnp.stack([collected[layer_no][member] for layer_no in range(LAYERS)], 0)
        for member in range(6)
    ]
    results = [stream, grad_stream]
    results.extend(adam_update(gains, stacked[0], gains_first, gains_second))
    results.extend(adam_update(w_qkv, stacked[1], w_qkv_first, w_qkv_second))
    results.extend(adam_update(w_out, stacked[2], w_out_first, w_out_second))
    results.extend(adam_update(router, stacked[3], router_first, router_second))
    results.extend(adam_update(w_in, stacked[4], w_in_first, w_in_second))
    results.extend(adam_update(w_down, stacked[5], w_down_first, w_down_second))
    return tuple(results)


def solution(mesh):
    return jax.shard_map(
        on_device,
        mesh=mesh,
        in_specs=(
            P(("expert", "shard"), None),
            P(("expert", "shard"), None),
            P(),
            P(None, ("expert", "shard"), None),
            P(None, None, "shard"),
            P(None, None, "shard"),
            P(None, None, "shard"),
            P(None, "shard", None),
            P(None, "shard", None),
            P(None, "shard", None),
            P(None, "shard", None),
            P(None, "shard", None),
            P(None, "shard", None),
            P(None, "shard", None),
            P(None, "shard", None),
            P(None, "shard", None),
            P(None, "expert", "shard", None),
            P(None, "expert", "shard", None),
            P(None, "expert", "shard", None),
            P(None, "expert", "shard", None),
            P(None, "expert", "shard", None),
            P(None, "expert", "shard", None),
        ),
        out_specs=(
            P(("expert", "shard"), None),
            P(("expert", "shard"), None),
            P(None, None, "shard"),
            P(None, None, "shard"),
            P(None, None, "shard"),
            P(None, None, "shard"),
            P(None, "shard", None),
            P(None, "shard", None),
            P(None, "shard", None),
            P(None, "shard", None),
            P(None, "shard", None),
            P(None, "shard", None),
            P(None, "shard", None),
            P(None, "shard", None),
            P(None, "shard", None),
            P(None, "shard", None),
            P(None, "shard", None),
            P(None, "shard", None),
            P(None, "expert", "shard", None),
            P(None, "expert", "shard", None),
            P(None, "expert", "shard", None),
            P(None, "expert", "shard", None),
            P(None, "expert", "shard", None),
            P(None, "expert", "shard", None),
            P(None, "expert", "shard", None),
            P(None, "expert", "shard", None),
        ),
        check_vma=False,
    )
```

```python
import functools

import jax
import jax.numpy as jnp
from jax import lax
from jax.experimental import pallas as pl
from jax.experimental.pallas import tpu as pltpu
from jax.sharding import PartitionSpec as P

HEADS = 16
KV_HEADS = 8
HEAD = 64
TOP = 8
LAYERS = 2
WINDOW = 1024
SPAN = 8

norm_eps = 1e-05
masked_score = -1e30
beta_one = 0.9
beta_two = 0.95
adam_eps = 1e-08
learn_rate = 0.05
decay_rate = 0.1
adam_step = 10.0

F32 = jnp.float32
BF16 = jnp.bfloat16
MESH = pl.DeviceIdType.MESH
VMEM_LIMIT = 60 * 1024 * 1024


def rms_scale(values, gain_row):
    return (
        values * lax.rsqrt(jnp.mean(values * values, axis=-1, keepdims=True) + norm_eps) * gain_row
    )


def inner_rows(left_side, right_side):
    return lax.dot_general(
        left_side, right_side, (((0,), (0,)), ((), ())), preferred_element_type=F32
    )


def outer_cols(left_side, right_side):
    return lax.dot_general(
        left_side, right_side, (((1,), (1,)), ((), ())), preferred_element_type=F32
    )


def adam_update(weight, gradient, first_moment, second_moment):
    new_first = beta_one * first_moment + (1.0 - beta_one) * gradient
    new_second = beta_two * second_moment + (1.0 - beta_two) * gradient * gradient
    corr_first = new_first / (1.0 - beta_one**adam_step)
    corr_second = new_second / (1.0 - beta_two**adam_step)
    weight_step = -learn_rate * (
        corr_first / (jnp.sqrt(corr_second) + adam_eps) + decay_rate * weight
    )
    return [gradient, new_first, new_second, weight_step]


def signal(barrier, where):
    pl.semaphore_signal(barrier, inc=1, device_id=where, device_id_type=MESH)


def greet_chips(owners):
    e = lax.axis_index("expert")
    partner = e + 1 - 2 * lax.rem(e, 2)
    barrier = pltpu.get_barrier_semaphore()
    signal(barrier, {"expert": partner})
    for d in range(1, owners // 2):
        signal(barrier, {"expert": lax.rem(e + 2 * d, owners)})
    pl.semaphore_wait(barrier, owners // 2)
    return e, partner


def spread_kernel(owners, cuts, x_ref, o_ref, pair_send, pair_recv, far_send, far_recv):
    e, partner = greet_chips(owners)
    chips = owners // 2
    size = x_ref.shape[0] // cuts

    def pair_copy(d, cut):
        rows = pl.ds(cut * size, size)
        there = o_ref.at[lax.rem(e + owners - 2 * d, owners), rows]
        return pltpu.make_async_remote_copy(
            src_ref=x_ref.at[rows] if d == 0 else there,
            dst_ref=there,
            send_sem=pair_send.at[d, cut],
            recv_sem=pair_recv.at[d, cut],
            device_id={"expert": partner},
            device_id_type=MESH,
        )

    def far_copy(d, cut):
        rows = pl.ds(cut * size, size)
        return pltpu.make_async_remote_copy(
            src_ref=x_ref.at[rows],
            dst_ref=o_ref.at[e, rows],
            send_sem=far_send.at[d - 1, cut],
            recv_sem=far_recv.at[d - 1, cut],
            device_id={"expert": lax.rem(e + 2 * d, owners)},
            device_id_type=MESH,
        )

    for cut in range(cuts):
        for d in range(1, chips):
            far_copy(d, cut).start()
    for cut in range(cuts):
        pair_copy(0, cut).start()
    o_ref[e] = x_ref[...]
    for cut in range(cuts):
        for d in range(1, chips):
            far_copy(d, cut).wait_recv()
            pair_copy(d, cut).start()
    for cut in range(cuts):
        for d in range(chips):
            pair_copy(d, cut).wait()
        for d in range(1, chips):
            far_copy(d, cut).wait_send()


def spread(rows, owners):
    dma = pltpu.SemaphoreType.DMA
    chips, cuts = owners // 2, 4
    return pl.pallas_call(
        functools.partial(spread_kernel, owners, cuts),
        out_shape=jax.ShapeDtypeStruct((owners,) + rows.shape, rows.dtype),
        in_specs=[pl.BlockSpec(memory_space=pltpu.VMEM)],
        out_specs=pl.BlockSpec(memory_space=pltpu.VMEM),
        scratch_shapes=[
            dma((chips, cuts)), dma((chips, cuts)), dma((chips - 1, cuts)), dma((chips - 1, cuts)),
        ],
        compiler_params=pltpu.CompilerParams(
            collective_id=1, has_side_effects=True, vmem_limit_bytes=VMEM_LIMIT
        ),
        name="spread",
    )(rows)


def collect_kernel(
    owners, cuts, p_ref, o_ref, paired, going, came, pair_send, pair_recv, far_send, far_recv
):
    e, partner = greet_chips(owners)
    chips = owners // 2
    size = o_ref.shape[0] // cuts

    def pair_copy(d, cut):
        rows = pl.ds(cut * size, size)
        return pltpu.make_async_remote_copy(
            src_ref=p_ref.at[lax.rem(partner + 2 * d, owners), rows],
            dst_ref=paired.at[d, rows],
            send_sem=pair_send.at[d, cut],
            recv_sem=pair_recv.at[d, cut],
            device_id={"expert": partner},
            device_id_type=MESH,
        )

    def far_copy(d, cut):
        rows = pl.ds(cut * size, size)
        return pltpu.make_async_remote_copy(
            src_ref=going.at[d - 1, rows],
            dst_ref=came.at[d - 1, rows],
            send_sem=far_send.at[d - 1, cut],
            recv_sem=far_recv.at[d - 1, cut],
            device_id={"expert": lax.rem(e + 2 * d, owners)},
            device_id_type=MESH,
        )

    for cut in range(cuts):
        for d in range(1, chips):
            pair_copy(d, cut).start()
    for cut in range(cuts):
        pair_copy(0, cut).start()
    for cut in range(cuts):
        rows = pl.ds(cut * size, size)
        for d in range(1, chips):
            pair_copy(d, cut).wait_recv()
            going[d - 1, rows, :] = (
                p_ref[lax.rem(e + 2 * d, owners), rows, :].astype(F32)
                + paired[d, rows, :].astype(F32)
            ).astype(BF16)
            far_copy(d, cut).start()
    for cut in range(cuts):
        rows = pl.ds(cut * size, size)
        pair_copy(0, cut).wait_recv()
        total = p_ref[e, rows, :].astype(F32) + paired[0, rows, :].astype(F32)
        for d in range(1, chips):
            far_copy(d, cut).wait_recv()
            total = total + came[d - 1, rows, :].astype(F32)
        o_ref[rows, :] = total
    for cut in range(cuts):
        for d in range(chips):
            pair_copy(d, cut).wait_send()
        for d in range(1, chips):
            far_copy(d, cut).wait_send()


def collect(parts):
    owners, rows, width = parts.shape
    dma = pltpu.SemaphoreType.DMA
    chips, cuts = owners // 2, 4
    return pl.pallas_call(
        functools.partial(collect_kernel, owners, cuts),
        out_shape=jax.ShapeDtypeStruct((rows, width), F32),
        in_specs=[pl.BlockSpec(memory_space=pltpu.VMEM)],
        out_specs=pl.BlockSpec(memory_space=pltpu.VMEM),
        scratch_shapes=[
            pltpu.VMEM((chips, rows, width), parts.dtype),
            pltpu.VMEM((chips - 1, rows, width), parts.dtype),
            pltpu.VMEM((chips - 1, rows, width), parts.dtype),
            dma((chips, cuts)), dma((chips, cuts)), dma((chips - 1, cuts)), dma((chips - 1, cuts)),
        ],
        compiler_params=pltpu.CompilerParams(
            collective_id=2, has_side_effects=True, vmem_limit_bytes=VMEM_LIMIT
        ),
        name="collect",
    )(parts)


def ring_shard(place, count):
    back = lax.div(place, count // 2)
    return (1 - back) * 2 * place + back * (2 * (count - 1 - place) + 1)


def ring_place(shard, count):
    odd, pair = lax.rem(shard, 2), lax.div(shard, 2)
    return (1 - odd) * pair + odd * (count - 1 - pair)


def gather_dense_kernel(
    n, rows, x_ref, o_ref, ring_send, ring_recv, pair_send, pair_recv, own_sem
):
    e, s = lax.axis_index("expert"), lax.axis_index("shard")
    core = lax.rem(e, 2)
    partner = e + 1 - 2 * core
    p = ring_place(s, n)
    ways = (ring_shard(lax.rem(p + 1, n), n), ring_shard(lax.rem(p + n - 1, n), n))
    barrier = pltpu.get_barrier_semaphore()
    signal(barrier, {"expert": partner})
    signal(barrier, {"shard": ways[0]})
    signal(barrier, {"shard": ways[1]})
    pl.semaphore_wait(barrier, 3)
    quarter = rows // 4

    def part(side, way):
        return pl.ds(pl.multiple_of(side * 2 * quarter + way * quarter, quarter), quarter)

    def block(way, k):
        return ring_shard(lax.rem(p + (n - k if way == 0 else k), n), n)

    def ring_copy(way, k, src):
        return pltpu.make_async_remote_copy(
            src_ref=src,
            dst_ref=o_ref.at[block(way, k), part(core, way)],
            send_sem=ring_send.at[way, k],
            recv_sem=ring_recv.at[way, k],
            device_id={"shard": ways[way]},
            device_id_type=MESH,
        )

    def pair_copy(way, k, side):
        there = o_ref.at[block(way, k), part(side, way)]
        return pltpu.make_async_remote_copy(
            src_ref=there,
            dst_ref=there,
            send_sem=pair_send.at[way, k - 1],
            recv_sem=pair_recv.at[way, k - 1],
            device_id={"expert": partner},
            device_id_type=MESH,
        )

    for way in range(2):
        ring_copy(way, 0, x_ref.at[part(core, way)]).start()
    own = pltpu.make_async_copy(x_ref, o_ref.at[s], own_sem)
    own.start()

    def step(k, carry):
        for way in range(2):
            came = o_ref.at[block(way, k), part(core, way)]
            pltpu.make_async_remote_copy(
                src_ref=came,
                dst_ref=came,
                send_sem=ring_send.at[way, k - 1],
                recv_sem=ring_recv.at[way, k - 1],
                device_id={"shard": ways[way]},
                device_id_type=MESH,
            ).wait_recv()

            @pl.when(k < n - 1)
            def _():
                ring_copy(way, k, came).start()

            pair_copy(way, k, core).start()
        return carry

    lax.fori_loop(1, n, step, 0)

    def finish(k, carry):
        for way in range(2):
            ring_copy(way, k - 1, x_ref.at[part(core, way)]).wait_send()
            pair_copy(way, k, core).wait_send()
            pair_copy(way, k, 1 - core).wait_recv()
        return carry

    lax.fori_loop(1, n, finish, 0)
    own.wait()


def gather_dense(piece, n):
    rows, columns = piece.shape
    dma = pltpu.SemaphoreType.DMA
    return pl.pallas_call(
        functools.partial(gather_dense_kernel, n, rows),
        out_shape=jax.ShapeDtypeStruct((n, rows, columns), piece.dtype),
        in_specs=[pl.BlockSpec(memory_space=pltpu.VMEM)],
        out_specs=pl.BlockSpec(memory_space=pl.ANY),
        scratch_shapes=[
            dma((2, n - 1)), dma((2, n - 1)), dma((2, n - 1)), dma((2, n - 1)), dma,
        ],
        compiler_params=pltpu.CompilerParams(
            collective_id=3, has_side_effects=True, vmem_limit_bytes=VMEM_LIMIT
        ),
        name="gather_dense",
    )(piece)


def reduce_dense_kernel(
    n, owners, rows, places, *refs,
):
    g_refs = refs[: len(places)]
    (
        o_ref, paired, came, going, crossed, last_in, pair_send, pair_recv, ring_send,
        ring_recv, cross_send, cross_recv, last_send, last_recv,
    ) = refs[len(places) :]
    e, s = lax.axis_index("expert"), lax.axis_index("shard")
    core, x = lax.rem(e, 2), lax.div(e, 2)
    partner = e + 1 - 2 * core
    columns = owners // 2
    p = ring_place(s, n)
    ways = (ring_shard(lax.rem(p + 1, n), n), ring_shard(lax.rem(p + n - 1, n), n))
    barrier = pltpu.get_barrier_semaphore()
    signal(barrier, {"expert": partner})
    signal(barrier, {"shard": ways[0]})
    signal(barrier, {"shard": ways[1]})
    for d in range(1, columns):
        signal(barrier, {"expert": lax.rem(e + 2 * d, owners)})
    pl.semaphore_wait(barrier, 3 + columns - 1)
    half, quarter = rows // 2, rows // 4

    def mine(way):
        return pl.ds(pl.multiple_of(core * half + way * quarter, quarter), quarter)

    def block(way, k):
        return ring_shard(lax.rem(p + (2 * n - 1 - k if way == 0 else k + 1), n), n)

    def pair_copy(k, i):
        b = block(0, k)
        at, wide = places[i]
        return pltpu.make_async_remote_copy(
            src_ref=g_refs[i].at[b, pl.ds(pl.multiple_of((1 - core) * half, half), half)],
            dst_ref=paired.at[b, :, pl.ds(at, wide)],
            send_sem=pair_send.at[i, b],
            recv_sem=pair_recv.at[i, b],
            device_id={"expert": partner},
            device_id_type=MESH,
        )

    def ring_copy(way, k):
        return pltpu.make_async_remote_copy(
            src_ref=going.at[way, k],
            dst_ref=came.at[way, k],
            send_sem=ring_send.at[way, k],
            recv_sem=ring_recv.at[way, k],
            device_id={"shard": ways[way]},
            device_id_type=MESH,
        )

    def put(target, way, b, more=None):
        for g_ref, (at, wide) in zip(g_refs, places):
            total = g_ref[b, mine(way), :].astype(F32) + paired[
                b, way * quarter : (way + 1) * quarter, at : at + wide
            ].astype(F32)
            if more is not None:
                total = total + more[:, at : at + wide].astype(F32)
            target[:, at : at + wide] = total.astype(BF16)

    order = []
    for k in range(n):
        for place in (k, n - 2 - k):
            place = place % n
            if place not in order:
                order.append(place)
    every = range(len(places))
    for k in order:
        for i in every:
            pair_copy(k, i).start()
    for k in order[:2]:
        for i in every:
            pair_copy(k, i).wait_recv()
    for way in range(2):
        put(going.at[way, 0], way, block(way, 0))
        ring_copy(way, 0).start()
    for k in order[2:]:
        for i in every:
            pair_copy(k, i).wait_recv()

    def step(k, carry):
        for way in range(2):
            ring_copy(way, k - 1).wait_recv()
            put(going.at[way, k], way, block(way, k), came.at[way, k - 1])
            ring_copy(way, k).start()
        return carry

    lax.fori_loop(1, n - 1, step, 0)
    for way in range(2):
        ring_copy(way, n - 2).wait_recv()
        put(
            crossed.at[x, pl.ds(way * quarter, quarter)], way, s, came.at[way, n - 2]
        )

    def cross_copy(d):
        return pltpu.make_async_remote_copy(
            src_ref=crossed.at[x],
            dst_ref=crossed.at[x],
            send_sem=cross_send.at[d - 1],
            recv_sem=cross_recv.at[d - 1],
            device_id={"expert": lax.rem(e + 2 * d, owners)},
            device_id_type=MESH,
        )

    for d in range(1, columns):
        cross_copy(d).start()
    for d in range(1, columns):
        cross_copy(d).wait()
    total = crossed[0].astype(F32)
    for d in range(1, columns):
        total = total + crossed[d].astype(F32)
    here = pl.ds(pl.multiple_of(core * half, half), half)
    o_ref[here, :] = total.astype(BF16)
    last = pltpu.make_async_remote_copy(
        src_ref=o_ref.at[here],
        dst_ref=last_in,
        send_sem=last_send,
        recv_sem=last_recv,
        device_id={"expert": partner},
        device_id_type=MESH,
    )
    last.start()
    for k in order:
        for i in every:
            pair_copy(k, i).wait_send()

    def finish(k, carry):
        for way in range(2):
            ring_copy(way, k).wait_send()
        return carry

    lax.fori_loop(0, n - 1, finish, 0)
    last.wait()
    o_ref[pl.ds(pl.multiple_of((1 - core) * half, half), half), :] = last_in[...]


def reduce_dense(grads, n, owners):
    rows = grads[0].shape[1]
    places, columns = [], 0
    for grad in grads:
        places.append((columns, grad.shape[2]))
        columns += grad.shape[2]
    dma = pltpu.SemaphoreType.DMA
    across = owners // 2
    return pl.pallas_call(
        functools.partial(reduce_dense_kernel, n, owners, rows, tuple(places)),
        out_shape=jax.ShapeDtypeStruct((rows, columns), BF16),
        in_specs=[pl.BlockSpec(memory_space=pltpu.VMEM)] * len(places),
        out_specs=pl.BlockSpec(memory_space=pltpu.VMEM),
        scratch_shapes=[
            pltpu.VMEM((n, rows // 2, columns), BF16),
            pltpu.VMEM((2, n - 1, rows // 4, columns), BF16),
            pltpu.VMEM((2, n - 1, rows // 4, columns), BF16),
            pltpu.VMEM((across, rows // 2, columns), BF16),
            pltpu.VMEM((rows // 2, columns), BF16),
            dma((len(places), n)), dma((len(places), n)), dma((2, n - 1)), dma((2, n - 1)),
            dma((across - 1,)), dma((across - 1,)), dma, dma,
        ],
        compiler_params=pltpu.CompilerParams(
            collective_id=4, has_side_effects=True, vmem_limit_bytes=VMEM_LIMIT
        ),
        name="reduce_dense",
    )(*grads)


def halo_links(n, s):
    odd = lax.rem(s, 2)
    return odd, s + 1 - 2 * odd, s + 2 < n, s >= 2


def halo_barrier(s, odd, mate, ahead, behind, sends_back):
    barrier = pltpu.get_barrier_semaphore()
    even = odd == 0
    to_ahead, to_behind = (ahead, behind) if not sends_back else (behind, ahead)
    step = -2 if not sends_back else 2
    mate_copies = (odd == 1) | behind if not sends_back else even | behind
    to_mate = even | behind if not sends_back else (odd == 1) | behind

    @pl.when(to_behind)
    def _():
        signal(barrier, {"shard": s + step})

    @pl.when(mate_copies)
    def _():
        signal(barrier, {"shard": mate})

    @pl.when(to_ahead & to_mate)
    def _():
        pl.semaphore_wait(barrier, 2)

    @pl.when(to_ahead != to_mate)
    def _():
        pl.semaphore_wait(barrier, 1)


def halo_kernel(n, rows, cuts, kv_ref, o_ref, sends, recvs, own_sem):
    s = lax.axis_index("shard")
    odd, mate, ahead, behind = halo_links(n, s)
    even = odd == 0
    size = rows // cuts

    def copy(kind, cut, src, slot, where):
        return pltpu.make_async_remote_copy(
            src_ref=src.at[pl.ds(cut * size, size)],
            dst_ref=o_ref.at[slot, pl.ds(cut * size, size)],
            send_sem=sends.at[kind, cut],
            recv_sem=recvs.at[kind, cut],
            device_id={"shard": where},
            device_id_type=MESH,
        )

    halo_barrier(s, odd, mate, ahead, behind, False)
    from_odd = (o_ref.at[2], o_ref.at[0])
    from_even = (kv_ref, o_ref.at[2])
    for cut in range(cuts):

        @pl.when(ahead)
        def _():
            copy(0, cut, kv_ref, 2, s + 2).start()

        @pl.when(even)
        def _():
            copy(2, cut, kv_ref, 3, mate).start()

    o_ref[4] = kv_ref[...]
    for slot in range(4):

        @pl.when(s < 4 - slot)
        def _():
            o_ref[slot] = jnp.zeros_like(o_ref[slot])

    for cut in range(cuts):

        @pl.when(behind)
        def _():
            copy(0, cut, kv_ref, 2, s).wait_recv()

        @pl.when(behind & ahead)
        def _():
            copy(1, cut, o_ref.at[2], 0, s + 2).start()

        @pl.when(behind & (odd == 1))
        def _():
            copy(2, cut, from_odd[0], 3, mate).start()

        @pl.when(behind & even)
        def _():
            copy(3, cut, from_even[1], 1, mate).start()

    for cut in range(cuts):

        @pl.when(s >= 4)
        def _():
            copy(1, cut, o_ref.at[2], 0, s).wait_recv()

        @pl.when((s >= 4) & (odd == 1))
        def _():
            copy(3, cut, from_odd[1], 1, mate).start()

    for cut in range(cuts):

        @pl.when(s >= 1)
        def _():
            copy(2, cut, kv_ref, 3, mate).wait_recv()

        @pl.when(s >= 3)
        def _():
            copy(3, cut, kv_ref, 1, mate).wait_recv()

        @pl.when(ahead)
        def _():
            copy(0, cut, kv_ref, 2, s).wait_send()

        @pl.when(behind & ahead)
        def _():
            copy(1, cut, kv_ref, 0, s).wait_send()

        @pl.when(even | behind)
        def _():
            copy(2, cut, kv_ref, 3, mate).wait_send()

        @pl.when((even & behind) | ((odd == 1) & (s >= 4)))
        def _():
            copy(3, cut, kv_ref, 1, mate).wait_send()


def halo(kv, n, slots):
    rows, columns = kv.shape
    dma = pltpu.SemaphoreType.DMA
    cuts = 2
    return pl.pallas_call(
        functools.partial(halo_kernel, n, rows, cuts),
        out_shape=jax.ShapeDtypeStruct((slots, rows, columns), kv.dtype),
        in_specs=[pl.BlockSpec(memory_space=pltpu.VMEM)],
        out_specs=pl.BlockSpec(memory_space=pltpu.VMEM),
        scratch_shapes=[dma((4, cuts)), dma((4, cuts)), dma],
        compiler_params=pltpu.CompilerParams(
            collective_id=5, has_side_effects=True, vmem_limit_bytes=VMEM_LIMIT
        ),
        name="halo",
    )(kv)


def halo_back_kernel(n, rows, cuts, g_ref, o_ref, own, came, sends, recvs):
    s = lax.axis_index("shard")
    odd, mate, ahead, behind = halo_links(n, s)
    even = odd == 0
    size = rows // cuts

    def copy(kind, cut, src, where):
        return pltpu.make_async_remote_copy(
            src_ref=src.at[pl.ds(cut * size, size)],
            dst_ref=came.at[kind, pl.ds(cut * size, size)],
            send_sem=sends.at[kind, cut],
            recv_sem=recvs.at[kind, cut],
            device_id={"shard": where},
            device_id_type=MESH,
        )

    def there(ref, cut, value=None):
        here = pl.ds(cut * size, size)
        return ref[here, :].astype(F32)

    halo_barrier(s, odd, mate, ahead, behind, True)
    for cut in range(cuts):

        @pl.when(s >= 3)
        def _():
            copy(3, cut, g_ref.at[1], mate).start()

        @pl.when(s >= 1)
        def _():
            copy(2, cut, g_ref.at[3], mate).start()

    for cut in range(cuts):
        here = pl.ds(cut * size, size)

        @pl.when((odd == 1) & (s >= 4))
        def _():
            copy(3, cut, g_ref.at[1], mate).wait_recv()
            own[0, here, :] = (there(g_ref.at[0], cut) + there(came.at[3], cut)).astype(BF16)

        @pl.when((odd == 1) & (s >= 4))
        def _():
            copy(1, cut, own.at[0], s - 2).start()

        @pl.when(even & (s >= 4))
        def _():
            copy(1, cut, g_ref.at[0], s - 2).start()

    for cut in range(cuts):
        here = pl.ds(cut * size, size)

        @pl.when((odd == 1) & behind)
        def _():
            copy(2, cut, g_ref.at[3], mate).wait_recv()
            own[1, here, :] = (there(g_ref.at[2], cut) + there(came.at[2], cut)).astype(BF16)

        @pl.when(even & behind)
        def _():
            copy(3, cut, g_ref.at[1], mate).wait_recv()
            own[1, here, :] = (there(g_ref.at[2], cut) + there(came.at[3], cut)).astype(BF16)

        @pl.when(behind & ahead)
        def _():
            copy(1, cut, g_ref.at[0], s).wait_recv()
            own[1, here, :] = (there(own.at[1], cut) + there(came.at[1], cut)).astype(BF16)

        @pl.when(behind)
        def _():
            copy(0, cut, own.at[1], s - 2).start()

    for cut in range(cuts):
        here = pl.ds(cut * size, size)
        o_ref[here, :] = there(g_ref.at[4], cut)

        @pl.when(even)
        def _():
            copy(2, cut, g_ref.at[3], mate).wait_recv()
            o_ref[here, :] += there(came.at[2], cut)

        @pl.when(ahead)
        def _():
            copy(0, cut, own.at[1], s).wait_recv()
            o_ref[here, :] += there(came.at[0], cut)

        @pl.when(s >= 3)
        def _():
            copy(3, cut, g_ref.at[1], mate).wait_send()

        @pl.when(s >= 1)
        def _():
            copy(2, cut, g_ref.at[3], mate).wait_send()

        @pl.when(s >= 4)
        def _():
            copy(1, cut, g_ref.at[0], mate).wait_send()

        @pl.when(behind)
        def _():
            copy(0, cut, own.at[1], mate).wait_send()


def halo_back(grads, n):
    slots, rows, columns = grads.shape
    dma = pltpu.SemaphoreType.DMA
    cuts = 2
    return pl.pallas_call(
        functools.partial(halo_back_kernel, n, rows, cuts),
        out_shape=jax.ShapeDtypeStruct((rows, columns), F32),
        in_specs=[pl.BlockSpec(memory_space=pltpu.VMEM)],
        out_specs=pl.BlockSpec(memory_space=pltpu.VMEM),
        scratch_shapes=[
            pltpu.VMEM((3, rows, columns), BF16),
            pltpu.VMEM((4, rows, columns), BF16),
            dma((4, cuts)),
            dma((4, cuts)),
        ],
        compiler_params=pltpu.CompilerParams(
            collective_id=6, has_side_effects=True, vmem_limit_bytes=VMEM_LIMIT
        ),
        name="halo_back",
    )(grads)


def column_of(extra, index, experts_total):
    lanes = lax.broadcasted_iota(jnp.int32, extra.shape, 1)
    hit = (lanes == index) | (lanes == index + experts_total)
    return jnp.sum(jnp.where(hit, extra.astype(F32), 0.0), axis=1, keepdims=True)


def ffn_forward_kernel(
    tile, width, in_rows, experts_total, first_ref, x_ref, w_ref, part_ref, gate_up_ref, acc
):
    e = pl.program_id(0)
    w_in = w_ref[:, 0, :in_rows, :].reshape(width, w_ref.shape[-1])
    w_down = w_ref[:, 0, in_rows:, :].reshape(-1, width)
    half = w_in.shape[1] // 2
    index = first_ref[0] + e
    count = x_ref.shape[0] // tile
    for t in range(count):
        rows = pl.ds(t * tile, tile)
        gate_up = jnp.dot(x_ref[rows, :width], w_in, preferred_element_type=F32)
        gate, up = gate_up[:, :half], gate_up[:, half:]
        gate_up_ref[0, rows, :] = gate_up.astype(BF16)
        weight = column_of(x_ref[rows, width:], index, experts_total)
        hidden = (gate * jax.nn.sigmoid(gate) * up * weight).astype(BF16)
        out = jnp.dot(hidden, w_down, preferred_element_type=F32)

        @pl.when(e == 0)
        def _():
            acc[rows, :] = out

        @pl.when(e > 0)
        def _():
            acc[rows, :] += out

        @pl.when(e == pl.num_programs(0) - 1)
        def _():
            part_ref[rows, :] = acc[rows, :].astype(BF16)


def ffn_forward(first, x_all, w_all, experts_total, in_rows):
    shards, local, piece, inner = w_all.shape
    tokens, wide = x_all.shape
    width = in_rows * shards
    return pl.pallas_call(
        functools.partial(ffn_forward_kernel, 256, width, in_rows, experts_total),
        grid_spec=pltpu.PrefetchScalarGridSpec(
            num_scalar_prefetch=1,
            grid=(local,),
            in_specs=[
                pl.BlockSpec((tokens, wide), lambda e, f: (0, 0)),
                pl.BlockSpec((shards, 1, piece, inner), lambda e, f: (0, e, 0, 0)),
            ],
            out_specs=[
                pl.BlockSpec((tokens, width), lambda e, f: (0, 0)),
                pl.BlockSpec((1, tokens, inner), lambda e, f: (e, 0, 0)),
            ],
            scratch_shapes=[pltpu.VMEM((tokens, width), F32)],
        ),
        out_shape=[
            jax.ShapeDtypeStruct((tokens, width), BF16),
            jax.ShapeDtypeStruct((local, tokens, inner), BF16),
        ],
        compiler_params=pltpu.CompilerParams(vmem_limit_bytes=VMEM_LIMIT),
        cost_estimate=pl.CostEstimate(
            flops=2 * local * tokens * width * (inner + inner // 2),
            bytes_accessed=2 * (w_all.size + local * tokens * inner + 2 * tokens * wide),
            transcendentals=0,
        ),
        name="ffn_forward",
    )(first, x_all, w_all)


def ffn_backward_kernel(
    tile,
    width,
    in_rows,
    experts_total,
    first_ref,
    x_ref,
    g_ref,
    gate_up_ref,
    w_ref,
    router_ref,
    part_ref,
    grad_ref,
    router_grad_ref,
    acc,
    d_gate_up,
    hidden_all,
    d_logits,
):
    e = pl.program_id(0)
    inner = w_ref.shape[-1]
    w_in = w_ref[:, 0, :in_rows, :].reshape(width, inner)
    w_down = w_ref[:, 0, in_rows:, :].reshape(-1, width)
    half = inner // 2
    index = first_ref[0] + e
    tokens = x_ref.shape[0]
    last = pl.num_programs(0) - 1
    for t in range(tokens // tile):
        rows = pl.ds(t * tile, tile)
        d_plain = outer_cols(g_ref[rows, :width], w_down)
        gate = gate_up_ref[0, rows, :half].astype(F32)
        up = gate_up_ref[0, rows, half:].astype(F32)
        weight = column_of(x_ref[rows, width:], index, experts_total)
        mean_d = column_of(g_ref[rows, width:], 0, 1)
        sig = jax.nn.sigmoid(gate)
        silu = gate * sig
        hidden = silu * up
        d_weight = jnp.sum(hidden * d_plain, axis=1, keepdims=True)
        d_hidden = d_plain * weight
        hidden_all[rows, :] = (hidden * weight).astype(BF16)
        d_gate_up[rows, :half] = (d_hidden * up * sig * (1.0 + gate * (1.0 - sig))).astype(BF16)
        d_gate_up[rows, half:] = (d_hidden * silu).astype(BF16)
        lanes = lax.broadcasted_iota(jnp.int32, (tile, d_logits.shape[1]), 1)
        d_logit = jnp.where(lanes == e, weight * (d_weight - mean_d), 0.0).astype(BF16)
        out = outer_cols(d_gate_up[rows, :], w_in)

        @pl.when(e == 0)
        def _():
            acc[rows, :] = out
            d_logits[rows, :] = d_logit

        @pl.when(e > 0)
        def _():
            acc[rows, :] += out
            d_logits[rows, :] += d_logit

    x = x_ref[:, :width]
    grad_ref[:, 0, :in_rows, :] = (
        inner_rows(x, d_gate_up[...]).astype(BF16).reshape(-1, in_rows, inner)
    )
    grad_ref[:, 0, in_rows:, :] = (
        inner_rows(hidden_all[...], g_ref[:, :width])
        .astype(BF16)
        .reshape(-1, w_ref.shape[2] - in_rows, width)
    )

    @pl.when(e == last)
    def _():
        for t in range(tokens // tile):
            rows = pl.ds(t * tile, tile)
            out = acc[rows, :] + jnp.dot(
                d_logits[rows, :], router_ref[...], preferred_element_type=F32
            )
            part_ref[rows, :] = out.astype(BF16)
        router_grad_ref[...] = inner_rows(x, d_logits[...])


def ffn_backward(first, x_all, g_all, gate_up, w_all, router_rows, experts_total, in_rows):
    shards, local, piece, inner = w_all.shape
    tokens, wide = x_all.shape
    width = in_rows * shards
    lanes = router_rows.shape[0]
    return pl.pallas_call(
        functools.partial(ffn_backward_kernel, 256, width, in_rows, experts_total),
        grid_spec=pltpu.PrefetchScalarGridSpec(
            num_scalar_prefetch=1,
            grid=(local,),
            in_specs=[
                pl.BlockSpec((tokens, wide), lambda e, f: (0, 0)),
                pl.BlockSpec((tokens, g_all.shape[1]), lambda e, f: (0, 0)),
                pl.BlockSpec((1, tokens, inner), lambda e, f: (e, 0, 0)),
                pl.BlockSpec((shards, 1, piece, inner), lambda e, f: (0, e, 0, 0)),
                pl.BlockSpec((lanes, width), lambda e, f: (0, 0)),
            ],
            out_specs=[
                pl.BlockSpec((tokens, width), lambda e, f: (0, 0)),
                pl.BlockSpec((shards, 1, piece, inner), lambda e, f: (0, e, 0, 0)),
                pl.BlockSpec((width, lanes), lambda e, f: (0, 0)),
            ],
            scratch_shapes=[
                pltpu.VMEM((tokens, width), F32),
                pltpu.VMEM((tokens, inner), BF16),
                pltpu.VMEM((tokens, inner // 2), BF16),
                pltpu.VMEM((tokens, lanes), BF16),
            ],
        ),
        out_shape=[
            jax.ShapeDtypeStruct((tokens, width), BF16),
            jax.ShapeDtypeStruct(w_all.shape, BF16),
            jax.ShapeDtypeStruct((width, lanes), F32),
        ],
        compiler_params=pltpu.CompilerParams(vmem_limit_bytes=VMEM_LIMIT),
        cost_estimate=pl.CostEstimate(
            flops=4 * local * tokens * width * (inner + inner // 2),
            bytes_accessed=2 * (2 * w_all.size + local * tokens * inner + 4 * tokens * wide),
            transcendentals=0,
        ),
        name="ffn_backward",
    )(first, x_all, g_all, gate_up, w_all, router_rows)


def on_device(
    hidden_in,
    cotangent,
    doc_lengths,
    routes,
    gains,
    gains_first,
    gains_second,
    w_qkv,
    w_qkv_first,
    w_qkv_second,
    w_out,
    w_out_first,
    w_out_second,
    router,
    router_first,
    router_second,
    w_in,
    w_in_first,
    w_in_second,
    w_down,
    w_down_first,
    w_down_second,
):
    tok_rows, width = hidden_in.shape
    owners = lax.axis_size("expert")
    shards = lax.axis_size("shard")
    local_experts = w_in.shape[1]
    in_rows = w_in.shape[2]
    experts_total = local_experts * owners
    seq_len = tok_rows * SPAN
    hop_count = min(-(-WINDOW // tok_rows), SPAN - 1)
    key_count = (hop_count + 1) * tok_rows
    q_width = HEADS * HEAD
    kv_width = KV_HEADS * HEAD
    qkv_width = q_width + 2 * kv_width
    groups = HEADS // KV_HEADS
    score_scale = HEAD ** (-0.5)
    extra = -(-2 * experts_total // 128) * 128
    my_owner = lax.axis_index("expert")
    first_expert = my_owner * local_experts
    first_array = first_expert.astype(jnp.int32).reshape(1)
    row_start = (my_owner * shards + lax.axis_index("shard")) * tok_rows
    my_seq = row_start // seq_len
    doc_ends = jnp.cumsum(lax.dynamic_slice_in_dim(doc_lengths, my_seq, 1, 0)[0])
    query_rows = row_start + jnp.arange(tok_rows, dtype=jnp.int32)
    key_rows = row_start - hop_count * tok_rows + jnp.arange(key_count, dtype=jnp.int32)
    query_docs = jnp.sum(
        (query_rows[:, None] % seq_len >= doc_ends[None, :]).astype(jnp.int32), axis=1
    )
    key_docs = jnp.sum((key_rows[:, None] % seq_len >= doc_ends[None, :]).astype(jnp.int32), axis=1)
    distance = query_rows[:, None] - key_rows[None, :]
    allowed = (
        (query_rows[:, None] // seq_len == key_rows[None, :] // seq_len)
        & (query_docs[:, None] == key_docs[None, :])
        & (distance >= 0)
        & (distance < WINDOW)
    )
    expert_ids = jnp.arange(experts_total, dtype=jnp.int32)
    side = 128

    def dense_piece(layer_no):
        rows = w_qkv.shape[1]
        return jnp.concatenate(
            [
                w_qkv[layer_no].astype(BF16),
                w_out[layer_no].astype(BF16),
                router[layer_no].astype(BF16),
                gains[layer_no].T.astype(BF16),
                jnp.zeros((rows, side - experts_total - 2), BF16),
            ],
            1,
        )

    def expert_piece(layer_no):
        return jnp.concatenate(
            [w_in[layer_no].astype(BF16), w_down[layer_no].astype(BF16)], 1
        )

    layer_columns = qkv_width + width
    dense = gather_dense(dense_piece(0), shards)
    expert_full = []
    for layer_no in range(LAYERS):
        piece, dense = lax.optimization_barrier((expert_piece(layer_no), dense))
        expert_full.append(lax.all_gather(piece, "shard", axis=0, tiled=False))

    kept_layers = []
    stream = hidden_in
    for layer_no in range(LAYERS):
        dense = dense.reshape(width, -1)
        w_qkv_full = dense[:, :qkv_width]
        w_out_full = dense[:, qkv_width:layer_columns]
        small = dense[:, layer_columns:]
        router_full = small[:, :experts_total]
        gain_pair = small[:, experts_total : experts_total + 2].astype(F32).T
        normed_one = rms_scale(stream, gain_pair[0]).astype(BF16)
        qkv_rows = jnp.dot(normed_one, w_qkv_full, preferred_element_type=F32).astype(BF16)
        queries = qkv_rows[:, :q_width].reshape(tok_rows, KV_HEADS, groups, HEAD)
        ext = halo(qkv_rows[:, q_width:], shards, hop_count + 1).reshape(key_count, 2 * kv_width)
        ext_keys = ext[:, :kv_width].reshape(key_count, KV_HEADS, HEAD)
        ext_values = ext[:, kv_width:].reshape(key_count, KV_HEADS, HEAD)
        scores = (
            jnp.einsum("tngd,snd->ngts", queries, ext_keys, preferred_element_type=F32)
            * score_scale
        )
        masked = jnp.where(allowed, scores, masked_score)
        row_top = jnp.max(masked, axis=-1, keepdims=True)
        log_total = row_top + jnp.log(jnp.sum(jnp.exp(masked - row_top), axis=-1, keepdims=True))
        prob_rows = jnp.exp(masked - log_total).astype(BF16)
        attended = (
            jnp.einsum("ngts,snd->tngd", prob_rows, ext_values, preferred_element_type=F32)
            .astype(BF16)
            .reshape(tok_rows, q_width)
        )
        mixed = stream + jnp.dot(attended, w_out_full, preferred_element_type=F32)
        normed_two = rms_scale(mixed, gain_pair[1]).astype(BF16)
        logits = jnp.dot(normed_two, router_full, preferred_element_type=F32)
        named = jnp.any(routes[layer_no][:, :, None] == expert_ids[None, None, :], axis=1)
        top_logit = jnp.max(jnp.where(named, logits, -jnp.inf), axis=1, keepdims=True)
        powers = jnp.where(named, jnp.exp(jnp.where(named, logits - top_logit, 0.0)), 0.0)
        weights = powers / jnp.sum(powers, axis=1, keepdims=True)
        high = weights.astype(BF16)
        low = (weights - high.astype(F32)).astype(BF16)
        wide_rows = jnp.concatenate(
            [normed_two, high, low, jnp.zeros((tok_rows, extra - 2 * experts_total), BF16)], 1
        )
        x_all = spread(wide_rows, owners).reshape(owners * tok_rows, width + extra)
        if layer_no + 1 < LAYERS:
            piece, x_all = lax.optimization_barrier((dense_piece(layer_no + 1), x_all))
            dense = gather_dense(piece, shards)
            dense, x_all = lax.optimization_barrier((dense, x_all))
        partial, gate_up = ffn_forward(
            first_array, x_all, expert_full[layer_no], experts_total, in_rows
        )
        moe_out = collect(partial.reshape(owners, tok_rows, width))
        kept_layers.append(
            (
                stream, normed_one, queries, ext_keys, ext_values, log_total, attended, mixed,
                x_all, gate_up, moe_out, w_qkv_full, w_out_full, router_full, gain_pair,
            )
        )
        stream = mixed + moe_out
    grad_stream = cotangent
    collected = [None] * LAYERS
    dense_parts = [None] * LAYERS
    small_parts = [None] * LAYERS
    for layer_no in reversed(range(LAYERS)):
        (
            layer_input, normed_one, queries, ext_keys, ext_values, log_total, attended, mixed,
            x_all, gate_up, moe_out, w_qkv_full, w_out_full, router_full, gain_pair,
        ) = kept_layers[layer_no]
        mean_d = jnp.sum(grad_stream * moe_out, axis=1, keepdims=True)
        high = mean_d.astype(BF16)
        low = (mean_d - high.astype(F32)).astype(BF16)
        wide_rows = jnp.concatenate(
            [grad_stream.astype(BF16), high, low, jnp.zeros((tok_rows, extra - 2), BF16)], 1
        )
        g_all = spread(wide_rows, owners).reshape(owners * tok_rows, width + extra)
        router_rows = jnp.concatenate(
            [
                lax.dynamic_slice_in_dim(router_full, first_expert, local_experts, 1).T,
                jnp.zeros((side - local_experts, width), BF16),
            ],
            0,
        )
        d_partial, d_experts, d_router_local = ffn_backward(
            first_array, x_all, g_all, gate_up, expert_full[layer_no], router_rows,
            experts_total, in_rows,
        )
        d_experts = lax.psum_scatter(d_experts, "shard", scatter_dimension=0, tiled=True)[0]
        d_normed_two = collect(d_partial.reshape(owners, tok_rows, width))
        _, norm_back = jax.vjp(rms_scale, mixed, gain_pair[1])
        d_mixed_norm, d_gain_two = norm_back(d_normed_two)
        grad_mixed = grad_stream + d_mixed_norm
        d_att = grad_mixed.astype(BF16)
        d_w_out = inner_rows(attended, d_att)
        d_attended = (
            outer_cols(d_att, w_out_full).astype(BF16).reshape(tok_rows, KV_HEADS, groups, HEAD)
        )
        scores = (
            jnp.einsum("tngd,snd->ngts", queries, ext_keys, preferred_element_type=F32)
            * score_scale
        )
        prob_rows = jnp.exp(jnp.where(allowed, scores, masked_score) - log_total)
        d_probs = jnp.einsum("tngd,snd->ngts", d_attended, ext_values, preferred_element_type=F32)
        d_scores = (
            prob_rows * (d_probs - jnp.sum(prob_rows * d_probs, axis=-1, keepdims=True))
        ).astype(BF16)
        d_queries = (
            jnp.einsum("ngts,snd->tngd", d_scores, ext_keys, preferred_element_type=F32)
            * score_scale
        )
        d_keys = (
            jnp.einsum("ngts,tngd->snd", d_scores, queries, preferred_element_type=F32)
            * score_scale
        )
        d_values = jnp.einsum(
            "ngts,tngd->snd", prob_rows.astype(BF16), d_attended, preferred_element_type=F32
        )
        blocks = jnp.concatenate(
            [d_keys.reshape(key_count, kv_width), d_values.reshape(key_count, kv_width)], 1
        ).reshape(hop_count + 1, tok_rows, 2 * kv_width)
        carried = halo_back(blocks.astype(BF16), shards)
        d_qkv = jnp.concatenate([d_queries.reshape(tok_rows, q_width), carried], 1).astype(BF16)
        d_w_qkv = inner_rows(normed_one, d_qkv)
        d_normed_one = outer_cols(d_qkv, w_qkv_full)
        _, norm_back = jax.vjp(rms_scale, layer_input, gain_pair[0])
        d_input_norm, d_gain_one = norm_back(d_normed_one)
        grad_stream = grad_mixed + d_input_norm
        lanes = jnp.arange(experts_total, dtype=jnp.int32)
        d_router = jnp.where(
            (lanes >= first_expert) & (lanes < first_expert + local_experts),
            jnp.tile(d_router_local[:, :local_experts], (1, owners)),
            0.0,
        )
        dense_parts[layer_no] = [d_w_qkv.astype(BF16), d_w_out.astype(BF16)]
        small_parts[layer_no] = [
            d_router.astype(BF16),
            jnp.stack([d_gain_one, d_gain_two], 1).astype(BF16),
        ]
        collected[layer_no] = (
            d_experts[:, :in_rows, :].astype(F32),
            d_experts[:, in_rows:, :].astype(F32),
        )
    small = sum(small_parts, [])
    small.append(jnp.zeros((width, side - LAYERS * (experts_total + 2)), BF16))
    parts = sum(dense_parts, []) + [jnp.concatenate(small, 1)]
    d_dense = [part.reshape(shards, width // shards, -1) for part in parts]
    d_dense = reduce_dense(d_dense, shards, owners).astype(F32)
    for layer_no in range(LAYERS):
        at = layer_no * layer_columns
        d_main = d_dense[:, at : at + layer_columns]
        at = LAYERS * layer_columns + layer_no * (experts_total + 2)
        small = d_dense[:, at : at + experts_total + 2]
        collected[layer_no] = (
            small[:, experts_total:].T,
            d_main[:, :qkv_width],
            d_main[:, qkv_width:],
            small[:, :experts_total],
        ) + collected[layer_no]
    stacked = [
        jnp.stack([collected[layer_no][member] for layer_no in range(LAYERS)], 0)
        for member in range(6)
    ]
    results = [stream, grad_stream]
    results.extend(adam_update(gains, stacked[0], gains_first, gains_second))
    results.extend(adam_update(w_qkv, stacked[1], w_qkv_first, w_qkv_second))
    results.extend(adam_update(w_out, stacked[2], w_out_first, w_out_second))
    results.extend(adam_update(router, stacked[3], router_first, router_second))
    results.extend(adam_update(w_in, stacked[4], w_in_first, w_in_second))
    results.extend(adam_update(w_down, stacked[5], w_down_first, w_down_second))
    return tuple(results)


def solution(mesh):
    return jax.shard_map(
        on_device,
        mesh=mesh,
        in_specs=(
            P(("expert", "shard"), None),
            P(("expert", "shard"), None),
            P(),
            P(None, ("expert", "shard"), None),
            P(None, None, "shard"),
            P(None, None, "shard"),
            P(None, None, "shard"),
            P(None, "shard", None),
            P(None, "shard", None),
            P(None, "shard", None),
            P(None, "shard", None),
            P(None, "shard", None),
            P(None, "shard", None),
            P(None, "shard", None),
            P(None, "shard", None),
            P(None, "shard", None),
            P(None, "expert", "shard", None),
            P(None, "expert", "shard", None),
            P(None, "expert", "shard", None),
            P(None, "expert", "shard", None),
            P(None, "expert", "shard", None),
            P(None, "expert", "shard", None),
        ),
        out_specs=(
            P(("expert", "shard"), None),
            P(("expert", "shard"), None),
            P(None, None, "shard"),
            P(None, None, "shard"),
            P(None, None, "shard"),
            P(None, None, "shard"),
            P(None, "shard", None),
            P(None, "shard", None),
            P(None, "shard", None),
            P(None, "shard", None),
            P(None, "shard", None),
            P(None, "shard", None),
            P(None, "shard", None),
            P(None, "shard", None),
            P(None, "shard", None),
            P(None, "shard", None),
            P(None, "shard", None),
            P(None, "shard", None),
            P(None, "expert", "shard", None),
            P(None, "expert", "shard", None),
            P(None, "expert", "shard", None),
            P(None, "expert", "shard", None),
            P(None, "expert", "shard", None),
            P(None, "expert", "shard", None),
            P(None, "expert", "shard", None),
            P(None, "expert", "shard", None),
        ),
        check_vma=False,
    )
```

```python
import functools

import jax
import jax.numpy as jnp
from jax import lax
from jax.experimental import pallas as pl
from jax.experimental.pallas import tpu as pltpu
from jax.sharding import PartitionSpec as P

HEADS = 16
KV_HEADS = 8
HEAD = 64
TOP = 8
LAYERS = 2
WINDOW = 1024
SPAN = 8

norm_eps = 1e-05
masked_score = -1e30
beta_one = 0.9
beta_two = 0.95
adam_eps = 1e-08
learn_rate = 0.05
decay_rate = 0.1
adam_step = 10.0

F32 = jnp.float32
BF16 = jnp.bfloat16
MESH = pl.DeviceIdType.MESH
VMEM_LIMIT = 60 * 1024 * 1024


def rms_scale(values, gain_row):
    return (
        values * lax.rsqrt(jnp.mean(values * values, axis=-1, keepdims=True) + norm_eps) * gain_row
    )


def inner_rows(left_side, right_side):
    return lax.dot_general(
        left_side, right_side, (((0,), (0,)), ((), ())), preferred_element_type=F32
    )


def outer_cols(left_side, right_side):
    return lax.dot_general(
        left_side, right_side, (((1,), (1,)), ((), ())), preferred_element_type=F32
    )


def adam_update(weight, gradient, first_moment, second_moment):
    new_first = beta_one * first_moment + (1.0 - beta_one) * gradient
    new_second = beta_two * second_moment + (1.0 - beta_two) * gradient * gradient
    corr_first = new_first / (1.0 - beta_one**adam_step)
    corr_second = new_second / (1.0 - beta_two**adam_step)
    weight_step = -learn_rate * (
        corr_first / (jnp.sqrt(corr_second) + adam_eps) + decay_rate * weight
    )
    return [gradient, new_first, new_second, weight_step]


def signal(barrier, where):
    pl.semaphore_signal(barrier, inc=1, device_id=where, device_id_type=MESH)


def greet_chips(owners):
    e = lax.axis_index("expert")
    partner = e + 1 - 2 * lax.rem(e, 2)
    barrier = pltpu.get_barrier_semaphore()
    signal(barrier, {"expert": partner})
    for d in range(1, owners // 2):
        signal(barrier, {"expert": lax.rem(e + 2 * d, owners)})
    pl.semaphore_wait(barrier, owners // 2)
    return e, partner


def spread_kernel(owners, cuts, x_ref, o_ref, pair_send, pair_recv, far_send, far_recv):
    e, partner = greet_chips(owners)
    chips = owners // 2
    size = x_ref.shape[0] // cuts

    def pair_copy(d, cut):
        rows = pl.ds(cut * size, size)
        there = o_ref.at[lax.rem(e + owners - 2 * d, owners), rows]
        return pltpu.make_async_remote_copy(
            src_ref=x_ref.at[rows] if d == 0 else there,
            dst_ref=there,
            send_sem=pair_send.at[d, cut],
            recv_sem=pair_recv.at[d, cut],
            device_id={"expert": partner},
            device_id_type=MESH,
        )

    def far_copy(d, cut):
        rows = pl.ds(cut * size, size)
        return pltpu.make_async_remote_copy(
            src_ref=x_ref.at[rows],
            dst_ref=o_ref.at[e, rows],
            send_sem=far_send.at[d - 1, cut],
            recv_sem=far_recv.at[d - 1, cut],
            device_id={"expert": lax.rem(e + 2 * d, owners)},
            device_id_type=MESH,
        )

    for cut in range(cuts):
        for d in range(1, chips):
            far_copy(d, cut).start()
    for cut in range(cuts):
        pair_copy(0, cut).start()
    o_ref[e] = x_ref[...]
    for cut in range(cuts):
        for d in range(1, chips):
            far_copy(d, cut).wait_recv()
            pair_copy(d, cut).start()
    for cut in range(cuts):
        for d in range(chips):
            pair_copy(d, cut).wait()
        for d in range(1, chips):
            far_copy(d, cut).wait_send()


def spread(rows, owners, collective):
    dma = pltpu.SemaphoreType.DMA
    chips, cuts = owners // 2, 4
    return pl.pallas_call(
        functools.partial(spread_kernel, owners, cuts),
        out_shape=jax.ShapeDtypeStruct((owners,) + rows.shape, rows.dtype),
        in_specs=[pl.BlockSpec(memory_space=pltpu.VMEM)],
        out_specs=pl.BlockSpec(memory_space=pltpu.VMEM),
        scratch_shapes=[
            dma((chips, cuts)), dma((chips, cuts)), dma((chips - 1, cuts)), dma((chips - 1, cuts)),
        ],
        compiler_params=pltpu.CompilerParams(
            collective_id=collective, has_side_effects=True, vmem_limit_bytes=VMEM_LIMIT
        ),
        name="spread",
    )(rows)


def collect_kernel(
    owners, cuts, p_ref, o_ref, paired, going, came, pair_send, pair_recv, far_send, far_recv
):
    e, partner = greet_chips(owners)
    chips = owners // 2
    size = o_ref.shape[0] // cuts

    def pair_copy(d, cut):
        rows = pl.ds(cut * size, size)
        return pltpu.make_async_remote_copy(
            src_ref=p_ref.at[lax.rem(partner + 2 * d, owners), rows],
            dst_ref=paired.at[d, rows],
            send_sem=pair_send.at[d, cut],
            recv_sem=pair_recv.at[d, cut],
            device_id={"expert": partner},
            device_id_type=MESH,
        )

    def far_copy(d, cut):
        rows = pl.ds(cut * size, size)
        return pltpu.make_async_remote_copy(
            src_ref=going.at[d - 1, rows],
            dst_ref=came.at[d - 1, rows],
            send_sem=far_send.at[d - 1, cut],
            recv_sem=far_recv.at[d - 1, cut],
            device_id={"expert": lax.rem(e + 2 * d, owners)},
            device_id_type=MESH,
        )

    for cut in range(cuts):
        for d in range(1, chips):
            pair_copy(d, cut).start()
    for cut in range(cuts):
        pair_copy(0, cut).start()
    for cut in range(cuts):
        rows = pl.ds(cut * size, size)
        for d in range(1, chips):
            pair_copy(d, cut).wait_recv()
            going[d - 1, rows, :] = (
                p_ref[lax.rem(e + 2 * d, owners), rows, :].astype(F32)
                + paired[d, rows, :].astype(F32)
            ).astype(BF16)
            far_copy(d, cut).start()
    for cut in range(cuts):
        rows = pl.ds(cut * size, size)
        pair_copy(0, cut).wait_recv()
        total = p_ref[e, rows, :].astype(F32) + paired[0, rows, :].astype(F32)
        for d in range(1, chips):
            far_copy(d, cut).wait_recv()
            total = total + came[d - 1, rows, :].astype(F32)
        o_ref[rows, :] = total
    for cut in range(cuts):
        for d in range(chips):
            pair_copy(d, cut).wait_send()
        for d in range(1, chips):
            far_copy(d, cut).wait_send()


def collect(parts, collective):
    owners, rows, width = parts.shape
    dma = pltpu.SemaphoreType.DMA
    chips, cuts = owners // 2, 4
    return pl.pallas_call(
        functools.partial(collect_kernel, owners, cuts),
        out_shape=jax.ShapeDtypeStruct((rows, width), F32),
        in_specs=[pl.BlockSpec(memory_space=pltpu.VMEM)],
        out_specs=pl.BlockSpec(memory_space=pltpu.VMEM),
        scratch_shapes=[
            pltpu.VMEM((chips, rows, width), parts.dtype),
            pltpu.VMEM((chips - 1, rows, width), parts.dtype),
            pltpu.VMEM((chips - 1, rows, width), parts.dtype),
            dma((chips, cuts)), dma((chips, cuts)), dma((chips - 1, cuts)), dma((chips - 1, cuts)),
        ],
        compiler_params=pltpu.CompilerParams(
            collective_id=collective, has_side_effects=True, vmem_limit_bytes=VMEM_LIMIT
        ),
        name="collect",
    )(parts)


def ring_shard(place, count):
    back = lax.div(place, count // 2)
    return (1 - back) * 2 * place + back * (2 * (count - 1 - place) + 1)


def ring_place(shard, count):
    odd, pair = lax.rem(shard, 2), lax.div(shard, 2)
    return (1 - odd) * pair + odd * (count - 1 - pair)


def gather_dense_kernel(
    n, rows, x_ref, o_ref, ring_send, ring_recv, pair_send, pair_recv, own_sem
):
    e, s = lax.axis_index("expert"), lax.axis_index("shard")
    core = lax.rem(e, 2)
    partner = e + 1 - 2 * core
    p = ring_place(s, n)
    ways = (ring_shard(lax.rem(p + 1, n), n), ring_shard(lax.rem(p + n - 1, n), n))
    barrier = pltpu.get_barrier_semaphore()
    signal(barrier, {"expert": partner})
    signal(barrier, {"shard": ways[0]})
    signal(barrier, {"shard": ways[1]})
    pl.semaphore_wait(barrier, 3)
    quarter = rows // 4

    def part(side, way):
        return pl.ds(pl.multiple_of(side * 2 * quarter + way * quarter, quarter), quarter)

    def block(way, k):
        return ring_shard(lax.rem(p + (n - k if way == 0 else k), n), n)

    def ring_copy(way, k, src):
        return pltpu.make_async_remote_copy(
            src_ref=src,
            dst_ref=o_ref.at[block(way, k), part(core, way)],
            send_sem=ring_send.at[way, k],
            recv_sem=ring_recv.at[way, k],
            device_id={"shard": ways[way]},
            device_id_type=MESH,
        )

    def pair_copy(way, k, side):
        there = o_ref.at[block(way, k), part(side, way)]
        return pltpu.make_async_remote_copy(
            src_ref=there,
            dst_ref=there,
            send_sem=pair_send.at[way, k - 1],
            recv_sem=pair_recv.at[way, k - 1],
            device_id={"expert": partner},
            device_id_type=MESH,
        )

    for way in range(2):
        ring_copy(way, 0, x_ref.at[part(core, way)]).start()
    own = pltpu.make_async_copy(x_ref, o_ref.at[s], own_sem)
    own.start()

    def step(k, carry):
        for way in range(2):
            came = o_ref.at[block(way, k), part(core, way)]
            pltpu.make_async_remote_copy(
                src_ref=came,
                dst_ref=came,
                send_sem=ring_send.at[way, k - 1],
                recv_sem=ring_recv.at[way, k - 1],
                device_id={"shard": ways[way]},
                device_id_type=MESH,
            ).wait_recv()

            @pl.when(k < n - 1)
            def _():
                ring_copy(way, k, came).start()

            pair_copy(way, k, core).start()
        return carry

    lax.fori_loop(1, n, step, 0)

    def finish(k, carry):
        for way in range(2):
            ring_copy(way, k - 1, x_ref.at[part(core, way)]).wait_send()
            pair_copy(way, k, core).wait_send()
            pair_copy(way, k, 1 - core).wait_recv()
        return carry

    lax.fori_loop(1, n, finish, 0)
    own.wait()


def gather_dense(piece, n):
    rows, columns = piece.shape
    dma = pltpu.SemaphoreType.DMA
    return pl.pallas_call(
        functools.partial(gather_dense_kernel, n, rows),
        out_shape=jax.ShapeDtypeStruct((n, rows, columns), piece.dtype),
        in_specs=[pl.BlockSpec(memory_space=pltpu.VMEM)],
        out_specs=pl.BlockSpec(memory_space=pl.ANY),
        scratch_shapes=[
            dma((2, n - 1)), dma((2, n - 1)), dma((2, n - 1)), dma((2, n - 1)), dma,
        ],
        compiler_params=pltpu.CompilerParams(
            collective_id=3, has_side_effects=True, vmem_limit_bytes=VMEM_LIMIT
        ),
        name="gather_dense",
    )(piece)


def reduce_dense_kernel(
    n, owners, rows, places, *refs,
):
    g_refs = refs[: len(places)]
    (
        o_ref, paired, came, going, crossed, last_in, pair_send, pair_recv, ring_send,
        ring_recv, cross_send, cross_recv, last_send, last_recv,
    ) = refs[len(places) :]
    e, s = lax.axis_index("expert"), lax.axis_index("shard")
    core, x = lax.rem(e, 2), lax.div(e, 2)
    partner = e + 1 - 2 * core
    columns = owners // 2
    p = ring_place(s, n)
    ways = (ring_shard(lax.rem(p + 1, n), n), ring_shard(lax.rem(p + n - 1, n), n))
    barrier = pltpu.get_barrier_semaphore()
    signal(barrier, {"expert": partner})
    signal(barrier, {"shard": ways[0]})
    signal(barrier, {"shard": ways[1]})
    for d in range(1, columns):
        signal(barrier, {"expert": lax.rem(e + 2 * d, owners)})
    pl.semaphore_wait(barrier, 3 + columns - 1)
    half, quarter = rows // 2, rows // 4

    def mine(way):
        return pl.ds(pl.multiple_of(core * half + way * quarter, quarter), quarter)

    def block(way, k):
        return ring_shard(lax.rem(p + (2 * n - 1 - k if way == 0 else k + 1), n), n)

    def pair_copy(k, i):
        b = block(0, k)
        at, wide = places[i]
        return pltpu.make_async_remote_copy(
            src_ref=g_refs[i].at[b, pl.ds(pl.multiple_of((1 - core) * half, half), half)],
            dst_ref=paired.at[b, :, pl.ds(at, wide)],
            send_sem=pair_send.at[i, b],
            recv_sem=pair_recv.at[i, b],
            device_id={"expert": partner},
            device_id_type=MESH,
        )

    def ring_copy(way, k):
        return pltpu.make_async_remote_copy(
            src_ref=going.at[way, k],
            dst_ref=came.at[way, k],
            send_sem=ring_send.at[way, k],
            recv_sem=ring_recv.at[way, k],
            device_id={"shard": ways[way]},
            device_id_type=MESH,
        )

    def put(target, way, b, more=None):
        for g_ref, (at, wide) in zip(g_refs, places):
            total = g_ref[b, mine(way), :].astype(F32) + paired[
                b, way * quarter : (way + 1) * quarter, at : at + wide
            ].astype(F32)
            if more is not None:
                total = total + more[:, at : at + wide].astype(F32)
            target[:, at : at + wide] = total.astype(BF16)

    order = []
    for k in range(n):
        for place in (k, n - 2 - k):
            place = place % n
            if place not in order:
                order.append(place)
    every = range(len(places))
    for k in order:
        for i in every:
            pair_copy(k, i).start()
    for k in order[:2]:
        for i in every:
            pair_copy(k, i).wait_recv()
    for way in range(2):
        put(going.at[way, 0], way, block(way, 0))
        ring_copy(way, 0).start()
    for k in order[2:]:
        for i in every:
            pair_copy(k, i).wait_recv()

    def step(k, carry):
        for way in range(2):
            ring_copy(way, k - 1).wait_recv()
            put(going.at[way, k], way, block(way, k), came.at[way, k - 1])
            ring_copy(way, k).start()
        return carry

    lax.fori_loop(1, n - 1, step, 0)
    for way in range(2):
        ring_copy(way, n - 2).wait_recv()
        put(
            crossed.at[x, pl.ds(way * quarter, quarter)], way, s, came.at[way, n - 2]
        )

    def cross_copy(d):
        return pltpu.make_async_remote_copy(
            src_ref=crossed.at[x],
            dst_ref=crossed.at[x],
            send_sem=cross_send.at[d - 1],
            recv_sem=cross_recv.at[d - 1],
            device_id={"expert": lax.rem(e + 2 * d, owners)},
            device_id_type=MESH,
        )

    for d in range(1, columns):
        cross_copy(d).start()
    for d in range(1, columns):
        cross_copy(d).wait()
    total = crossed[0].astype(F32)
    for d in range(1, columns):
        total = total + crossed[d].astype(F32)
    here = pl.ds(pl.multiple_of(core * half, half), half)
    o_ref[here, :] = total.astype(BF16)
    last = pltpu.make_async_remote_copy(
        src_ref=o_ref.at[here],
        dst_ref=last_in,
        send_sem=last_send,
        recv_sem=last_recv,
        device_id={"expert": partner},
        device_id_type=MESH,
    )
    last.start()
    for k in order:
        for i in every:
            pair_copy(k, i).wait_send()

    def finish(k, carry):
        for way in range(2):
            ring_copy(way, k).wait_send()
        return carry

    lax.fori_loop(0, n - 1, finish, 0)
    last.wait()
    o_ref[pl.ds(pl.multiple_of((1 - core) * half, half), half), :] = last_in[...]


def reduce_dense(grads, n, owners):
    rows = grads[0].shape[1]
    places, columns = [], 0
    for grad in grads:
        places.append((columns, grad.shape[2]))
        columns += grad.shape[2]
    dma = pltpu.SemaphoreType.DMA
    across = owners // 2
    return pl.pallas_call(
        functools.partial(reduce_dense_kernel, n, owners, rows, tuple(places)),
        out_shape=jax.ShapeDtypeStruct((rows, columns), BF16),
        in_specs=[pl.BlockSpec(memory_space=pltpu.VMEM)] * len(places),
        out_specs=pl.BlockSpec(memory_space=pltpu.VMEM),
        scratch_shapes=[
            pltpu.VMEM((n, rows // 2, columns), BF16),
            pltpu.VMEM((2, n - 1, rows // 4, columns), BF16),
            pltpu.VMEM((2, n - 1, rows // 4, columns), BF16),
            pltpu.VMEM((across, rows // 2, columns), BF16),
            pltpu.VMEM((rows // 2, columns), BF16),
            dma((len(places), n)), dma((len(places), n)), dma((2, n - 1)), dma((2, n - 1)),
            dma((across - 1,)), dma((across - 1,)), dma, dma,
        ],
        compiler_params=pltpu.CompilerParams(
            collective_id=4, has_side_effects=True, vmem_limit_bytes=VMEM_LIMIT
        ),
        name="reduce_dense",
    )(*grads)


def halo_links(n, s):
    odd = lax.rem(s, 2)
    return odd, s + 1 - 2 * odd, s + 2 < n, s >= 2


def halo_barrier(s, odd, mate, ahead, behind, sends_back):
    barrier = pltpu.get_barrier_semaphore()
    even = odd == 0
    to_ahead, to_behind = (ahead, behind) if not sends_back else (behind, ahead)
    step = -2 if not sends_back else 2
    mate_copies = (odd == 1) | behind if not sends_back else even | behind
    to_mate = even | behind if not sends_back else (odd == 1) | behind

    @pl.when(to_behind)
    def _():
        signal(barrier, {"shard": s + step})

    @pl.when(mate_copies)
    def _():
        signal(barrier, {"shard": mate})

    @pl.when(to_ahead & to_mate)
    def _():
        pl.semaphore_wait(barrier, 2)

    @pl.when(to_ahead != to_mate)
    def _():
        pl.semaphore_wait(barrier, 1)


def halo_kernel(n, rows, cuts, kv_ref, o_ref, sends, recvs, own_sem):
    s = lax.axis_index("shard")
    odd, mate, ahead, behind = halo_links(n, s)
    even = odd == 0
    size = rows // cuts

    def copy(kind, cut, src, slot, where):
        return pltpu.make_async_remote_copy(
            src_ref=src.at[pl.ds(cut * size, size)],
            dst_ref=o_ref.at[slot, pl.ds(cut * size, size)],
            send_sem=sends.at[kind, cut],
            recv_sem=recvs.at[kind, cut],
            device_id={"shard": where},
            device_id_type=MESH,
        )

    halo_barrier(s, odd, mate, ahead, behind, False)
    from_odd = (o_ref.at[2], o_ref.at[0])
    from_even = (kv_ref, o_ref.at[2])
    for cut in range(cuts):

        @pl.when(ahead)
        def _():
            copy(0, cut, kv_ref, 2, s + 2).start()

        @pl.when(even)
        def _():
            copy(2, cut, kv_ref, 3, mate).start()

    o_ref[4] = kv_ref[...]
    for slot in range(4):

        @pl.when(s < 4 - slot)
        def _():
            o_ref[slot] = jnp.zeros_like(o_ref[slot])

    for cut in range(cuts):

        @pl.when(behind)
        def _():
            copy(0, cut, kv_ref, 2, s).wait_recv()

        @pl.when(behind & ahead)
        def _():
            copy(1, cut, o_ref.at[2], 0, s + 2).start()

        @pl.when(behind & (odd == 1))
        def _():
            copy(2, cut, from_odd[0], 3, mate).start()

        @pl.when(behind & even)
        def _():
            copy(3, cut, from_even[1], 1, mate).start()

    for cut in range(cuts):

        @pl.when(s >= 4)
        def _():
            copy(1, cut, o_ref.at[2], 0, s).wait_recv()

        @pl.when((s >= 4) & (odd == 1))
        def _():
            copy(3, cut, from_odd[1], 1, mate).start()

    for cut in range(cuts):

        @pl.when(s >= 1)
        def _():
            copy(2, cut, kv_ref, 3, mate).wait_recv()

        @pl.when(s >= 3)
        def _():
            copy(3, cut, kv_ref, 1, mate).wait_recv()

        @pl.when(ahead)
        def _():
            copy(0, cut, kv_ref, 2, s).wait_send()

        @pl.when(behind & ahead)
        def _():
            copy(1, cut, kv_ref, 0, s).wait_send()

        @pl.when(even | behind)
        def _():
            copy(2, cut, kv_ref, 3, mate).wait_send()

        @pl.when((even & behind) | ((odd == 1) & (s >= 4)))
        def _():
            copy(3, cut, kv_ref, 1, mate).wait_send()


def halo(kv, n, slots):
    rows, columns = kv.shape
    dma = pltpu.SemaphoreType.DMA
    cuts = 2
    return pl.pallas_call(
        functools.partial(halo_kernel, n, rows, cuts),
        out_shape=jax.ShapeDtypeStruct((slots, rows, columns), kv.dtype),
        in_specs=[pl.BlockSpec(memory_space=pltpu.VMEM)],
        out_specs=pl.BlockSpec(memory_space=pltpu.VMEM),
        scratch_shapes=[dma((4, cuts)), dma((4, cuts)), dma],
        compiler_params=pltpu.CompilerParams(
            collective_id=5, has_side_effects=True, vmem_limit_bytes=VMEM_LIMIT
        ),
        name="halo",
    )(kv)


def halo_back_kernel(n, rows, cuts, g_ref, o_ref, own, came, sends, recvs):
    s = lax.axis_index("shard")
    odd, mate, ahead, behind = halo_links(n, s)
    even = odd == 0
    size = rows // cuts

    def copy(kind, cut, src, where):
        return pltpu.make_async_remote_copy(
            src_ref=src.at[pl.ds(cut * size, size)],
            dst_ref=came.at[kind, pl.ds(cut * size, size)],
            send_sem=sends.at[kind, cut],
            recv_sem=recvs.at[kind, cut],
            device_id={"shard": where},
            device_id_type=MESH,
        )

    def there(ref, cut, value=None):
        here = pl.ds(cut * size, size)
        return ref[here, :].astype(F32)

    halo_barrier(s, odd, mate, ahead, behind, True)
    for cut in range(cuts):

        @pl.when(s >= 3)
        def _():
            copy(3, cut, g_ref.at[1], mate).start()

        @pl.when(s >= 1)
        def _():
            copy(2, cut, g_ref.at[3], mate).start()

    for cut in range(cuts):
        here = pl.ds(cut * size, size)

        @pl.when((odd == 1) & (s >= 4))
        def _():
            copy(3, cut, g_ref.at[1], mate).wait_recv()
            own[0, here, :] = (there(g_ref.at[0], cut) + there(came.at[3], cut)).astype(BF16)

        @pl.when((odd == 1) & (s >= 4))
        def _():
            copy(1, cut, own.at[0], s - 2).start()

        @pl.when(even & (s >= 4))
        def _():
            copy(1, cut, g_ref.at[0], s - 2).start()

    for cut in range(cuts):
        here = pl.ds(cut * size, size)

        @pl.when((odd == 1) & behind)
        def _():
            copy(2, cut, g_ref.at[3], mate).wait_recv()
            own[1, here, :] = (there(g_ref.at[2], cut) + there(came.at[2], cut)).astype(BF16)

        @pl.when(even & behind)
        def _():
            copy(3, cut, g_ref.at[1], mate).wait_recv()
            own[1, here, :] = (there(g_ref.at[2], cut) + there(came.at[3], cut)).astype(BF16)

        @pl.when(behind & ahead)
        def _():
            copy(1, cut, g_ref.at[0], s).wait_recv()
            own[1, here, :] = (there(own.at[1], cut) + there(came.at[1], cut)).astype(BF16)

        @pl.when(behind)
        def _():
            copy(0, cut, own.at[1], s - 2).start()

    for cut in range(cuts):
        here = pl.ds(cut * size, size)
        o_ref[here, :] = there(g_ref.at[4], cut)

        @pl.when(even)
        def _():
            copy(2, cut, g_ref.at[3], mate).wait_recv()
            o_ref[here, :] += there(came.at[2], cut)

        @pl.when(ahead)
        def _():
            copy(0, cut, own.at[1], s).wait_recv()
            o_ref[here, :] += there(came.at[0], cut)

        @pl.when(s >= 3)
        def _():
            copy(3, cut, g_ref.at[1], mate).wait_send()

        @pl.when(s >= 1)
        def _():
            copy(2, cut, g_ref.at[3], mate).wait_send()

        @pl.when(s >= 4)
        def _():
            copy(1, cut, g_ref.at[0], mate).wait_send()

        @pl.when(behind)
        def _():
            copy(0, cut, own.at[1], mate).wait_send()


def halo_back(grads, n):
    slots, rows, columns = grads.shape
    dma = pltpu.SemaphoreType.DMA
    cuts = 2
    return pl.pallas_call(
        functools.partial(halo_back_kernel, n, rows, cuts),
        out_shape=jax.ShapeDtypeStruct((rows, columns), F32),
        in_specs=[pl.BlockSpec(memory_space=pltpu.VMEM)],
        out_specs=pl.BlockSpec(memory_space=pltpu.VMEM),
        scratch_shapes=[
            pltpu.VMEM((3, rows, columns), BF16),
            pltpu.VMEM((4, rows, columns), BF16),
            dma((4, cuts)),
            dma((4, cuts)),
        ],
        compiler_params=pltpu.CompilerParams(
            collective_id=6, has_side_effects=True, vmem_limit_bytes=VMEM_LIMIT
        ),
        name="halo_back",
    )(grads)


def column_of(extra, index, experts_total):
    lanes = lax.broadcasted_iota(jnp.int32, extra.shape, 1)
    hit = (lanes == index) | (lanes == index + experts_total)
    return jnp.sum(jnp.where(hit, extra.astype(F32), 0.0), axis=1, keepdims=True)


def ffn_forward_kernel(
    tile, width, in_rows, experts_total, first_ref, x_ref, w_ref, part_ref, gate_up_ref, acc
):
    e = pl.program_id(0)
    w_in = w_ref[:, 0, :in_rows, :].reshape(width, w_ref.shape[-1])
    w_down = w_ref[:, 0, in_rows:, :].reshape(-1, width)
    half = w_in.shape[1] // 2
    index = first_ref[0] + e
    count = x_ref.shape[0] // tile
    for t in range(count):
        rows = pl.ds(t * tile, tile)
        gate_up = jnp.dot(x_ref[rows, :width], w_in, preferred_element_type=F32)
        gate, up = gate_up[:, :half], gate_up[:, half:]
        gate_up_ref[0, rows, :] = gate_up.astype(BF16)
        weight = column_of(x_ref[rows, width:], index, experts_total)
        hidden = (gate * jax.nn.sigmoid(gate) * up * weight).astype(BF16)
        out = jnp.dot(hidden, w_down, preferred_element_type=F32)

        @pl.when(e == 0)
        def _():
            acc[rows, :] = out

        @pl.when(e > 0)
        def _():
            acc[rows, :] += out

        @pl.when(e == pl.num_programs(0) - 1)
        def _():
            part_ref[rows, :] = acc[rows, :].astype(BF16)


def ffn_forward(first, x_all, w_all, experts_total, in_rows):
    shards, local, piece, inner = w_all.shape
    tokens, wide = x_all.shape
    width = in_rows * shards
    return pl.pallas_call(
        functools.partial(ffn_forward_kernel, 256, width, in_rows, experts_total),
        grid_spec=pltpu.PrefetchScalarGridSpec(
            num_scalar_prefetch=1,
            grid=(local,),
            in_specs=[
                pl.BlockSpec((tokens, wide), lambda e, f: (0, 0)),
                pl.BlockSpec((shards, 1, piece, inner), lambda e, f: (0, e, 0, 0)),
            ],
            out_specs=[
                pl.BlockSpec((tokens, width), lambda e, f: (0, 0)),
                pl.BlockSpec((1, tokens, inner), lambda e, f: (e, 0, 0)),
            ],
            scratch_shapes=[pltpu.VMEM((tokens, width), F32)],
        ),
        out_shape=[
            jax.ShapeDtypeStruct((tokens, width), BF16),
            jax.ShapeDtypeStruct((local, tokens, inner), BF16),
        ],
        compiler_params=pltpu.CompilerParams(vmem_limit_bytes=VMEM_LIMIT),
        cost_estimate=pl.CostEstimate(
            flops=2 * local * tokens * width * (inner + inner // 2),
            bytes_accessed=2 * (w_all.size + local * tokens * inner + 2 * tokens * wide),
            transcendentals=0,
        ),
        name="ffn_forward",
    )(first, x_all, w_all)


def ffn_backward_kernel(
    tile,
    width,
    in_rows,
    experts_total,
    first_ref,
    x_ref,
    g_ref,
    gate_up_ref,
    w_ref,
    part_ref,
    grad_ref,
    acc,
    d_gate_up,
    hidden_all,
    d_weights,
):
    e = pl.program_id(0)
    inner = w_ref.shape[-1]
    w_in = w_ref[:, 0, :in_rows, :].reshape(width, inner)
    w_down = w_ref[:, 0, in_rows:, :].reshape(-1, width)
    half = inner // 2
    index = first_ref[0] + e
    tokens = x_ref.shape[0]
    last = pl.num_programs(0) - 1
    for t in range(tokens // tile):
        rows = pl.ds(t * tile, tile)
        d_plain = outer_cols(g_ref[rows, :], w_down)
        gate = gate_up_ref[0, rows, :half].astype(F32)
        up = gate_up_ref[0, rows, half:].astype(F32)
        weight = column_of(x_ref[rows, width:], index, experts_total)
        sig = jax.nn.sigmoid(gate)
        silu = gate * sig
        hidden = silu * up
        d_weight = jnp.sum(hidden * d_plain, axis=1, keepdims=True)
        d_hidden = d_plain * weight
        hidden_all[rows, :] = (hidden * weight).astype(BF16)
        d_gate_up[rows, :half] = (d_hidden * up * sig * (1.0 + gate * (1.0 - sig))).astype(BF16)
        d_gate_up[rows, half:] = (d_hidden * silu).astype(BF16)
        lanes = lax.broadcasted_iota(jnp.int32, (tile, d_weights.shape[1]), 1)
        high = d_weight.astype(BF16).astype(F32)
        columns = jnp.where(
            lanes == index, high, jnp.where(lanes == index + experts_total, d_weight - high, 0.0)
        )
        out = outer_cols(d_gate_up[rows, :], w_in)

        @pl.when(e == 0)
        def _():
            acc[rows, :] = out
            d_weights[rows, :] = columns

        @pl.when(e > 0)
        def _():
            acc[rows, :] += out
            d_weights[rows, :] += columns

        @pl.when(e == last)
        def _():
            part_ref[rows, :width] = acc[rows, :].astype(BF16)
            part_ref[rows, width:] = d_weights[rows, :].astype(BF16)

    grad_ref[:, 0, :in_rows, :] = (
        inner_rows(x_ref[:, :width], d_gate_up[...]).astype(BF16).reshape(-1, in_rows, inner)
    )
    grad_ref[:, 0, in_rows:, :] = (
        inner_rows(hidden_all[...], g_ref[...])
        .astype(BF16)
        .reshape(-1, w_ref.shape[2] - in_rows, width)
    )


def ffn_backward(first, x_all, g_all, gate_up, w_all, experts_total, in_rows):
    shards, local, piece, inner = w_all.shape
    tokens, wide = x_all.shape
    width = in_rows * shards
    return pl.pallas_call(
        functools.partial(ffn_backward_kernel, 256, width, in_rows, experts_total),
        grid_spec=pltpu.PrefetchScalarGridSpec(
            num_scalar_prefetch=1,
            grid=(local,),
            in_specs=[
                pl.BlockSpec((tokens, wide), lambda e, f: (0, 0)),
                pl.BlockSpec((tokens, width), lambda e, f: (0, 0)),
                pl.BlockSpec((1, tokens, inner), lambda e, f: (e, 0, 0)),
                pl.BlockSpec((shards, 1, piece, inner), lambda e, f: (0, e, 0, 0)),
            ],
            out_specs=[
                pl.BlockSpec((tokens, wide), lambda e, f: (0, 0)),
                pl.BlockSpec((shards, 1, piece, inner), lambda e, f: (0, e, 0, 0)),
            ],
            scratch_shapes=[
                pltpu.VMEM((tokens, width), F32),
                pltpu.VMEM((tokens, inner), BF16),
                pltpu.VMEM((tokens, inner // 2), BF16),
                pltpu.VMEM((tokens, wide - width), F32),
            ],
        ),
        out_shape=[
            jax.ShapeDtypeStruct((tokens, wide), BF16),
            jax.ShapeDtypeStruct(w_all.shape, BF16),
        ],
        compiler_params=pltpu.CompilerParams(vmem_limit_bytes=VMEM_LIMIT),
        cost_estimate=pl.CostEstimate(
            flops=4 * local * tokens * width * (inner + inner // 2),
            bytes_accessed=2 * (2 * w_all.size + local * tokens * inner + 4 * tokens * wide),
            transcendentals=0,
        ),
        name="ffn_backward",
    )(first, x_all, g_all, gate_up, w_all)


def on_device(
    hidden_in,
    cotangent,
    doc_lengths,
    routes,
    gains,
    gains_first,
    gains_second,
    w_qkv,
    w_qkv_first,
    w_qkv_second,
    w_out,
    w_out_first,
    w_out_second,
    router,
    router_first,
    router_second,
    w_in,
    w_in_first,
    w_in_second,
    w_down,
    w_down_first,
    w_down_second,
):
    tok_rows, width = hidden_in.shape
    owners = lax.axis_size("expert")
    shards = lax.axis_size("shard")
    local_experts = w_in.shape[1]
    in_rows = w_in.shape[2]
    experts_total = local_experts * owners
    seq_len = tok_rows * SPAN
    hop_count = min(-(-WINDOW // tok_rows), SPAN - 1)
    key_count = (hop_count + 1) * tok_rows
    q_width = HEADS * HEAD
    kv_width = KV_HEADS * HEAD
    qkv_width = q_width + 2 * kv_width
    groups = HEADS // KV_HEADS
    score_scale = HEAD ** (-0.5)
    extra = -(-2 * experts_total // 128) * 128
    my_owner = lax.axis_index("expert")
    first_expert = my_owner * local_experts
    first_array = first_expert.astype(jnp.int32).reshape(1)
    row_start = (my_owner * shards + lax.axis_index("shard")) * tok_rows
    my_seq = row_start // seq_len
    doc_ends = jnp.cumsum(lax.dynamic_slice_in_dim(doc_lengths, my_seq, 1, 0)[0])
    query_rows = row_start + jnp.arange(tok_rows, dtype=jnp.int32)
    key_rows = row_start - hop_count * tok_rows + jnp.arange(key_count, dtype=jnp.int32)
    query_docs = jnp.sum(
        (query_rows[:, None] % seq_len >= doc_ends[None, :]).astype(jnp.int32), axis=1
    )
    key_docs = jnp.sum((key_rows[:, None] % seq_len >= doc_ends[None, :]).astype(jnp.int32), axis=1)
    distance = query_rows[:, None] - key_rows[None, :]
    allowed = (
        (query_rows[:, None] // seq_len == key_rows[None, :] // seq_len)
        & (query_docs[:, None] == key_docs[None, :])
        & (distance >= 0)
        & (distance < WINDOW)
    )
    expert_ids = jnp.arange(experts_total, dtype=jnp.int32)
    side = 128

    def dense_piece():
        rows = w_qkv.shape[1]
        parts = []
        for layer_no in range(LAYERS):
            parts += [w_qkv[layer_no].astype(BF16), w_out[layer_no].astype(BF16)]
        for layer_no in range(LAYERS):
            parts += [router[layer_no].astype(BF16), gains[layer_no].T.astype(BF16)]
        parts.append(jnp.zeros((rows, side - LAYERS * (experts_total + 2)), BF16))
        return jnp.concatenate(parts, 1)

    def expert_piece(layer_no):
        return jnp.concatenate(
            [w_in[layer_no].astype(BF16), w_down[layer_no].astype(BF16)], 1
        )

    layer_columns = qkv_width + width
    expert_full = []
    for layer_no in range(LAYERS):
        expert_full.append(
            lax.all_gather(expert_piece(layer_no), "shard", axis=0, tiled=False)
        )
    dense = gather_dense(dense_piece(), shards).reshape(width, -1)

    kept_layers = []
    stream = hidden_in
    for layer_no in range(LAYERS):
        at = layer_no * layer_columns
        w_qkv_full = dense[:, at : at + qkv_width]
        w_out_full = dense[:, at + qkv_width : at + layer_columns]
        at = LAYERS * layer_columns + layer_no * (experts_total + 2)
        small = dense[:, at : at + experts_total + 2]
        router_full = small[:, :experts_total]
        gain_pair = small[:, experts_total : experts_total + 2].astype(F32).T
        normed_one = rms_scale(stream, gain_pair[0]).astype(BF16)
        qkv_rows = jnp.dot(normed_one, w_qkv_full, preferred_element_type=F32).astype(BF16)
        queries = qkv_rows[:, :q_width].reshape(tok_rows, KV_HEADS, groups, HEAD)
        ext = halo(qkv_rows[:, q_width:], shards, hop_count + 1).reshape(key_count, 2 * kv_width)
        ext_keys = ext[:, :kv_width].reshape(key_count, KV_HEADS, HEAD)
        ext_values = ext[:, kv_width:].reshape(key_count, KV_HEADS, HEAD)
        scores = (
            jnp.einsum("tngd,snd->ngts", queries, ext_keys, preferred_element_type=F32)
            * score_scale
        )
        masked = jnp.where(allowed, scores, masked_score)
        row_top = jnp.max(masked, axis=-1, keepdims=True)
        log_total = row_top + jnp.log(jnp.sum(jnp.exp(masked - row_top), axis=-1, keepdims=True))
        prob_rows = jnp.exp(masked - log_total).astype(BF16)
        attended = (
            jnp.einsum("ngts,snd->tngd", prob_rows, ext_values, preferred_element_type=F32)
            .astype(BF16)
            .reshape(tok_rows, q_width)
        )
        mixed = stream + jnp.dot(attended, w_out_full, preferred_element_type=F32)
        normed_two = rms_scale(mixed, gain_pair[1]).astype(BF16)
        logits = jnp.dot(normed_two, router_full, preferred_element_type=F32)
        named = jnp.any(routes[layer_no][:, :, None] == expert_ids[None, None, :], axis=1)
        top_logit = jnp.max(jnp.where(named, logits, -jnp.inf), axis=1, keepdims=True)
        powers = jnp.where(named, jnp.exp(jnp.where(named, logits - top_logit, 0.0)), 0.0)
        weights = powers / jnp.sum(powers, axis=1, keepdims=True)
        high = weights.astype(BF16)
        low = (weights - high.astype(F32)).astype(BF16)
        wide_rows = jnp.concatenate(
            [normed_two, high, low, jnp.zeros((tok_rows, extra - 2 * experts_total), BF16)], 1
        )
        x_all = spread(wide_rows, owners, 1).reshape(owners * tok_rows, width + extra)
        if layer_no + 1 == LAYERS:
            g_rows, x_all = lax.optimization_barrier((cotangent.astype(BF16), x_all))
            g_all = spread(g_rows, owners, 8).reshape(owners * tok_rows, width)
            g_all, x_all = lax.optimization_barrier((g_all, x_all))
        partial, gate_up = ffn_forward(
            first_array, x_all, expert_full[layer_no], experts_total, in_rows
        )
        if layer_no + 1 == LAYERS:
            d_partial, d_experts = ffn_backward(
                first_array, x_all, g_all, gate_up, expert_full[layer_no], experts_total, in_rows
            )
            partial, d_partial = lax.optimization_barrier((partial, d_partial))
        moe_out = collect(partial.reshape(owners, tok_rows, width), 2)
        kept_layers.append(
            (
                stream, normed_one, queries, ext_keys, ext_values, log_total, attended, mixed,
                x_all, gate_up, normed_two, weights, w_qkv_full, w_out_full, router_full,
                gain_pair,
            )
        )
        stream = mixed + moe_out
    grad_stream = cotangent
    collected = [None] * LAYERS
    dense_parts = [None] * LAYERS
    small_parts = [None] * LAYERS
    for layer_no in reversed(range(LAYERS)):
        (
            layer_input, normed_one, queries, ext_keys, ext_values, log_total, attended, mixed,
            x_all, gate_up, normed_two, weights, w_qkv_full, w_out_full, router_full,
            gain_pair,
        ) = kept_layers[layer_no]
        if layer_no + 1 < LAYERS:
            g_all = spread(grad_stream.astype(BF16), owners, 8).reshape(owners * tok_rows, width)
            d_partial, d_experts = ffn_backward(
                first_array, x_all, g_all, gate_up, expert_full[layer_no], experts_total, in_rows
            )
        d_experts = lax.psum_scatter(d_experts, "shard", scatter_dimension=0, tiled=True)[0]
        d_all = collect(d_partial.reshape(owners, tok_rows, -1), 7)
        d_weights = (
            d_all[:, width : width + experts_total]
            + d_all[:, width + experts_total : width + 2 * experts_total]
        )
        mean_d = jnp.sum(weights * d_weights, axis=1, keepdims=True)
        d_logits = (weights * (d_weights - mean_d)).astype(BF16)
        d_router = inner_rows(normed_two, d_logits)
        d_normed_two = d_all[:, :width] + outer_cols(d_logits, router_full)
        _, norm_back = jax.vjp(rms_scale, mixed, gain_pair[1])
        d_mixed_norm, d_gain_two = norm_back(d_normed_two)
        grad_mixed = grad_stream + d_mixed_norm
        d_att = grad_mixed.astype(BF16)
        d_w_out = inner_rows(attended, d_att)
        d_attended = (
            outer_cols(d_att, w_out_full).astype(BF16).reshape(tok_rows, KV_HEADS, groups, HEAD)
        )
        scores = (
            jnp.einsum("tngd,snd->ngts", queries, ext_keys, preferred_element_type=F32)
            * score_scale
        )
        prob_rows = jnp.exp(jnp.where(allowed, scores, masked_score) - log_total)
        d_probs = jnp.einsum("tngd,snd->ngts", d_attended, ext_values, preferred_element_type=F32)
        d_scores = (
            prob_rows * (d_probs - jnp.sum(prob_rows * d_probs, axis=-1, keepdims=True))
        ).astype(BF16)
        d_queries = (
            jnp.einsum("ngts,snd->tngd", d_scores, ext_keys, preferred_element_type=F32)
            * score_scale
        )
        d_keys = (
            jnp.einsum("ngts,tngd->snd", d_scores, queries, preferred_element_type=F32)
            * score_scale
        )
        d_values = jnp.einsum(
            "ngts,tngd->snd", prob_rows.astype(BF16), d_attended, preferred_element_type=F32
        )
        blocks = jnp.concatenate(
            [d_keys.reshape(key_count, kv_width), d_values.reshape(key_count, kv_width)], 1
        ).reshape(hop_count + 1, tok_rows, 2 * kv_width)
        carried = halo_back(blocks.astype(BF16), shards)
        d_qkv = jnp.concatenate([d_queries.reshape(tok_rows, q_width), carried], 1).astype(BF16)
        d_w_qkv = inner_rows(normed_one, d_qkv)
        d_normed_one = outer_cols(d_qkv, w_qkv_full)
        _, norm_back = jax.vjp(rms_scale, layer_input, gain_pair[0])
        d_input_norm, d_gain_one = norm_back(d_normed_one)
        grad_stream = grad_mixed + d_input_norm
        dense_parts[layer_no] = [d_w_qkv.astype(BF16), d_w_out.astype(BF16)]
        small_parts[layer_no] = [
            d_router.astype(BF16),
            jnp.stack([d_gain_one, d_gain_two], 1).astype(BF16),
        ]
        collected[layer_no] = (
            d_experts[:, :in_rows, :].astype(F32),
            d_experts[:, in_rows:, :].astype(F32),
        )
    small = sum(small_parts, [])
    small.append(jnp.zeros((width, side - LAYERS * (experts_total + 2)), BF16))
    parts = sum(dense_parts, []) + [jnp.concatenate(small, 1)]
    d_dense = [part.reshape(shards, width // shards, -1) for part in parts]
    d_dense = reduce_dense(d_dense, shards, owners).astype(F32)
    for layer_no in range(LAYERS):
        at = layer_no * layer_columns
        d_main = d_dense[:, at : at + layer_columns]
        at = LAYERS * layer_columns + layer_no * (experts_total + 2)
        small = d_dense[:, at : at + experts_total + 2]
        collected[layer_no] = (
            small[:, experts_total:].T,
            d_main[:, :qkv_width],
            d_main[:, qkv_width:],
            small[:, :experts_total],
        ) + collected[layer_no]
    stacked = [
        jnp.stack([collected[layer_no][member] for layer_no in range(LAYERS)], 0)
        for member in range(6)
    ]
    results = [stream, grad_stream]
    results.extend(adam_update(gains, stacked[0], gains_first, gains_second))
    results.extend(adam_update(w_qkv, stacked[1], w_qkv_first, w_qkv_second))
    results.extend(adam_update(w_out, stacked[2], w_out_first, w_out_second))
    results.extend(adam_update(router, stacked[3], router_first, router_second))
    results.extend(adam_update(w_in, stacked[4], w_in_first, w_in_second))
    results.extend(adam_update(w_down, stacked[5], w_down_first, w_down_second))
    return tuple(results)


def solution(mesh):
    return jax.shard_map(
        on_device,
        mesh=mesh,
        in_specs=(
            P(("expert", "shard"), None),
            P(("expert", "shard"), None),
            P(),
            P(None, ("expert", "shard"), None),
            P(None, None, "shard"),
            P(None, None, "shard"),
            P(None, None, "shard"),
            P(None, "shard", None),
            P(None, "shard", None),
            P(None, "shard", None),
            P(None, "shard", None),
            P(None, "shard", None),
            P(None, "shard", None),
            P(None, "shard", None),
            P(None, "shard", None),
            P(None, "shard", None),
            P(None, "expert", "shard", None),
            P(None, "expert", "shard", None),
            P(None, "expert", "shard", None),
            P(None, "expert", "shard", None),
            P(None, "expert", "shard", None),
            P(None, "expert", "shard", None),
        ),
        out_specs=(
            P(("expert", "shard"), None),
            P(("expert", "shard"), None),
            P(None, None, "shard"),
            P(None, None, "shard"),
            P(None, None, "shard"),
            P(None, None, "shard"),
            P(None, "shard", None),
            P(None, "shard", None),
            P(None, "shard", None),
            P(None, "shard", None),
            P(None, "shard", None),
            P(None, "shard", None),
            P(None, "shard", None),
            P(None, "shard", None),
            P(None, "shard", None),
            P(None, "shard", None),
            P(None, "shard", None),
            P(None, "shard", None),
            P(None, "expert", "shard", None),
            P(None, "expert", "shard", None),
            P(None, "expert", "shard", None),
            P(None, "expert", "shard", None),
            P(None, "expert", "shard", None),
            P(None, "expert", "shard", None),
            P(None, "expert", "shard", None),
            P(None, "expert", "shard", None),
        ),
        check_vma=False,
    )
```

```python
import functools

import jax
import jax.numpy as jnp
from jax import lax
from jax.experimental import pallas as pl
from jax.experimental.pallas import tpu as pltpu
from jax.sharding import PartitionSpec as P

HEADS = 16
KV_HEADS = 8
HEAD = 64
TOP = 8
LAYERS = 2
WINDOW = 1024
SPAN = 8

norm_eps = 1e-05
masked_score = -1e30
beta_one = 0.9
beta_two = 0.95
adam_eps = 1e-08
learn_rate = 0.05
decay_rate = 0.1
adam_step = 10.0

F32 = jnp.float32
BF16 = jnp.bfloat16
MESH = pl.DeviceIdType.MESH
VMEM_LIMIT = 60 * 1024 * 1024


def rms_scale(values, gain_row):
    return (
        values * lax.rsqrt(jnp.mean(values * values, axis=-1, keepdims=True) + norm_eps) * gain_row
    )


def inner_rows(left_side, right_side):
    return lax.dot_general(
        left_side, right_side, (((0,), (0,)), ((), ())), preferred_element_type=F32
    )


def outer_cols(left_side, right_side):
    return lax.dot_general(
        left_side, right_side, (((1,), (1,)), ((), ())), preferred_element_type=F32
    )


def adam_update(weight, gradient, first_moment, second_moment):
    new_first = beta_one * first_moment + (1.0 - beta_one) * gradient
    new_second = beta_two * second_moment + (1.0 - beta_two) * gradient * gradient
    corr_first = new_first / (1.0 - beta_one**adam_step)
    corr_second = new_second / (1.0 - beta_two**adam_step)
    weight_step = -learn_rate * (
        corr_first / (jnp.sqrt(corr_second) + adam_eps) + decay_rate * weight
    )
    return [gradient, new_first, new_second, weight_step]


def signal(barrier, where):
    pl.semaphore_signal(barrier, inc=1, device_id=where, device_id_type=MESH)


def greet_chips(owners):
    e = lax.axis_index("expert")
    partner = e + 1 - 2 * lax.rem(e, 2)
    barrier = pltpu.get_barrier_semaphore()
    signal(barrier, {"expert": partner})
    for d in range(1, owners // 2):
        signal(barrier, {"expert": lax.rem(e + 2 * d, owners)})
    pl.semaphore_wait(barrier, owners // 2)
    return e, partner


def spread_kernel(owners, cuts, x_ref, o_ref, pair_send, pair_recv, far_send, far_recv):
    e, partner = greet_chips(owners)
    chips = owners // 2
    size = x_ref.shape[0] // cuts

    def pair_copy(d, cut):
        rows = pl.ds(cut * size, size)
        there = o_ref.at[lax.rem(e + owners - 2 * d, owners), rows]
        return pltpu.make_async_remote_copy(
            src_ref=x_ref.at[rows] if d == 0 else there,
            dst_ref=there,
            send_sem=pair_send.at[d, cut],
            recv_sem=pair_recv.at[d, cut],
            device_id={"expert": partner},
            device_id_type=MESH,
        )

    def far_copy(d, cut):
        rows = pl.ds(cut * size, size)
        return pltpu.make_async_remote_copy(
            src_ref=x_ref.at[rows],
            dst_ref=o_ref.at[e, rows],
            send_sem=far_send.at[d - 1, cut],
            recv_sem=far_recv.at[d - 1, cut],
            device_id={"expert": lax.rem(e + 2 * d, owners)},
            device_id_type=MESH,
        )

    for cut in range(cuts):
        for d in range(1, chips):
            far_copy(d, cut).start()
    for cut in range(cuts):
        pair_copy(0, cut).start()
    o_ref[e] = x_ref[...]
    for cut in range(cuts):
        for d in range(1, chips):
            far_copy(d, cut).wait_recv()
            pair_copy(d, cut).start()
    for cut in range(cuts):
        for d in range(chips):
            pair_copy(d, cut).wait()
        for d in range(1, chips):
            far_copy(d, cut).wait_send()


def spread(rows, owners, collective):
    dma = pltpu.SemaphoreType.DMA
    chips, cuts = owners // 2, 4
    return pl.pallas_call(
        functools.partial(spread_kernel, owners, cuts),
        out_shape=jax.ShapeDtypeStruct((owners,) + rows.shape, rows.dtype),
        in_specs=[pl.BlockSpec(memory_space=pltpu.VMEM)],
        out_specs=pl.BlockSpec(memory_space=pltpu.VMEM),
        scratch_shapes=[
            dma((chips, cuts)), dma((chips, cuts)), dma((chips - 1, cuts)), dma((chips - 1, cuts)),
        ],
        compiler_params=pltpu.CompilerParams(
            collective_id=collective, has_side_effects=True, vmem_limit_bytes=VMEM_LIMIT
        ),
        name="spread",
    )(rows)


def collect_kernel(
    owners, cuts, p_ref, o_ref, paired, going, came, pair_send, pair_recv, far_send, far_recv
):
    e, partner = greet_chips(owners)
    chips = owners // 2
    size = o_ref.shape[0] // cuts

    def pair_copy(d, cut):
        rows = pl.ds(cut * size, size)
        return pltpu.make_async_remote_copy(
            src_ref=p_ref.at[lax.rem(partner + 2 * d, owners), rows],
            dst_ref=paired.at[d, rows],
            send_sem=pair_send.at[d, cut],
            recv_sem=pair_recv.at[d, cut],
            device_id={"expert": partner},
            device_id_type=MESH,
        )

    def far_copy(d, cut):
        rows = pl.ds(cut * size, size)
        return pltpu.make_async_remote_copy(
            src_ref=going.at[d - 1, rows],
            dst_ref=came.at[d - 1, rows],
            send_sem=far_send.at[d - 1, cut],
            recv_sem=far_recv.at[d - 1, cut],
            device_id={"expert": lax.rem(e + 2 * d, owners)},
            device_id_type=MESH,
        )

    for cut in range(cuts):
        for d in range(1, chips):
            pair_copy(d, cut).start()
    for cut in range(cuts):
        pair_copy(0, cut).start()
    for cut in range(cuts):
        rows = pl.ds(cut * size, size)
        for d in range(1, chips):
            pair_copy(d, cut).wait_recv()
            going[d - 1, rows, :] = (
                p_ref[lax.rem(e + 2 * d, owners), rows, :].astype(F32)
                + paired[d, rows, :].astype(F32)
            ).astype(BF16)
            far_copy(d, cut).start()
    for cut in range(cuts):
        rows = pl.ds(cut * size, size)
        pair_copy(0, cut).wait_recv()
        total = p_ref[e, rows, :].astype(F32) + paired[0, rows, :].astype(F32)
        for d in range(1, chips):
            far_copy(d, cut).wait_recv()
            total = total + came[d - 1, rows, :].astype(F32)
        o_ref[rows, :] = total
    for cut in range(cuts):
        for d in range(chips):
            pair_copy(d, cut).wait_send()
        for d in range(1, chips):
            far_copy(d, cut).wait_send()


def collect(parts, collective):
    owners, rows, width = parts.shape
    dma = pltpu.SemaphoreType.DMA
    chips, cuts = owners // 2, 4
    return pl.pallas_call(
        functools.partial(collect_kernel, owners, cuts),
        out_shape=jax.ShapeDtypeStruct((rows, width), F32),
        in_specs=[pl.BlockSpec(memory_space=pltpu.VMEM)],
        out_specs=pl.BlockSpec(memory_space=pltpu.VMEM),
        scratch_shapes=[
            pltpu.VMEM((chips, rows, width), parts.dtype),
            pltpu.VMEM((chips - 1, rows, width), parts.dtype),
            pltpu.VMEM((chips - 1, rows, width), parts.dtype),
            dma((chips, cuts)), dma((chips, cuts)), dma((chips - 1, cuts)), dma((chips - 1, cuts)),
        ],
        compiler_params=pltpu.CompilerParams(
            collective_id=collective, has_side_effects=True, vmem_limit_bytes=VMEM_LIMIT
        ),
        name="collect",
    )(parts)


def ring_shard(place, count):
    back = lax.div(place, count // 2)
    return (1 - back) * 2 * place + back * (2 * (count - 1 - place) + 1)


def ring_place(shard, count):
    odd, pair = lax.rem(shard, 2), lax.div(shard, 2)
    return (1 - odd) * pair + odd * (count - 1 - pair)


def gather_dense_kernel(
    n, owners, rows, x_ref, o_ref,
    ring_send, ring_recv, pair_send, pair_recv, far_send, far_recv, own_sem,
):
    e, s = lax.axis_index("expert"), lax.axis_index("shard")
    partner = e + 1 - 2 * lax.rem(e, 2)
    chips = owners // 2
    p = ring_place(s, n)
    ways = (ring_shard(lax.rem(p + 1, n), n), ring_shard(lax.rem(p + n - 1, n), n))
    barrier = pltpu.get_barrier_semaphore()
    signal(barrier, {"expert": partner})
    signal(barrier, {"shard": ways[0]})
    signal(barrier, {"shard": ways[1]})
    for d in range(1, chips):
        signal(barrier, {"expert": lax.rem(e + 2 * d, owners)})
    pl.semaphore_wait(barrier, 2 + chips)
    half, wide = rows // 2, x_ref.shape[1] // owners

    def columns(owner):
        return pl.ds(pl.multiple_of(owner * wide, 128), wide)

    def region(way, k, owner):
        block = ring_shard(lax.rem(p + (n - k if way == 0 else k), n), n)
        return o_ref.at[block, pl.ds(way * half, half), columns(owner)]

    def ring_copy(way, k, src):
        return pltpu.make_async_remote_copy(
            src_ref=src,
            dst_ref=region(way, k, e),
            send_sem=ring_send.at[way, k],
            recv_sem=ring_recv.at[way, k],
            device_id={"shard": ways[way]},
            device_id_type=MESH,
        )

    def far_copy(d, way, k):
        return pltpu.make_async_remote_copy(
            src_ref=region(way, k, e),
            dst_ref=region(way, k, e),
            send_sem=far_send.at[d - 1, way, k - 1],
            recv_sem=far_recv.at[d - 1, way, k - 1],
            device_id={"expert": lax.rem(e + 2 * d, owners)},
            device_id_type=MESH,
        )

    def pair_copy(d, way, k):
        there = region(way, k, lax.rem(e + owners - 2 * d, owners))
        return pltpu.make_async_remote_copy(
            src_ref=there,
            dst_ref=there,
            send_sem=pair_send.at[d, way, k - 1],
            recv_sem=pair_recv.at[d, way, k - 1],
            device_id={"expert": partner},
            device_id_type=MESH,
        )

    def hand_on(k):
        for way in range(2):
            for d in range(1, chips):
                far_copy(d, way, k).wait_recv()
                pair_copy(d, way, k).start()

    for way in range(2):
        ring_copy(way, 0, x_ref.at[pl.ds(way * half, half), columns(e)]).start()
    own = pltpu.make_async_copy(x_ref, o_ref.at[s], own_sem)
    own.start()

    def step(k, carry):
        for way in range(2):
            came = region(way, k, e)
            ring_copy(way, k - 1, came).wait_recv()

            @pl.when(k < n - 1)
            def _():
                ring_copy(way, k, came).start()

            for d in range(1, chips):
                far_copy(d, way, k).start()
            pair_copy(0, way, k).start()

        @pl.when(k > 1)
        def _():
            hand_on(k - 1)

        return carry

    lax.fori_loop(1, n, step, 0)
    hand_on(n - 1)

    def finish(k, carry):
        for way in range(2):
            ring_copy(way, k - 1, region(way, k, e)).wait_send()
            for d in range(chips):
                pair_copy(d, way, k).wait()
            for d in range(1, chips):
                far_copy(d, way, k).wait_send()
        return carry

    lax.fori_loop(1, n, finish, 0)
    own.wait()


def gather_dense(piece, n, owners):
    rows, columns = piece.shape
    dma = pltpu.SemaphoreType.DMA
    chips = owners // 2
    return pl.pallas_call(
        functools.partial(gather_dense_kernel, n, owners, rows),
        out_shape=jax.ShapeDtypeStruct((n, rows, columns), piece.dtype),
        in_specs=[pl.BlockSpec(memory_space=pltpu.VMEM)],
        out_specs=pl.BlockSpec(memory_space=pl.ANY),
        scratch_shapes=[
            dma((2, n - 1)), dma((2, n - 1)), dma((chips, 2, n - 1)), dma((chips, 2, n - 1)),
            dma((chips - 1, 2, n - 1)), dma((chips - 1, 2, n - 1)), dma,
        ],
        compiler_params=pltpu.CompilerParams(
            collective_id=3, has_side_effects=True, vmem_limit_bytes=VMEM_LIMIT
        ),
        name="gather_dense",
    )(piece)


def reduce_dense_kernel(
    n, owners, rows, places, *refs,
):
    g_refs = refs[: len(places)]
    (
        o_ref, paired, came, going, crossed, last_in, pair_send, pair_recv, ring_send,
        ring_recv, cross_send, cross_recv, last_send, last_recv,
    ) = refs[len(places) :]
    e, s = lax.axis_index("expert"), lax.axis_index("shard")
    core, x = lax.rem(e, 2), lax.div(e, 2)
    partner = e + 1 - 2 * core
    columns = owners // 2
    p = ring_place(s, n)
    ways = (ring_shard(lax.rem(p + 1, n), n), ring_shard(lax.rem(p + n - 1, n), n))
    barrier = pltpu.get_barrier_semaphore()
    signal(barrier, {"expert": partner})
    signal(barrier, {"shard": ways[0]})
    signal(barrier, {"shard": ways[1]})
    for d in range(1, columns):
        signal(barrier, {"expert": lax.rem(e + 2 * d, owners)})
    pl.semaphore_wait(barrier, 3 + columns - 1)
    half, quarter = rows // 2, rows // 4

    def mine(way):
        return pl.ds(pl.multiple_of(core * half + way * quarter, quarter), quarter)

    def block(way, k):
        return ring_shard(lax.rem(p + (2 * n - 1 - k if way == 0 else k + 1), n), n)

    def pair_copy(k, i):
        b = block(0, k)
        at, wide = places[i]
        return pltpu.make_async_remote_copy(
            src_ref=g_refs[i].at[b, pl.ds(pl.multiple_of((1 - core) * half, half), half)],
            dst_ref=paired.at[b, :, pl.ds(at, wide)],
            send_sem=pair_send.at[i, b],
            recv_sem=pair_recv.at[i, b],
            device_id={"expert": partner},
            device_id_type=MESH,
        )

    def ring_copy(way, k):
        return pltpu.make_async_remote_copy(
            src_ref=going.at[way, k],
            dst_ref=came.at[way, k],
            send_sem=ring_send.at[way, k],
            recv_sem=ring_recv.at[way, k],
            device_id={"shard": ways[way]},
            device_id_type=MESH,
        )

    def put(target, way, b, more=None):
        for g_ref, (at, wide) in zip(g_refs, places):
            total = g_ref[b, mine(way), :].astype(F32) + paired[
                b, way * quarter : (way + 1) * quarter, at : at + wide
            ].astype(F32)
            if more is not None:
                total = total + more[:, at : at + wide].astype(F32)
            target[:, at : at + wide] = total.astype(BF16)

    order = []
    for k in range(n):
        for place in (k, n - 2 - k):
            place = place % n
            if place not in order:
                order.append(place)
    every = range(len(places))
    for k in order:
        for i in every:
            pair_copy(k, i).start()
    for k in order[:2]:
        for i in every:
            pair_copy(k, i).wait_recv()
    for way in range(2):
        put(going.at[way, 0], way, block(way, 0))
        ring_copy(way, 0).start()
    for k in order[2:]:
        for i in every:
            pair_copy(k, i).wait_recv()

    def step(k, carry):
        for way in range(2):
            ring_copy(way, k - 1).wait_recv()
            put(going.at[way, k], way, block(way, k), came.at[way, k - 1])
            ring_copy(way, k).start()
        return carry

    lax.fori_loop(1, n - 1, step, 0)
    for way in range(2):
        ring_copy(way, n - 2).wait_recv()
        put(
            crossed.at[x, pl.ds(way * quarter, quarter)], way, s, came.at[way, n - 2]
        )

    def cross_copy(d):
        return pltpu.make_async_remote_copy(
            src_ref=crossed.at[x],
            dst_ref=crossed.at[x],
            send_sem=cross_send.at[d - 1],
            recv_sem=cross_recv.at[d - 1],
            device_id={"expert": lax.rem(e + 2 * d, owners)},
            device_id_type=MESH,
        )

    for d in range(1, columns):
        cross_copy(d).start()
    for d in range(1, columns):
        cross_copy(d).wait()
    total = crossed[0].astype(F32)
    for d in range(1, columns):
        total = total + crossed[d].astype(F32)
    here = pl.ds(pl.multiple_of(core * half, half), half)
    o_ref[here, :] = total.astype(BF16)
    last = pltpu.make_async_remote_copy(
        src_ref=o_ref.at[here],
        dst_ref=last_in,
        send_sem=last_send,
        recv_sem=last_recv,
        device_id={"expert": partner},
        device_id_type=MESH,
    )
    last.start()
    for k in order:
        for i in every:
            pair_copy(k, i).wait_send()

    def finish(k, carry):
        for way in range(2):
            ring_copy(way, k).wait_send()
        return carry

    lax.fori_loop(0, n - 1, finish, 0)
    last.wait()
    o_ref[pl.ds(pl.multiple_of((1 - core) * half, half), half), :] = last_in[...]


def reduce_dense(grads, n, owners):
    rows = grads[0].shape[1]
    places, columns = [], 0
    for grad in grads:
        places.append((columns, grad.shape[2]))
        columns += grad.shape[2]
    dma = pltpu.SemaphoreType.DMA
    across = owners // 2
    return pl.pallas_call(
        functools.partial(reduce_dense_kernel, n, owners, rows, tuple(places)),
        out_shape=jax.ShapeDtypeStruct((rows, columns), BF16),
        in_specs=[pl.BlockSpec(memory_space=pltpu.VMEM)] * len(places),
        out_specs=pl.BlockSpec(memory_space=pltpu.VMEM),
        scratch_shapes=[
            pltpu.VMEM((n, rows // 2, columns), BF16),
            pltpu.VMEM((2, n - 1, rows // 4, columns), BF16),
            pltpu.VMEM((2, n - 1, rows // 4, columns), BF16),
            pltpu.VMEM((across, rows // 2, columns), BF16),
            pltpu.VMEM((rows // 2, columns), BF16),
            dma((len(places), n)), dma((len(places), n)), dma((2, n - 1)), dma((2, n - 1)),
            dma((across - 1,)), dma((across - 1,)), dma, dma,
        ],
        compiler_params=pltpu.CompilerParams(
            collective_id=4, has_side_effects=True, vmem_limit_bytes=VMEM_LIMIT
        ),
        name="reduce_dense",
    )(*grads)


def halo_links(n, s):
    odd = lax.rem(s, 2)
    return odd, s + 1 - 2 * odd, s + 2 < n, s >= 2


def halo_barrier(s, odd, mate, ahead, behind, sends_back):
    barrier = pltpu.get_barrier_semaphore()
    even = odd == 0
    to_ahead, to_behind = (ahead, behind) if not sends_back else (behind, ahead)
    step = -2 if not sends_back else 2
    mate_copies = (odd == 1) | behind if not sends_back else even | behind
    to_mate = even | behind if not sends_back else (odd == 1) | behind

    @pl.when(to_behind)
    def _():
        signal(barrier, {"shard": s + step})

    @pl.when(mate_copies)
    def _():
        signal(barrier, {"shard": mate})

    @pl.when(to_ahead & to_mate)
    def _():
        pl.semaphore_wait(barrier, 2)

    @pl.when(to_ahead != to_mate)
    def _():
        pl.semaphore_wait(barrier, 1)


def halo_kernel(n, rows, cuts, kv_ref, o_ref, sends, recvs, own_sem):
    s = lax.axis_index("shard")
    odd, mate, ahead, behind = halo_links(n, s)
    even = odd == 0
    size = rows // cuts

    def copy(kind, cut, src, slot, where):
        return pltpu.make_async_remote_copy(
            src_ref=src.at[pl.ds(cut * size, size)],
            dst_ref=o_ref.at[slot, pl.ds(cut * size, size)],
            send_sem=sends.at[kind, cut],
            recv_sem=recvs.at[kind, cut],
            device_id={"shard": where},
            device_id_type=MESH,
        )

    halo_barrier(s, odd, mate, ahead, behind, False)
    from_odd = (o_ref.at[2], o_ref.at[0])
    from_even = (kv_ref, o_ref.at[2])
    for cut in range(cuts):

        @pl.when(ahead)
        def _():
            copy(0, cut, kv_ref, 2, s + 2).start()

        @pl.when(even)
        def _():
            copy(2, cut, kv_ref, 3, mate).start()

    o_ref[4] = kv_ref[...]
    for slot in range(4):

        @pl.when(s < 4 - slot)
        def _():
            o_ref[slot] = jnp.zeros_like(o_ref[slot])

    for cut in range(cuts):

        @pl.when(behind)
        def _():
            copy(0, cut, kv_ref, 2, s).wait_recv()

        @pl.when(behind & ahead)
        def _():
            copy(1, cut, o_ref.at[2], 0, s + 2).start()

        @pl.when(behind & (odd == 1))
        def _():
            copy(2, cut, from_odd[0], 3, mate).start()

        @pl.when(behind & even)
        def _():
            copy(3, cut, from_even[1], 1, mate).start()

    for cut in range(cuts):

        @pl.when(s >= 4)
        def _():
            copy(1, cut, o_ref.at[2], 0, s).wait_recv()

        @pl.when((s >= 4) & (odd == 1))
        def _():
            copy(3, cut, from_odd[1], 1, mate).start()

    for cut in range(cuts):

        @pl.when(s >= 1)
        def _():
            copy(2, cut, kv_ref, 3, mate).wait_recv()

        @pl.when(s >= 3)
        def _():
            copy(3, cut, kv_ref, 1, mate).wait_recv()

        @pl.when(ahead)
        def _():
            copy(0, cut, kv_ref, 2, s).wait_send()

        @pl.when(behind & ahead)
        def _():
            copy(1, cut, kv_ref, 0, s).wait_send()

        @pl.when(even | behind)
        def _():
            copy(2, cut, kv_ref, 3, mate).wait_send()

        @pl.when((even & behind) | ((odd == 1) & (s >= 4)))
        def _():
            copy(3, cut, kv_ref, 1, mate).wait_send()


def halo(kv, n, slots):
    rows, columns = kv.shape
    dma = pltpu.SemaphoreType.DMA
    cuts = 2
    return pl.pallas_call(
        functools.partial(halo_kernel, n, rows, cuts),
        out_shape=jax.ShapeDtypeStruct((slots, rows, columns), kv.dtype),
        in_specs=[pl.BlockSpec(memory_space=pltpu.VMEM)],
        out_specs=pl.BlockSpec(memory_space=pltpu.VMEM),
        scratch_shapes=[dma((4, cuts)), dma((4, cuts)), dma],
        compiler_params=pltpu.CompilerParams(
            collective_id=5, has_side_effects=True, vmem_limit_bytes=VMEM_LIMIT
        ),
        name="halo",
    )(kv)


def halo_back_kernel(n, rows, cuts, g_ref, o_ref, own, came, sends, recvs):
    s = lax.axis_index("shard")
    odd, mate, ahead, behind = halo_links(n, s)
    even = odd == 0
    size = rows // cuts

    def copy(kind, cut, src, where):
        return pltpu.make_async_remote_copy(
            src_ref=src.at[pl.ds(cut * size, size)],
            dst_ref=came.at[kind, pl.ds(cut * size, size)],
            send_sem=sends.at[kind, cut],
            recv_sem=recvs.at[kind, cut],
            device_id={"shard": where},
            device_id_type=MESH,
        )

    def there(ref, cut, value=None):
        here = pl.ds(cut * size, size)
        return ref[here, :].astype(F32)

    halo_barrier(s, odd, mate, ahead, behind, True)
    for cut in range(cuts):

        @pl.when(s >= 3)
        def _():
            copy(3, cut, g_ref.at[1], mate).start()

        @pl.when(s >= 1)
        def _():
            copy(2, cut, g_ref.at[3], mate).start()

    for cut in range(cuts):
        here = pl.ds(cut * size, size)

        @pl.when((odd == 1) & (s >= 4))
        def _():
            copy(3, cut, g_ref.at[1], mate).wait_recv()
            own[0, here, :] = (there(g_ref.at[0], cut) + there(came.at[3], cut)).astype(BF16)

        @pl.when((odd == 1) & (s >= 4))
        def _():
            copy(1, cut, own.at[0], s - 2).start()

        @pl.when(even & (s >= 4))
        def _():
            copy(1, cut, g_ref.at[0], s - 2).start()

    for cut in range(cuts):
        here = pl.ds(cut * size, size)

        @pl.when((odd == 1) & behind)
        def _():
            copy(2, cut, g_ref.at[3], mate).wait_recv()
            own[1, here, :] = (there(g_ref.at[2], cut) + there(came.at[2], cut)).astype(BF16)

        @pl.when(even & behind)
        def _():
            copy(3, cut, g_ref.at[1], mate).wait_recv()
            own[1, here, :] = (there(g_ref.at[2], cut) + there(came.at[3], cut)).astype(BF16)

        @pl.when(behind & ahead)
        def _():
            copy(1, cut, g_ref.at[0], s).wait_recv()
            own[1, here, :] = (there(own.at[1], cut) + there(came.at[1], cut)).astype(BF16)

        @pl.when(behind)
        def _():
            copy(0, cut, own.at[1], s - 2).start()

    for cut in range(cuts):
        here = pl.ds(cut * size, size)
        o_ref[here, :] = there(g_ref.at[4], cut)

        @pl.when(even)
        def _():
            copy(2, cut, g_ref.at[3], mate).wait_recv()
            o_ref[here, :] += there(came.at[2], cut)

        @pl.when(ahead)
        def _():
            copy(0, cut, own.at[1], s).wait_recv()
            o_ref[here, :] += there(came.at[0], cut)

        @pl.when(s >= 3)
        def _():
            copy(3, cut, g_ref.at[1], mate).wait_send()

        @pl.when(s >= 1)
        def _():
            copy(2, cut, g_ref.at[3], mate).wait_send()

        @pl.when(s >= 4)
        def _():
            copy(1, cut, g_ref.at[0], mate).wait_send()

        @pl.when(behind)
        def _():
            copy(0, cut, own.at[1], mate).wait_send()


def halo_back(grads, n):
    slots, rows, columns = grads.shape
    dma = pltpu.SemaphoreType.DMA
    cuts = 2
    return pl.pallas_call(
        functools.partial(halo_back_kernel, n, rows, cuts),
        out_shape=jax.ShapeDtypeStruct((rows, columns), F32),
        in_specs=[pl.BlockSpec(memory_space=pltpu.VMEM)],
        out_specs=pl.BlockSpec(memory_space=pltpu.VMEM),
        scratch_shapes=[
            pltpu.VMEM((3, rows, columns), BF16),
            pltpu.VMEM((4, rows, columns), BF16),
            dma((4, cuts)),
            dma((4, cuts)),
        ],
        compiler_params=pltpu.CompilerParams(
            collective_id=6, has_side_effects=True, vmem_limit_bytes=VMEM_LIMIT
        ),
        name="halo_back",
    )(grads)


def attend_kernel(q_ref, k_ref, v_ref, bias_ref, o_ref, total_ref):
    for h in range(q_ref.shape[1] // HEAD):
        at = pl.ds(h * HEAD, HEAD)
        kv_at = pl.ds(h // (HEADS // KV_HEADS) * HEAD, HEAD)
        query = q_ref[:, at] * jnp.asarray(HEAD**-0.5, BF16)
        scores = outer_cols(k_ref[:, kv_at], query) + bias_ref[...]
        top = jnp.max(scores, axis=0, keepdims=True)
        powers = jnp.exp(scores - top)
        total = jnp.sum(powers, axis=0, keepdims=True)
        value = inner_rows(v_ref[:, kv_at], powers.astype(BF16)) / total
        o_ref[:, at] = value.T.astype(BF16)
        total_ref[0, h : h + 1, :] = top + jnp.log(total)


def attention_specs(tok_rows, key_count):
    span = 2 * HEAD
    groups = HEADS // KV_HEADS
    steps = KV_HEADS // 2
    return steps, [
        pl.BlockSpec((tok_rows, groups * span), lambda j: (0, j)),
        pl.BlockSpec((key_count, span), lambda j: (0, j)),
        pl.BlockSpec((key_count, span), lambda j: (0, j + steps)),
        pl.BlockSpec((key_count, tok_rows), lambda j: (0, 0)),
    ]


def attend(qkv_rows, ext, bias):
    key_count, tok_rows = bias.shape
    steps, specs = attention_specs(tok_rows, key_count)
    return pl.pallas_call(
        attend_kernel,
        grid=(steps,),
        in_specs=specs,
        out_specs=[specs[0], pl.BlockSpec((1, 8, tok_rows), lambda j: (j, 0, 0))],
        out_shape=[
            jax.ShapeDtypeStruct((tok_rows, HEADS * HEAD), BF16),
            jax.ShapeDtypeStruct((steps, 8, tok_rows), F32),
        ],
        compiler_params=pltpu.CompilerParams(vmem_limit_bytes=VMEM_LIMIT),
        cost_estimate=pl.CostEstimate(
            flops=4 * HEADS * HEAD * tok_rows * key_count,
            bytes_accessed=4 * key_count * tok_rows + 4 * key_count * KV_HEADS * HEAD,
            transcendentals=HEADS * tok_rows * key_count,
        ),
        name="attend",
    )(qkv_rows, ext, ext, bias)


def attend_back_kernel(
    q_ref, k_ref, v_ref, bias_ref, d_ref, total_ref, d_query_ref, d_kv_ref
):
    groups = HEADS // KV_HEADS
    scale = jnp.asarray(HEAD**-0.5, BF16)
    span = k_ref.shape[1]
    for kv in range(span // HEAD):
        kv_at = pl.ds(kv * HEAD, HEAD)
        key, value = k_ref[:, kv_at], v_ref[:, kv_at]
        d_key = d_value = None
        for h in range(kv * groups, (kv + 1) * groups):
            at = pl.ds(h * HEAD, HEAD)
            query = q_ref[:, at] * scale
            d_out = d_ref[:, at]
            scores = outer_cols(key, query) + bias_ref[...]
            probs = jnp.exp(scores - total_ref[0, h : h + 1, :])
            d_probs = outer_cols(value, d_out)
            mean_d = jnp.sum(probs * d_probs, axis=0, keepdims=True)
            d_scores = (probs * (d_probs - mean_d)).astype(BF16)
            d_query = inner_rows(key, d_scores) * (HEAD**-0.5)
            d_query_ref[:, at] = d_query.T.astype(BF16)
            more_key = jnp.dot(d_scores, query, preferred_element_type=F32)
            more_value = jnp.dot(probs.astype(BF16), d_out, preferred_element_type=F32)
            d_key = more_key if d_key is None else d_key + more_key
            d_value = more_value if d_value is None else d_value + more_value
        d_kv_ref[:, kv * HEAD : (kv + 1) * HEAD] = d_key.astype(BF16)
        d_kv_ref[:, span + kv * HEAD : span + (kv + 1) * HEAD] = d_value.astype(BF16)


def attend_back(qkv_rows, ext, bias, d_attended, totals):
    key_count, tok_rows = bias.shape
    steps, specs = attention_specs(tok_rows, key_count)
    return pl.pallas_call(
        attend_back_kernel,
        grid=(steps,),
        in_specs=specs + [specs[0], pl.BlockSpec((1, 8, tok_rows), lambda j: (j, 0, 0))],
        out_specs=[specs[0], pl.BlockSpec((key_count, 4 * HEAD), lambda j: (0, j))],
        out_shape=[
            jax.ShapeDtypeStruct((tok_rows, HEADS * HEAD), BF16),
            jax.ShapeDtypeStruct((key_count, 2 * KV_HEADS * HEAD), BF16),
        ],
        compiler_params=pltpu.CompilerParams(vmem_limit_bytes=VMEM_LIMIT),
        cost_estimate=pl.CostEstimate(
            flops=10 * HEADS * HEAD * tok_rows * key_count,
            bytes_accessed=4 * key_count * tok_rows + 8 * key_count * KV_HEADS * HEAD,
            transcendentals=HEADS * tok_rows * key_count,
        ),
        name="attend_back",
    )(qkv_rows, ext, ext, bias, d_attended, totals)


def column_of(extra, index, experts_total):
    lanes = lax.broadcasted_iota(jnp.int32, extra.shape, 1)
    hit = (lanes == index) | (lanes == index + experts_total)
    return jnp.sum(jnp.where(hit, extra.astype(F32), 0.0), axis=1, keepdims=True)


def ffn_forward_kernel(
    tile, width, in_rows, experts_total, first_ref, x_ref, w_ref, part_ref, gate_up_ref, acc
):
    e = pl.program_id(0)
    w_in = w_ref[:, 0, :in_rows, :].reshape(width, w_ref.shape[-1])
    w_down = w_ref[:, 0, in_rows:, :].reshape(-1, width)
    half = w_in.shape[1] // 2
    index = first_ref[0] + e
    count = x_ref.shape[0] // tile
    for t in range(count):
        rows = pl.ds(t * tile, tile)
        gate_up = jnp.dot(x_ref[rows, :width], w_in, preferred_element_type=F32)
        gate, up = gate_up[:, :half], gate_up[:, half:]
        gate_up_ref[0, rows, :] = gate_up.astype(BF16)
        weight = column_of(x_ref[rows, width:], index, experts_total)
        hidden = (gate * jax.nn.sigmoid(gate) * up * weight).astype(BF16)
        out = jnp.dot(hidden, w_down, preferred_element_type=F32)

        @pl.when(e == 0)
        def _():
            acc[rows, :] = out

        @pl.when(e > 0)
        def _():
            acc[rows, :] += out

        @pl.when(e == pl.num_programs(0) - 1)
        def _():
            part_ref[rows, :] = acc[rows, :].astype(BF16)


def ffn_forward(first, x_all, w_all, experts_total, in_rows):
    shards, local, piece, inner = w_all.shape
    tokens, wide = x_all.shape
    width = in_rows * shards
    return pl.pallas_call(
        functools.partial(ffn_forward_kernel, 256, width, in_rows, experts_total),
        grid_spec=pltpu.PrefetchScalarGridSpec(
            num_scalar_prefetch=1,
            grid=(local,),
            in_specs=[
                pl.BlockSpec((tokens, wide), lambda e, f: (0, 0)),
                pl.BlockSpec((shards, 1, piece, inner), lambda e, f: (0, e, 0, 0)),
            ],
            out_specs=[
                pl.BlockSpec((tokens, width), lambda e, f: (0, 0)),
                pl.BlockSpec((1, tokens, inner), lambda e, f: (e, 0, 0)),
            ],
            scratch_shapes=[pltpu.VMEM((tokens, width), F32)],
        ),
        out_shape=[
            jax.ShapeDtypeStruct((tokens, width), BF16),
            jax.ShapeDtypeStruct((local, tokens, inner), BF16),
        ],
        compiler_params=pltpu.CompilerParams(vmem_limit_bytes=VMEM_LIMIT),
        cost_estimate=pl.CostEstimate(
            flops=2 * local * tokens * width * (inner + inner // 2),
            bytes_accessed=2 * (w_all.size + local * tokens * inner + 2 * tokens * wide),
            transcendentals=0,
        ),
        name="ffn_forward",
    )(first, x_all, w_all)


def ffn_backward_kernel(
    tile,
    width,
    in_rows,
    experts_total,
    first_ref,
    x_ref,
    g_ref,
    gate_up_ref,
    w_ref,
    part_ref,
    grad_ref,
    acc,
    d_gate_up,
    hidden_all,
    d_weights,
):
    e = pl.program_id(0)
    inner = w_ref.shape[-1]
    w_in = w_ref[:, 0, :in_rows, :].reshape(width, inner)
    w_down = w_ref[:, 0, in_rows:, :].reshape(-1, width)
    half = inner // 2
    index = first_ref[0] + e
    tokens = x_ref.shape[0]
    last = pl.num_programs(0) - 1
    for t in range(tokens // tile):
        rows = pl.ds(t * tile, tile)
        d_plain = outer_cols(g_ref[rows, :], w_down)
        gate = gate_up_ref[0, rows, :half].astype(F32)
        up = gate_up_ref[0, rows, half:].astype(F32)
        weight = column_of(x_ref[rows, width:], index, experts_total)
        sig = jax.nn.sigmoid(gate)
        silu = gate * sig
        hidden = silu * up
        d_weight = jnp.sum(hidden * d_plain, axis=1, keepdims=True)
        d_hidden = d_plain * weight
        hidden_all[rows, :] = (hidden * weight).astype(BF16)
        d_gate_up[rows, :half] = (d_hidden * up * sig * (1.0 + gate * (1.0 - sig))).astype(BF16)
        d_gate_up[rows, half:] = (d_hidden * silu).astype(BF16)
        lanes = lax.broadcasted_iota(jnp.int32, (tile, d_weights.shape[1]), 1)
        high = d_weight.astype(BF16).astype(F32)
        columns = jnp.where(
            lanes == index, high, jnp.where(lanes == index + experts_total, d_weight - high, 0.0)
        )
        out = outer_cols(d_gate_up[rows, :], w_in)

        @pl.when(e == 0)
        def _():
            acc[rows, :] = out
            d_weights[rows, :] = columns

        @pl.when(e > 0)
        def _():
            acc[rows, :] += out
            d_weights[rows, :] += columns

        @pl.when(e == last)
        def _():
            part_ref[rows, :width] = acc[rows, :].astype(BF16)
            part_ref[rows, width:] = d_weights[rows, :].astype(BF16)

    grad_ref[:, 0, :in_rows, :] = (
        inner_rows(x_ref[:, :width], d_gate_up[...]).astype(BF16).reshape(-1, in_rows, inner)
    )
    grad_ref[:, 0, in_rows:, :] = (
        inner_rows(hidden_all[...], g_ref[...])
        .astype(BF16)
        .reshape(-1, w_ref.shape[2] - in_rows, width)
    )


def ffn_backward(first, x_all, g_all, gate_up, w_all, experts_total, in_rows):
    shards, local, piece, inner = w_all.shape
    tokens, wide = x_all.shape
    width = in_rows * shards
    return pl.pallas_call(
        functools.partial(ffn_backward_kernel, 256, width, in_rows, experts_total),
        grid_spec=pltpu.PrefetchScalarGridSpec(
            num_scalar_prefetch=1,
            grid=(local,),
            in_specs=[
                pl.BlockSpec((tokens, wide), lambda e, f: (0, 0)),
                pl.BlockSpec((tokens, width), lambda e, f: (0, 0)),
                pl.BlockSpec((1, tokens, inner), lambda e, f: (e, 0, 0)),
                pl.BlockSpec((shards, 1, piece, inner), lambda e, f: (0, e, 0, 0)),
            ],
            out_specs=[
                pl.BlockSpec((tokens, wide), lambda e, f: (0, 0)),
                pl.BlockSpec((shards, 1, piece, inner), lambda e, f: (0, e, 0, 0)),
            ],
            scratch_shapes=[
                pltpu.VMEM((tokens, width), F32),
                pltpu.VMEM((tokens, inner), BF16),
                pltpu.VMEM((tokens, inner // 2), BF16),
                pltpu.VMEM((tokens, wide - width), F32),
            ],
        ),
        out_shape=[
            jax.ShapeDtypeStruct((tokens, wide), BF16),
            jax.ShapeDtypeStruct(w_all.shape, BF16),
        ],
        compiler_params=pltpu.CompilerParams(vmem_limit_bytes=VMEM_LIMIT),
        cost_estimate=pl.CostEstimate(
            flops=4 * local * tokens * width * (inner + inner // 2),
            bytes_accessed=2 * (2 * w_all.size + local * tokens * inner + 4 * tokens * wide),
            transcendentals=0,
        ),
        name="ffn_backward",
    )(first, x_all, g_all, gate_up, w_all)


def on_device(
    hidden_in,
    cotangent,
    doc_lengths,
    routes,
    gains,
    gains_first,
    gains_second,
    w_qkv,
    w_qkv_first,
    w_qkv_second,
    w_out,
    w_out_first,
    w_out_second,
    router,
    router_first,
    router_second,
    w_in,
    w_in_first,
    w_in_second,
    w_down,
    w_down_first,
    w_down_second,
):
    tok_rows, width = hidden_in.shape
    owners = lax.axis_size("expert")
    shards = lax.axis_size("shard")
    local_experts = w_in.shape[1]
    in_rows = w_in.shape[2]
    experts_total = local_experts * owners
    seq_len = tok_rows * SPAN
    hop_count = min(-(-WINDOW // tok_rows), SPAN - 1)
    key_count = (hop_count + 1) * tok_rows
    q_width = HEADS * HEAD
    kv_width = KV_HEADS * HEAD
    qkv_width = q_width + 2 * kv_width
    extra = -(-2 * experts_total // 128) * 128
    my_owner = lax.axis_index("expert")
    first_expert = my_owner * local_experts
    first_array = first_expert.astype(jnp.int32).reshape(1)
    row_start = (my_owner * shards + lax.axis_index("shard")) * tok_rows
    my_seq = row_start // seq_len
    doc_ends = jnp.cumsum(lax.dynamic_slice_in_dim(doc_lengths, my_seq, 1, 0)[0])
    query_rows = row_start + jnp.arange(tok_rows, dtype=jnp.int32)
    key_rows = row_start - hop_count * tok_rows + jnp.arange(key_count, dtype=jnp.int32)
    query_docs = jnp.sum(
        (query_rows[:, None] % seq_len >= doc_ends[None, :]).astype(jnp.int32), axis=1
    )
    key_docs = jnp.sum((key_rows[:, None] % seq_len >= doc_ends[None, :]).astype(jnp.int32), axis=1)
    distance = query_rows[None, :] - key_rows[:, None]
    allowed = (
        (query_rows[None, :] // seq_len == key_rows[:, None] // seq_len)
        & (query_docs[None, :] == key_docs[:, None])
        & (distance >= 0)
        & (distance < WINDOW)
    )
    bias = jnp.where(allowed, 0.0, masked_score).astype(F32)
    expert_ids = jnp.arange(experts_total, dtype=jnp.int32)
    side = 128
    layer_columns = qkv_width + width

    def dense_piece():
        rows = w_qkv.shape[1]
        parts = []
        for layer_no in range(LAYERS):
            parts += [w_qkv[layer_no].astype(BF16), w_out[layer_no].astype(BF16)]
        for layer_no in range(LAYERS):
            parts += [router[layer_no].astype(BF16), gains[layer_no].T.astype(BF16)]
        filled = LAYERS * (layer_columns + experts_total + 2)
        parts.append(jnp.zeros((rows, -filled % (128 * owners)), BF16))
        return jnp.concatenate(parts, 1)

    def expert_piece(layer_no):
        return jnp.concatenate(
            [w_in[layer_no].astype(BF16), w_down[layer_no].astype(BF16)], 1
        )

    expert_full = []
    for layer_no in range(LAYERS):
        expert_full.append(
            lax.all_gather(expert_piece(layer_no), "shard", axis=0, tiled=False)
        )
    dense = gather_dense(dense_piece(), shards, owners).reshape(width, -1)

    kept_layers = []
    stream = hidden_in
    for layer_no in range(LAYERS):
        at = layer_no * layer_columns
        w_qkv_full = dense[:, at : at + qkv_width]
        w_out_full = dense[:, at + qkv_width : at + layer_columns]
        at = LAYERS * layer_columns + layer_no * (experts_total + 2)
        small = dense[:, at : at + experts_total + 2]
        router_full = small[:, :experts_total]
        gain_pair = small[:, experts_total : experts_total + 2].astype(F32).T
        normed_one = rms_scale(stream, gain_pair[0]).astype(BF16)
        qkv_rows = jnp.dot(normed_one, w_qkv_full, preferred_element_type=F32).astype(BF16)
        ext = halo(qkv_rows[:, q_width:], shards, hop_count + 1).reshape(key_count, 2 * kv_width)
        attended, log_total = attend(qkv_rows, ext, bias)
        mixed = stream + jnp.dot(attended, w_out_full, preferred_element_type=F32)
        normed_two = rms_scale(mixed, gain_pair[1]).astype(BF16)
        logits = jnp.dot(normed_two, router_full, preferred_element_type=F32)
        named = jnp.any(routes[layer_no][:, :, None] == expert_ids[None, None, :], axis=1)
        top_logit = jnp.max(jnp.where(named, logits, -jnp.inf), axis=1, keepdims=True)
        powers = jnp.where(named, jnp.exp(jnp.where(named, logits - top_logit, 0.0)), 0.0)
        weights = powers / jnp.sum(powers, axis=1, keepdims=True)
        high = weights.astype(BF16)
        low = (weights - high.astype(F32)).astype(BF16)
        wide_rows = jnp.concatenate(
            [normed_two, high, low, jnp.zeros((tok_rows, extra - 2 * experts_total), BF16)], 1
        )
        x_all = spread(wide_rows, owners, 1).reshape(owners * tok_rows, width + extra)
        if layer_no == 0:
            g_rows, x_all = lax.optimization_barrier((cotangent.astype(BF16), x_all))
            g_all = spread(g_rows, owners, 8).reshape(owners * tok_rows, width)
            g_all, x_all = lax.optimization_barrier((g_all, x_all))
        partial, gate_up = ffn_forward(
            first_array, x_all, expert_full[layer_no], experts_total, in_rows
        )
        if layer_no + 1 == LAYERS:
            d_partial, d_experts = ffn_backward(
                first_array, x_all, g_all, gate_up, expert_full[layer_no], experts_total, in_rows
            )
            partial, d_partial = lax.optimization_barrier((partial, d_partial))
        moe_out = collect(partial.reshape(owners, tok_rows, width), 2)
        kept_layers.append(
            (
                stream, normed_one, qkv_rows, ext, log_total, attended, mixed,
                x_all, gate_up, normed_two, weights, w_qkv_full, w_out_full, router_full,
                gain_pair,
            )
        )
        stream = mixed + moe_out
    grad_stream = cotangent
    collected = [None] * LAYERS
    dense_parts = [None] * LAYERS
    small_parts = [None] * LAYERS
    for layer_no in reversed(range(LAYERS)):
        (
            layer_input, normed_one, qkv_rows, ext, log_total, attended, mixed,
            x_all, gate_up, normed_two, weights, w_qkv_full, w_out_full, router_full,
            gain_pair,
        ) = kept_layers[layer_no]
        if layer_no + 1 < LAYERS:
            g_all = spread(grad_stream.astype(BF16), owners, 8).reshape(owners * tok_rows, width)
            d_partial, d_experts = ffn_backward(
                first_array, x_all, g_all, gate_up, expert_full[layer_no], experts_total, in_rows
            )
        d_experts = lax.psum_scatter(d_experts, "shard", scatter_dimension=0, tiled=True)[0]
        d_all = collect(d_partial.reshape(owners, tok_rows, -1), 7)
        d_weights = (
            d_all[:, width : width + experts_total]
            + d_all[:, width + experts_total : width + 2 * experts_total]
        )
        mean_d = jnp.sum(weights * d_weights, axis=1, keepdims=True)
        d_logits = (weights * (d_weights - mean_d)).astype(BF16)
        d_router = inner_rows(normed_two, d_logits)
        d_normed_two = d_all[:, :width] + outer_cols(d_logits, router_full)
        _, norm_back = jax.vjp(rms_scale, mixed, gain_pair[1])
        d_mixed_norm, d_gain_two = norm_back(d_normed_two)
        grad_mixed = grad_stream + d_mixed_norm
        d_att = grad_mixed.astype(BF16)
        d_w_out = inner_rows(attended, d_att)
        d_attended = outer_cols(d_att, w_out_full).astype(BF16)
        d_queries, d_kv = attend_back(qkv_rows, ext, bias, d_attended, log_total)
        d_kv = halo_back(d_kv.reshape(hop_count + 1, tok_rows, 2 * kv_width), shards)
        d_kv = d_kv.astype(BF16).reshape(tok_rows, KV_HEADS // 2, 2, 2 * HEAD)
        d_qkv = jnp.concatenate(
            [
                d_queries,
                d_kv[:, :, 0].reshape(tok_rows, kv_width),
                d_kv[:, :, 1].reshape(tok_rows, kv_width),
            ],
            1,
        )
        d_w_qkv = inner_rows(normed_one, d_qkv)
        d_normed_one = outer_cols(d_qkv, w_qkv_full)
        _, norm_back = jax.vjp(rms_scale, layer_input, gain_pair[0])
        d_input_norm, d_gain_one = norm_back(d_normed_one)
        grad_stream = grad_mixed + d_input_norm
        dense_parts[layer_no] = [d_w_qkv.astype(BF16), d_w_out.astype(BF16)]
        small_parts[layer_no] = [
            d_router.astype(BF16),
            jnp.stack([d_gain_one, d_gain_two], 1).astype(BF16),
        ]
        collected[layer_no] = (
            d_experts[:, :in_rows, :].astype(F32),
            d_experts[:, in_rows:, :].astype(F32),
        )
    small = sum(small_parts, [])
    small.append(jnp.zeros((width, side - LAYERS * (experts_total + 2)), BF16))
    parts = sum(dense_parts, []) + [jnp.concatenate(small, 1)]
    d_dense = [part.reshape(shards, width // shards, -1) for part in parts]
    d_dense = reduce_dense(d_dense, shards, owners).astype(F32)
    for layer_no in range(LAYERS):
        at = layer_no * layer_columns
        d_main = d_dense[:, at : at + layer_columns]
        at = LAYERS * layer_columns + layer_no * (experts_total + 2)
        small = d_dense[:, at : at + experts_total + 2]
        collected[layer_no] = (
            small[:, experts_total:].T,
            d_main[:, :qkv_width],
            d_main[:, qkv_width:],
            small[:, :experts_total],
        ) + collected[layer_no]
    stacked = [
        jnp.stack([collected[layer_no][member] for layer_no in range(LAYERS)], 0)
        for member in range(6)
    ]
    results = [stream, grad_stream]
    results.extend(adam_update(gains, stacked[0], gains_first, gains_second))
    results.extend(adam_update(w_qkv, stacked[1], w_qkv_first, w_qkv_second))
    results.extend(adam_update(w_out, stacked[2], w_out_first, w_out_second))
    results.extend(adam_update(router, stacked[3], router_first, router_second))
    results.extend(adam_update(w_in, stacked[4], w_in_first, w_in_second))
    results.extend(adam_update(w_down, stacked[5], w_down_first, w_down_second))
    return tuple(results)


def solution(mesh):
    return jax.shard_map(
        on_device,
        mesh=mesh,
        in_specs=(
            P(("expert", "shard"), None),
            P(("expert", "shard"), None),
            P(),
            P(None, ("expert", "shard"), None),
            P(None, None, "shard"),
            P(None, None, "shard"),
            P(None, None, "shard"),
            P(None, "shard", None),
            P(None, "shard", None),
            P(None, "shard", None),
            P(None, "shard", None),
            P(None, "shard", None),
            P(None, "shard", None),
            P(None, "shard", None),
            P(None, "shard", None),
            P(None, "shard", None),
            P(None, "expert", "shard", None),
            P(None, "expert", "shard", None),
            P(None, "expert", "shard", None),
            P(None, "expert", "shard", None),
            P(None, "expert", "shard", None),
            P(None, "expert", "shard", None),
        ),
        out_specs=(
            P(("expert", "shard"), None),
            P(("expert", "shard"), None),
            P(None, None, "shard"),
            P(None, None, "shard"),
            P(None, None, "shard"),
            P(None, None, "shard"),
            P(None, "shard", None),
            P(None, "shard", None),
            P(None, "shard", None),
            P(None, "shard", None),
            P(None, "shard", None),
            P(None, "shard", None),
            P(None, "shard", None),
            P(None, "shard", None),
            P(None, "shard", None),
            P(None, "shard", None),
            P(None, "shard", None),
            P(None, "shard", None),
            P(None, "expert", "shard", None),
            P(None, "expert", "shard", None),
            P(None, "expert", "shard", None),
            P(None, "expert", "shard", None),
            P(None, "expert", "shard", None),
            P(None, "expert", "shard", None),
            P(None, "expert", "shard", None),
            P(None, "expert", "shard", None),
        ),
        check_vma=False,
    )
```

```python
import functools

import jax
import jax.numpy as jnp
from jax import lax
from jax.experimental import pallas as pl
from jax.experimental.pallas import tpu as pltpu
from jax.sharding import PartitionSpec as P

HEADS = 16
KV_HEADS = 8
HEAD = 64
TOP = 8
LAYERS = 2
WINDOW = 1024
SPAN = 8

norm_eps = 1e-05
masked_score = -1e30
beta_one = 0.9
beta_two = 0.95
adam_eps = 1e-08
learn_rate = 0.05
decay_rate = 0.1
adam_step = 10.0

F32 = jnp.float32
BF16 = jnp.bfloat16
MESH = pl.DeviceIdType.MESH
VMEM_LIMIT = 60 * 1024 * 1024


def rms_scale(values, gain_row):
    return (
        values * lax.rsqrt(jnp.mean(values * values, axis=-1, keepdims=True) + norm_eps) * gain_row
    )


def inner_rows(left_side, right_side):
    return lax.dot_general(
        left_side, right_side, (((0,), (0,)), ((), ())), preferred_element_type=F32
    )


def outer_cols(left_side, right_side):
    return lax.dot_general(
        left_side, right_side, (((1,), (1,)), ((), ())), preferred_element_type=F32
    )


def adam_update(weight, gradient, first_moment, second_moment):
    new_first = beta_one * first_moment + (1.0 - beta_one) * gradient
    new_second = beta_two * second_moment + (1.0 - beta_two) * gradient * gradient
    corr_first = new_first / (1.0 - beta_one**adam_step)
    corr_second = new_second / (1.0 - beta_two**adam_step)
    weight_step = -learn_rate * (
        corr_first / (jnp.sqrt(corr_second) + adam_eps) + decay_rate * weight
    )
    return [gradient, new_first, new_second, weight_step]


def signal(barrier, where):
    pl.semaphore_signal(barrier, inc=1, device_id=where, device_id_type=MESH)


def greet_chips(owners):
    e = lax.axis_index("expert")
    partner = e + 1 - 2 * lax.rem(e, 2)
    barrier = pltpu.get_barrier_semaphore()
    signal(barrier, {"expert": partner})
    for d in range(1, owners // 2):
        signal(barrier, {"expert": lax.rem(e + 2 * d, owners)})
    pl.semaphore_wait(barrier, owners // 2)
    return e, partner


def spread_kernel(owners, cuts, x_ref, o_ref, pair_send, pair_recv, far_send, far_recv):
    e, partner = greet_chips(owners)
    chips = owners // 2
    size = x_ref.shape[0] // cuts

    def pair_copy(d, cut):
        rows = pl.ds(cut * size, size)
        there = o_ref.at[lax.rem(e + owners - 2 * d, owners), rows]
        return pltpu.make_async_remote_copy(
            src_ref=x_ref.at[rows] if d == 0 else there,
            dst_ref=there,
            send_sem=pair_send.at[d, cut],
            recv_sem=pair_recv.at[d, cut],
            device_id={"expert": partner},
            device_id_type=MESH,
        )

    def far_copy(d, cut):
        rows = pl.ds(cut * size, size)
        return pltpu.make_async_remote_copy(
            src_ref=x_ref.at[rows],
            dst_ref=o_ref.at[e, rows],
            send_sem=far_send.at[d - 1, cut],
            recv_sem=far_recv.at[d - 1, cut],
            device_id={"expert": lax.rem(e + 2 * d, owners)},
            device_id_type=MESH,
        )

    for cut in range(cuts):
        for d in range(1, chips):
            far_copy(d, cut).start()
    for cut in range(cuts):
        pair_copy(0, cut).start()
    o_ref[e] = x_ref[...]
    for cut in range(cuts):
        for d in range(1, chips):
            far_copy(d, cut).wait_recv()
            pair_copy(d, cut).start()
    for cut in range(cuts):
        for d in range(chips):
            pair_copy(d, cut).wait()
        for d in range(1, chips):
            far_copy(d, cut).wait_send()


def spread(rows, owners, collective):
    dma = pltpu.SemaphoreType.DMA
    chips, cuts = owners // 2, 4
    return pl.pallas_call(
        functools.partial(spread_kernel, owners, cuts),
        out_shape=jax.ShapeDtypeStruct((owners,) + rows.shape, rows.dtype),
        in_specs=[pl.BlockSpec(memory_space=pltpu.VMEM)],
        out_specs=pl.BlockSpec(memory_space=pltpu.VMEM),
        scratch_shapes=[
            dma((chips, cuts)), dma((chips, cuts)), dma((chips - 1, cuts)), dma((chips - 1, cuts)),
        ],
        compiler_params=pltpu.CompilerParams(
            collective_id=collective, has_side_effects=True, vmem_limit_bytes=VMEM_LIMIT
        ),
        name="spread",
    )(rows)


def collect_kernel(
    owners, cuts, p_ref, o_ref, paired, going, came, pair_send, pair_recv, far_send, far_recv
):
    e, partner = greet_chips(owners)
    chips = owners // 2
    size = o_ref.shape[0] // cuts

    def pair_copy(d, cut):
        rows = pl.ds(cut * size, size)
        return pltpu.make_async_remote_copy(
            src_ref=p_ref.at[lax.rem(partner + 2 * d, owners), rows],
            dst_ref=paired.at[d, rows],
            send_sem=pair_send.at[d, cut],
            recv_sem=pair_recv.at[d, cut],
            device_id={"expert": partner},
            device_id_type=MESH,
        )

    def far_copy(d, cut):
        rows = pl.ds(cut * size, size)
        return pltpu.make_async_remote_copy(
            src_ref=going.at[d - 1, rows],
            dst_ref=came.at[d - 1, rows],
            send_sem=far_send.at[d - 1, cut],
            recv_sem=far_recv.at[d - 1, cut],
            device_id={"expert": lax.rem(e + 2 * d, owners)},
            device_id_type=MESH,
        )

    for cut in range(cuts):
        for d in range(1, chips):
            pair_copy(d, cut).start()
    for cut in range(cuts):
        pair_copy(0, cut).start()
    for cut in range(cuts):
        rows = pl.ds(cut * size, size)
        for d in range(1, chips):
            pair_copy(d, cut).wait_recv()
            going[d - 1, rows, :] = (
                p_ref[lax.rem(e + 2 * d, owners), rows, :].astype(F32)
                + paired[d, rows, :].astype(F32)
            ).astype(BF16)
            far_copy(d, cut).start()
    for cut in range(cuts):
        rows = pl.ds(cut * size, size)
        pair_copy(0, cut).wait_recv()
        total = p_ref[e, rows, :].astype(F32) + paired[0, rows, :].astype(F32)
        for d in range(1, chips):
            far_copy(d, cut).wait_recv()
            total = total + came[d - 1, rows, :].astype(F32)
        o_ref[rows, :] = total
    for cut in range(cuts):
        for d in range(chips):
            pair_copy(d, cut).wait_send()
        for d in range(1, chips):
            far_copy(d, cut).wait_send()


def collect(parts, collective):
    owners, rows, width = parts.shape
    dma = pltpu.SemaphoreType.DMA
    chips, cuts = owners // 2, 4
    return pl.pallas_call(
        functools.partial(collect_kernel, owners, cuts),
        out_shape=jax.ShapeDtypeStruct((rows, width), F32),
        in_specs=[pl.BlockSpec(memory_space=pltpu.VMEM)],
        out_specs=pl.BlockSpec(memory_space=pltpu.VMEM),
        scratch_shapes=[
            pltpu.VMEM((chips, rows, width), parts.dtype),
            pltpu.VMEM((chips - 1, rows, width), parts.dtype),
            pltpu.VMEM((chips - 1, rows, width), parts.dtype),
            dma((chips, cuts)), dma((chips, cuts)), dma((chips - 1, cuts)), dma((chips - 1, cuts)),
        ],
        compiler_params=pltpu.CompilerParams(
            collective_id=collective, has_side_effects=True, vmem_limit_bytes=VMEM_LIMIT
        ),
        name="collect",
    )(parts)


def ring_shard(place, count):
    back = lax.div(place, count // 2)
    return (1 - back) * 2 * place + back * (2 * (count - 1 - place) + 1)


def ring_place(shard, count):
    odd, pair = lax.rem(shard, 2), lax.div(shard, 2)
    return (1 - odd) * pair + odd * (count - 1 - pair)


def gather_dense_kernel(
    n, owners, rows, x_ref, o_ref,
    ring_send, ring_recv, pair_send, pair_recv, far_send, far_recv, own_sem,
):
    e, s = lax.axis_index("expert"), lax.axis_index("shard")
    partner = e + 1 - 2 * lax.rem(e, 2)
    chips = owners // 2
    p = ring_place(s, n)
    ways = (ring_shard(lax.rem(p + 1, n), n), ring_shard(lax.rem(p + n - 1, n), n))
    barrier = pltpu.get_barrier_semaphore()
    signal(barrier, {"expert": partner})
    signal(barrier, {"shard": ways[0]})
    signal(barrier, {"shard": ways[1]})
    for d in range(1, chips):
        signal(barrier, {"expert": lax.rem(e + 2 * d, owners)})
    pl.semaphore_wait(barrier, 2 + chips)
    half, wide = rows // 2, x_ref.shape[1] // owners

    def columns(owner):
        return pl.ds(pl.multiple_of(owner * wide, 128), wide)

    def region(way, k, owner):
        block = ring_shard(lax.rem(p + (n - k if way == 0 else k), n), n)
        return o_ref.at[block, pl.ds(way * half, half), columns(owner)]

    def ring_copy(way, k, src):
        return pltpu.make_async_remote_copy(
            src_ref=src,
            dst_ref=region(way, k, e),
            send_sem=ring_send.at[way, k],
            recv_sem=ring_recv.at[way, k],
            device_id={"shard": ways[way]},
            device_id_type=MESH,
        )

    def far_copy(d, way, k):
        return pltpu.make_async_remote_copy(
            src_ref=region(way, k, e),
            dst_ref=region(way, k, e),
            send_sem=far_send.at[d - 1, way, k - 1],
            recv_sem=far_recv.at[d - 1, way, k - 1],
            device_id={"expert": lax.rem(e + 2 * d, owners)},
            device_id_type=MESH,
        )

    def pair_copy(d, way, k):
        there = region(way, k, lax.rem(e + owners - 2 * d, owners))
        return pltpu.make_async_remote_copy(
            src_ref=there,
            dst_ref=there,
            send_sem=pair_send.at[d, way, k - 1],
            recv_sem=pair_recv.at[d, way, k - 1],
            device_id={"expert": partner},
            device_id_type=MESH,
        )

    def hand_on(k):
        for way in range(2):
            for d in range(1, chips):
                far_copy(d, way, k).wait_recv()
                pair_copy(d, way, k).start()

    for way in range(2):
        ring_copy(way, 0, x_ref.at[pl.ds(way * half, half), columns(e)]).start()
    own = pltpu.make_async_copy(x_ref, o_ref.at[s], own_sem)
    own.start()

    def step(k, carry):
        for way in range(2):
            came = region(way, k, e)
            ring_copy(way, k - 1, came).wait_recv()

            @pl.when(k < n - 1)
            def _():
                ring_copy(way, k, came).start()

            for d in range(1, chips):
                far_copy(d, way, k).start()
            pair_copy(0, way, k).start()

        @pl.when(k > 1)
        def _():
            hand_on(k - 1)

        return carry

    lax.fori_loop(1, n, step, 0)
    hand_on(n - 1)

    def finish(k, carry):
        for way in range(2):
            ring_copy(way, k - 1, region(way, k, e)).wait_send()
            for d in range(chips):
                pair_copy(d, way, k).wait()
            for d in range(1, chips):
                far_copy(d, way, k).wait_send()
        return carry

    lax.fori_loop(1, n, finish, 0)
    own.wait()


def gather_dense(piece, n, owners):
    rows, columns = piece.shape
    dma = pltpu.SemaphoreType.DMA
    chips = owners // 2
    return pl.pallas_call(
        functools.partial(gather_dense_kernel, n, owners, rows),
        out_shape=jax.ShapeDtypeStruct((n, rows, columns), piece.dtype),
        in_specs=[pl.BlockSpec(memory_space=pltpu.VMEM)],
        out_specs=pl.BlockSpec(memory_space=pl.ANY),
        scratch_shapes=[
            dma((2, n - 1)), dma((2, n - 1)), dma((chips, 2, n - 1)), dma((chips, 2, n - 1)),
            dma((chips - 1, 2, n - 1)), dma((chips - 1, 2, n - 1)), dma,
        ],
        compiler_params=pltpu.CompilerParams(
            collective_id=3, has_side_effects=True, vmem_limit_bytes=VMEM_LIMIT
        ),
        name="gather_dense",
    )(piece)


def reduce_dense_kernel(
    n, owners, rows, places, *refs,
):
    g_refs = refs[: len(places)]
    (
        h_ref, o_ref, h_out, h_came, h_going, h_send, h_recv, paired, came, going, crossed, last_in, pair_send, pair_recv, ring_send,
        ring_recv, cross_send, cross_recv, last_send, last_recv,
    ) = refs[len(places) :]
    e, s = lax.axis_index("expert"), lax.axis_index("shard")
    core, x = lax.rem(e, 2), lax.div(e, 2)
    partner = e + 1 - 2 * core
    columns = owners // 2
    p = ring_place(s, n)
    ways = (ring_shard(lax.rem(p + 1, n), n), ring_shard(lax.rem(p + n - 1, n), n))
    barrier = pltpu.get_barrier_semaphore()
    signal(barrier, {"expert": partner})
    signal(barrier, {"shard": ways[0]})
    signal(barrier, {"shard": ways[1]})
    for d in range(1, columns):
        signal(barrier, {"expert": lax.rem(e + 2 * d, owners)})
    pl.semaphore_wait(barrier, 3 + columns - 1)
    half, quarter = rows // 2, rows // 4

    def mine(way):
        return pl.ds(pl.multiple_of(core * half + way * quarter, quarter), quarter)

    def block(way, k):
        return ring_shard(lax.rem(p + (2 * n - 1 - k if way == 0 else k + 1), n), n)

    def pair_copy(k, i):
        b = block(0, k)
        at, wide = places[i]
        return pltpu.make_async_remote_copy(
            src_ref=g_refs[i].at[b, pl.ds(pl.multiple_of((1 - core) * half, half), half)],
            dst_ref=paired.at[b, :, pl.ds(at, wide)],
            send_sem=pair_send.at[i, b],
            recv_sem=pair_recv.at[i, b],
            device_id={"expert": partner},
            device_id_type=MESH,
        )

    def ring_copy(way, k):
        return pltpu.make_async_remote_copy(
            src_ref=going.at[way, k],
            dst_ref=came.at[way, k],
            send_sem=ring_send.at[way, k],
            recv_sem=ring_recv.at[way, k],
            device_id={"shard": ways[way]},
            device_id_type=MESH,
        )

    def put(target, way, b, more=None):
        for g_ref, (at, wide) in zip(g_refs, places):
            total = g_ref[b, mine(way), :].astype(F32) + paired[
                b, way * quarter : (way + 1) * quarter, at : at + wide
            ].astype(F32)
            if more is not None:
                total = total + more[:, at : at + wide].astype(F32)
            target[:, at : at + wide] = total.astype(BF16)

    few = h_ref.shape[1] // 2

    def solo_copy(way, k, src):
        return pltpu.make_async_remote_copy(
            src_ref=src,
            dst_ref=h_came.at[way, k],
            send_sem=h_send.at[way, k],
            recv_sem=h_recv.at[way, k],
            device_id={"shard": ways[way]},
            device_id_type=MESH,
        )

    def solo(way, b):
        return h_ref.at[b, pl.ds(way * few, few)]

    order = []
    for k in range(n):
        for place in (k, n - 2 - k):
            place = place % n
            if place not in order:
                order.append(place)
    every = range(len(places))
    for way in range(2):
        solo_copy(way, 0, solo(way, block(way, 0))).start()
    for k in order:
        for i in every:
            pair_copy(k, i).start()
    for k in order[:2]:
        for i in every:
            pair_copy(k, i).wait_recv()
    for way in range(2):
        put(going.at[way, 0], way, block(way, 0))
        ring_copy(way, 0).start()
    for k in order[2:]:
        for i in every:
            pair_copy(k, i).wait_recv()

    def step(k, carry):
        for way in range(2):
            ring_copy(way, k - 1).wait_recv()
            put(going.at[way, k], way, block(way, k), came.at[way, k - 1])
            ring_copy(way, k).start()
        for way in range(2):
            solo_copy(way, k - 1, h_going.at[way, k]).wait_recv()
            h_going[way, k] = (
                h_came[way, k - 1].astype(F32) + solo(way, block(way, k))[...].astype(F32)
            ).astype(BF16)
            solo_copy(way, k, h_going.at[way, k]).start()
        return carry

    lax.fori_loop(1, n - 1, step, 0)
    for way in range(2):
        ring_copy(way, n - 2).wait_recv()
        put(
            crossed.at[x, pl.ds(way * quarter, quarter)], way, s, came.at[way, n - 2]
        )

    for way in range(2):
        solo_copy(way, n - 2, h_going.at[way, 0]).wait_recv()
        h_out[way * few : (way + 1) * few] = (
            h_came[way, n - 2].astype(F32) + solo(way, s)[...].astype(F32)
        ).astype(BF16)

    def cross_copy(d):
        return pltpu.make_async_remote_copy(
            src_ref=crossed.at[x],
            dst_ref=crossed.at[x],
            send_sem=cross_send.at[d - 1],
            recv_sem=cross_recv.at[d - 1],
            device_id={"expert": lax.rem(e + 2 * d, owners)},
            device_id_type=MESH,
        )

    for d in range(1, columns):
        cross_copy(d).start()
    for d in range(1, columns):
        cross_copy(d).wait()
    total = crossed[0].astype(F32)
    for d in range(1, columns):
        total = total + crossed[d].astype(F32)
    here = pl.ds(pl.multiple_of(core * half, half), half)
    o_ref[here, :] = total.astype(BF16)
    last = pltpu.make_async_remote_copy(
        src_ref=o_ref.at[here],
        dst_ref=last_in,
        send_sem=last_send,
        recv_sem=last_recv,
        device_id={"expert": partner},
        device_id_type=MESH,
    )
    last.start()
    for k in order:
        for i in every:
            pair_copy(k, i).wait_send()

    def finish(k, carry):
        for way in range(2):
            ring_copy(way, k).wait_send()
            solo_copy(way, k, h_going.at[way, k]).wait_send()
        return carry

    lax.fori_loop(0, n - 1, finish, 0)
    last.wait()
    o_ref[pl.ds(pl.multiple_of((1 - core) * half, half), half), :] = last_in[...]


def reduce_dense(grads, downs, n, owners):
    rows = grads[0].shape[1]
    places, columns = [], 0
    for grad in grads:
        places.append((columns, grad.shape[2]))
        columns += grad.shape[2]
    dma = pltpu.SemaphoreType.DMA
    across = owners // 2
    some = (downs.shape[1] // 2,) + downs.shape[2:]
    return pl.pallas_call(
        functools.partial(reduce_dense_kernel, n, owners, rows, tuple(places)),
        out_shape=[
            jax.ShapeDtypeStruct((rows, columns), BF16),
            jax.ShapeDtypeStruct(downs.shape[1:], BF16),
        ],
        in_specs=[pl.BlockSpec(memory_space=pltpu.VMEM)] * (len(places) + 1),
        out_specs=[pl.BlockSpec(memory_space=pltpu.VMEM)] * 2,
        scratch_shapes=[
            pltpu.VMEM((2, n - 1) + some, BF16),
            pltpu.VMEM((2, n - 1) + some, BF16),
            dma((2, n - 1)),
            dma((2, n - 1)),
            pltpu.VMEM((n, rows // 2, columns), BF16),
            pltpu.VMEM((2, n - 1, rows // 4, columns), BF16),
            pltpu.VMEM((2, n - 1, rows // 4, columns), BF16),
            pltpu.VMEM((across, rows // 2, columns), BF16),
            pltpu.VMEM((rows // 2, columns), BF16),
            dma((len(places), n)), dma((len(places), n)), dma((2, n - 1)), dma((2, n - 1)),
            dma((across - 1,)), dma((across - 1,)), dma, dma,
        ],
        compiler_params=pltpu.CompilerParams(
            collective_id=4, has_side_effects=True, vmem_limit_bytes=VMEM_LIMIT
        ),
        name="reduce_dense",
    )(*grads, downs)


def halo_links(n, s):
    odd = lax.rem(s, 2)
    return odd, s + 1 - 2 * odd, s + 2 < n, s >= 2


def halo_barrier(s, odd, mate, ahead, behind, sends_back):
    barrier = pltpu.get_barrier_semaphore()
    even = odd == 0
    to_ahead, to_behind = (ahead, behind) if not sends_back else (behind, ahead)
    step = -2 if not sends_back else 2
    mate_copies = (odd == 1) | behind if not sends_back else even | behind
    to_mate = even | behind if not sends_back else (odd == 1) | behind

    @pl.when(to_behind)
    def _():
        signal(barrier, {"shard": s + step})

    @pl.when(mate_copies)
    def _():
        signal(barrier, {"shard": mate})

    @pl.when(to_ahead & to_mate)
    def _():
        pl.semaphore_wait(barrier, 2)

    @pl.when(to_ahead != to_mate)
    def _():
        pl.semaphore_wait(barrier, 1)


def halo_kernel(n, rows, cuts, kv_ref, o_ref, sends, recvs, own_sem):
    s = lax.axis_index("shard")
    odd, mate, ahead, behind = halo_links(n, s)
    even = odd == 0
    size = rows // cuts

    def copy(kind, cut, src, slot, where):
        return pltpu.make_async_remote_copy(
            src_ref=src.at[pl.ds(cut * size, size)],
            dst_ref=o_ref.at[slot, pl.ds(cut * size, size)],
            send_sem=sends.at[kind, cut],
            recv_sem=recvs.at[kind, cut],
            device_id={"shard": where},
            device_id_type=MESH,
        )

    halo_barrier(s, odd, mate, ahead, behind, False)
    from_odd = (o_ref.at[2], o_ref.at[0])
    from_even = (kv_ref, o_ref.at[2])
    for cut in range(cuts):

        @pl.when(ahead)
        def _():
            copy(0, cut, kv_ref, 2, s + 2).start()

        @pl.when(even)
        def _():
            copy(2, cut, kv_ref, 3, mate).start()

    o_ref[4] = kv_ref[...]
    for slot in range(4):

        @pl.when(s < 4 - slot)
        def _():
            o_ref[slot] = jnp.zeros_like(o_ref[slot])

    for cut in range(cuts):

        @pl.when(behind)
        def _():
            copy(0, cut, kv_ref, 2, s).wait_recv()

        @pl.when(behind & ahead)
        def _():
            copy(1, cut, o_ref.at[2], 0, s + 2).start()

        @pl.when(behind & (odd == 1))
        def _():
            copy(2, cut, from_odd[0], 3, mate).start()

        @pl.when(behind & even)
        def _():
            copy(3, cut, from_even[1], 1, mate).start()

    for cut in range(cuts):

        @pl.when(s >= 4)
        def _():
            copy(1, cut, o_ref.at[2], 0, s).wait_recv()

        @pl.when((s >= 4) & (odd == 1))
        def _():
            copy(3, cut, from_odd[1], 1, mate).start()

    for cut in range(cuts):

        @pl.when(s >= 1)
        def _():
            copy(2, cut, kv_ref, 3, mate).wait_recv()

        @pl.when(s >= 3)
        def _():
            copy(3, cut, kv_ref, 1, mate).wait_recv()

        @pl.when(ahead)
        def _():
            copy(0, cut, kv_ref, 2, s).wait_send()

        @pl.when(behind & ahead)
        def _():
            copy(1, cut, kv_ref, 0, s).wait_send()

        @pl.when(even | behind)
        def _():
            copy(2, cut, kv_ref, 3, mate).wait_send()

        @pl.when((even & behind) | ((odd == 1) & (s >= 4)))
        def _():
            copy(3, cut, kv_ref, 1, mate).wait_send()


def halo(kv, n, slots):
    rows, columns = kv.shape
    dma = pltpu.SemaphoreType.DMA
    cuts = 2
    return pl.pallas_call(
        functools.partial(halo_kernel, n, rows, cuts),
        out_shape=jax.ShapeDtypeStruct((slots, rows, columns), kv.dtype),
        in_specs=[pl.BlockSpec(memory_space=pltpu.VMEM)],
        out_specs=pl.BlockSpec(memory_space=pltpu.VMEM),
        scratch_shapes=[dma((4, cuts)), dma((4, cuts)), dma],
        compiler_params=pltpu.CompilerParams(
            collective_id=5, has_side_effects=True, vmem_limit_bytes=VMEM_LIMIT
        ),
        name="halo",
    )(kv)


def halo_back_kernel(n, rows, cuts, q_ref, g_ref, o_ref, own, came, total, sends, recvs):
    s = lax.axis_index("shard")
    odd, mate, ahead, behind = halo_links(n, s)
    even = odd == 0
    size = rows // cuts

    def copy(kind, cut, src, where):
        return pltpu.make_async_remote_copy(
            src_ref=src.at[pl.ds(cut * size, size)],
            dst_ref=came.at[kind, pl.ds(cut * size, size)],
            send_sem=sends.at[kind, cut],
            recv_sem=recvs.at[kind, cut],
            device_id={"shard": where},
            device_id_type=MESH,
        )

    def there(ref, cut, value=None):
        here = pl.ds(cut * size, size)
        return ref[here, :].astype(F32)

    def put(here):
        pair, after = 2 * HEAD, q_ref.shape[1]
        for j in range(KV_HEADS // 2):
            for part in range(2):
                at = after + part * KV_HEADS * HEAD + j * pair
                o_ref[here, at : at + pair] = total[
                    :, (2 * j + part) * pair : (2 * j + part + 1) * pair
                ].astype(BF16)

    halo_barrier(s, odd, mate, ahead, behind, True)
    width = q_ref.shape[1]
    for cut in range(cuts):

        @pl.when(s >= 3)
        def _():
            copy(3, cut, g_ref.at[1], mate).start()

        @pl.when(s >= 1)
        def _():
            copy(2, cut, g_ref.at[3], mate).start()

    o_ref[:, :width] = q_ref[...]
    for cut in range(cuts):
        here = pl.ds(cut * size, size)

        @pl.when((odd == 1) & (s >= 4))
        def _():
            copy(3, cut, g_ref.at[1], mate).wait_recv()
            own[0, here, :] = (there(g_ref.at[0], cut) + there(came.at[3], cut)).astype(BF16)

        @pl.when((odd == 1) & (s >= 4))
        def _():
            copy(1, cut, own.at[0], s - 2).start()

        @pl.when(even & (s >= 4))
        def _():
            copy(1, cut, g_ref.at[0], s - 2).start()

    for cut in range(cuts):
        here = pl.ds(cut * size, size)

        @pl.when((odd == 1) & behind)
        def _():
            copy(2, cut, g_ref.at[3], mate).wait_recv()
            own[1, here, :] = (there(g_ref.at[2], cut) + there(came.at[2], cut)).astype(BF16)

        @pl.when(even & behind)
        def _():
            copy(3, cut, g_ref.at[1], mate).wait_recv()
            own[1, here, :] = (there(g_ref.at[2], cut) + there(came.at[3], cut)).astype(BF16)

        @pl.when(behind & ahead)
        def _():
            copy(1, cut, g_ref.at[0], s).wait_recv()
            own[1, here, :] = (there(own.at[1], cut) + there(came.at[1], cut)).astype(BF16)

        @pl.when(behind)
        def _():
            copy(0, cut, own.at[1], s - 2).start()

    for cut in range(cuts):
        here = pl.ds(cut * size, size)
        total[...] = there(g_ref.at[4], cut)

        @pl.when(even)
        def _():
            copy(2, cut, g_ref.at[3], mate).wait_recv()
            total[...] += there(came.at[2], cut)

        @pl.when(ahead)
        def _():
            copy(0, cut, own.at[1], s).wait_recv()
            total[...] += there(came.at[0], cut)

        put(here)

        @pl.when(s >= 3)
        def _():
            copy(3, cut, g_ref.at[1], mate).wait_send()

        @pl.when(s >= 1)
        def _():
            copy(2, cut, g_ref.at[3], mate).wait_send()

        @pl.when(s >= 4)
        def _():
            copy(1, cut, g_ref.at[0], mate).wait_send()

        @pl.when(behind)
        def _():
            copy(0, cut, own.at[1], mate).wait_send()


def halo_back(d_queries, grads, n):
    slots, rows, columns = grads.shape
    dma = pltpu.SemaphoreType.DMA
    cuts = 2
    return pl.pallas_call(
        functools.partial(halo_back_kernel, n, rows, cuts),
        out_shape=jax.ShapeDtypeStruct((rows, d_queries.shape[1] + columns), BF16),
        in_specs=[pl.BlockSpec(memory_space=pltpu.VMEM)] * 2,
        out_specs=pl.BlockSpec(memory_space=pltpu.VMEM),
        scratch_shapes=[
            pltpu.VMEM((2, rows, columns), BF16),
            pltpu.VMEM((4, rows, columns), BF16),
            pltpu.VMEM((rows // cuts, columns), F32),
            dma((4, cuts)),
            dma((4, cuts)),
        ],
        compiler_params=pltpu.CompilerParams(
            collective_id=6, has_side_effects=True, vmem_limit_bytes=VMEM_LIMIT
        ),
        name="halo_back",
    )(d_queries, grads)


def attend_kernel(q_ref, k_ref, v_ref, bias_ref, o_ref, total_ref):
    for h in range(q_ref.shape[1] // HEAD):
        at = pl.ds(h * HEAD, HEAD)
        kv_at = pl.ds(h // (HEADS // KV_HEADS) * HEAD, HEAD)
        query = q_ref[:, at] * jnp.asarray(HEAD**-0.5, BF16)
        scores = outer_cols(k_ref[:, kv_at], query) + bias_ref[...]
        top = jnp.max(scores, axis=0, keepdims=True)
        powers = jnp.exp(scores - top)
        total = jnp.sum(powers, axis=0, keepdims=True)
        value = inner_rows(v_ref[:, kv_at], powers.astype(BF16)) / total
        o_ref[:, at] = value.T.astype(BF16)
        total_ref[0, h : h + 1, :] = top + jnp.log(total)


def attention_specs(tok_rows, key_count):
    span = 2 * HEAD
    groups = HEADS // KV_HEADS
    steps = KV_HEADS // 2
    return steps, [
        pl.BlockSpec((tok_rows, groups * span), lambda j: (0, j)),
        pl.BlockSpec((key_count, span), lambda j: (0, j)),
        pl.BlockSpec((key_count, span), lambda j: (0, j + steps)),
        pl.BlockSpec((key_count, tok_rows), lambda j: (0, 0)),
    ]


def attend(qkv_rows, ext, bias):
    key_count, tok_rows = bias.shape
    steps, specs = attention_specs(tok_rows, key_count)
    return pl.pallas_call(
        attend_kernel,
        grid=(steps,),
        in_specs=specs,
        out_specs=[specs[0], pl.BlockSpec((1, 8, tok_rows), lambda j: (j, 0, 0))],
        out_shape=[
            jax.ShapeDtypeStruct((tok_rows, HEADS * HEAD), BF16),
            jax.ShapeDtypeStruct((steps, 8, tok_rows), F32),
        ],
        compiler_params=pltpu.CompilerParams(vmem_limit_bytes=VMEM_LIMIT),
        cost_estimate=pl.CostEstimate(
            flops=4 * HEADS * HEAD * tok_rows * key_count,
            bytes_accessed=4 * key_count * tok_rows + 4 * key_count * KV_HEADS * HEAD,
            transcendentals=HEADS * tok_rows * key_count,
        ),
        name="attend",
    )(qkv_rows, ext, ext, bias)


def attend_back_kernel(
    q_ref, k_ref, v_ref, bias_ref, d_ref, total_ref, d_query_ref, d_kv_ref
):
    groups = HEADS // KV_HEADS
    scale = jnp.asarray(HEAD**-0.5, BF16)
    span = k_ref.shape[1]
    for kv in range(span // HEAD):
        kv_at = pl.ds(kv * HEAD, HEAD)
        key, value = k_ref[:, kv_at], v_ref[:, kv_at]
        d_key = d_value = None
        for h in range(kv * groups, (kv + 1) * groups):
            at = pl.ds(h * HEAD, HEAD)
            query = q_ref[:, at] * scale
            d_out = d_ref[:, at]
            scores = outer_cols(key, query) + bias_ref[...]
            probs = jnp.exp(scores - total_ref[0, h : h + 1, :])
            d_probs = outer_cols(value, d_out)
            mean_d = jnp.sum(probs * d_probs, axis=0, keepdims=True)
            d_scores = (probs * (d_probs - mean_d)).astype(BF16)
            d_query = inner_rows(key, d_scores) * (HEAD**-0.5)
            d_query_ref[:, at] = d_query.T.astype(BF16)
            more_key = jnp.dot(d_scores, query, preferred_element_type=F32)
            more_value = jnp.dot(probs.astype(BF16), d_out, preferred_element_type=F32)
            d_key = more_key if d_key is None else d_key + more_key
            d_value = more_value if d_value is None else d_value + more_value
        d_kv_ref[:, kv * HEAD : (kv + 1) * HEAD] = d_key.astype(BF16)
        d_kv_ref[:, span + kv * HEAD : span + (kv + 1) * HEAD] = d_value.astype(BF16)


def attend_back(qkv_rows, ext, bias, d_attended, totals):
    key_count, tok_rows = bias.shape
    steps, specs = attention_specs(tok_rows, key_count)
    return pl.pallas_call(
        attend_back_kernel,
        grid=(steps,),
        in_specs=specs + [specs[0], pl.BlockSpec((1, 8, tok_rows), lambda j: (j, 0, 0))],
        out_specs=[specs[0], pl.BlockSpec((key_count, 4 * HEAD), lambda j: (0, j))],
        out_shape=[
            jax.ShapeDtypeStruct((tok_rows, HEADS * HEAD), BF16),
            jax.ShapeDtypeStruct((key_count, 2 * KV_HEADS * HEAD), BF16),
        ],
        compiler_params=pltpu.CompilerParams(vmem_limit_bytes=VMEM_LIMIT),
        cost_estimate=pl.CostEstimate(
            flops=10 * HEADS * HEAD * tok_rows * key_count,
            bytes_accessed=4 * key_count * tok_rows + 8 * key_count * KV_HEADS * HEAD,
            transcendentals=HEADS * tok_rows * key_count,
        ),
        name="attend_back",
    )(qkv_rows, ext, ext, bias, d_attended, totals)


def column_of(extra, index, experts_total):
    lanes = lax.broadcasted_iota(jnp.int32, extra.shape, 1)
    hit = (lanes == index) | (lanes == index + experts_total)
    return jnp.sum(jnp.where(hit, extra.astype(F32), 0.0), axis=1, keepdims=True)


def ffn_forward_kernel(
    tile, width, in_rows, experts_total, first_ref, x_ref, w_ref, part_ref, gate_up_ref, acc
):
    e = pl.program_id(0)
    w_in = w_ref[:, 0, :in_rows, :].reshape(width, w_ref.shape[-1])
    w_down = w_ref[:, 0, in_rows:, :].reshape(-1, width)
    half = w_in.shape[1] // 2
    index = first_ref[0] + e
    count = x_ref.shape[0] // tile
    for t in range(count):
        rows = pl.ds(t * tile, tile)
        gate_up = jnp.dot(x_ref[rows, :width], w_in, preferred_element_type=F32)
        gate, up = gate_up[:, :half], gate_up[:, half:]
        gate_up_ref[0, rows, :] = gate_up.astype(BF16)
        weight = column_of(x_ref[rows, width:], index, experts_total)
        hidden = (gate * jax.nn.sigmoid(gate) * up * weight).astype(BF16)
        out = jnp.dot(hidden, w_down, preferred_element_type=F32)

        @pl.when(e == 0)
        def _():
            acc[rows, :] = out

        @pl.when(e > 0)
        def _():
            acc[rows, :] += out

        @pl.when(e == pl.num_programs(0) - 1)
        def _():
            part_ref[rows, :] = acc[rows, :].astype(BF16)


def ffn_forward(first, x_all, w_all, experts_total, in_rows):
    shards, local, piece, inner = w_all.shape
    tokens, wide = x_all.shape
    width = in_rows * shards
    return pl.pallas_call(
        functools.partial(ffn_forward_kernel, 256, width, in_rows, experts_total),
        grid_spec=pltpu.PrefetchScalarGridSpec(
            num_scalar_prefetch=1,
            grid=(local,),
            in_specs=[
                pl.BlockSpec((tokens, wide), lambda e, f: (0, 0)),
                pl.BlockSpec((shards, 1, piece, inner), lambda e, f: (0, e, 0, 0)),
            ],
            out_specs=[
                pl.BlockSpec((tokens, width), lambda e, f: (0, 0)),
                pl.BlockSpec((1, tokens, inner), lambda e, f: (e, 0, 0)),
            ],
            scratch_shapes=[pltpu.VMEM((tokens, width), F32)],
        ),
        out_shape=[
            jax.ShapeDtypeStruct((tokens, width), BF16),
            jax.ShapeDtypeStruct((local, tokens, inner), BF16),
        ],
        compiler_params=pltpu.CompilerParams(vmem_limit_bytes=VMEM_LIMIT),
        cost_estimate=pl.CostEstimate(
            flops=2 * local * tokens * width * (inner + inner // 2),
            bytes_accessed=2 * (w_all.size + local * tokens * inner + 2 * tokens * wide),
            transcendentals=0,
        ),
        name="ffn_forward",
    )(first, x_all, w_all)


def ffn_backward_kernel(
    tile,
    width,
    in_rows,
    experts_total,
    first_ref,
    x_ref,
    g_ref,
    gate_up_ref,
    w_ref,
    part_ref,
    *refs,
):
    acc, d_gate_up, hidden_all, d_weights = refs[-4:]
    grad_in = refs[0].at[:, 0, :in_rows]
    grad_down = refs[0].at[:, 0, in_rows:] if len(refs) == 5 else refs[1].at[:, 0]
    e = pl.program_id(0)
    inner = w_ref.shape[-1]
    w_in = w_ref[:, 0, :in_rows, :].reshape(width, inner)
    w_down = w_ref[:, 0, in_rows:, :].reshape(-1, width)
    half = inner // 2
    index = first_ref[0] + e
    tokens = x_ref.shape[0]
    last = pl.num_programs(0) - 1
    for t in range(tokens // tile):
        rows = pl.ds(t * tile, tile)
        d_plain = outer_cols(g_ref[rows, :], w_down)
        gate = gate_up_ref[0, rows, :half].astype(F32)
        up = gate_up_ref[0, rows, half:].astype(F32)
        weight = column_of(x_ref[rows, width:], index, experts_total)
        sig = jax.nn.sigmoid(gate)
        silu = gate * sig
        hidden = silu * up
        d_weight = jnp.sum(hidden * d_plain, axis=1, keepdims=True)
        d_hidden = d_plain * weight
        hidden_all[rows, :] = (hidden * weight).astype(BF16)
        d_gate_up[rows, :half] = (d_hidden * up * sig * (1.0 + gate * (1.0 - sig))).astype(BF16)
        d_gate_up[rows, half:] = (d_hidden * silu).astype(BF16)
        lanes = lax.broadcasted_iota(jnp.int32, (tile, d_weights.shape[1]), 1)
        high = d_weight.astype(BF16).astype(F32)
        columns = jnp.where(
            lanes == index, high, jnp.where(lanes == index + experts_total, d_weight - high, 0.0)
        )
        out = outer_cols(d_gate_up[rows, :], w_in)

        @pl.when(e == 0)
        def _():
            acc[rows, :] = out
            d_weights[rows, :] = columns

        @pl.when(e > 0)
        def _():
            acc[rows, :] += out
            d_weights[rows, :] += columns

        @pl.when(e == last)
        def _():
            part_ref[rows, :width] = acc[rows, :].astype(BF16)
            part_ref[rows, width:] = d_weights[rows, :].astype(BF16)

    grad_in[...] = (
        inner_rows(x_ref[:, :width], d_gate_up[...]).astype(BF16).reshape(-1, in_rows, inner)
    )
    grad_down[...] = (
        inner_rows(hidden_all[...], g_ref[...])
        .astype(BF16)
        .reshape(-1, w_ref.shape[2] - in_rows, width)
    )


def ffn_backward(first, x_all, g_all, gate_up, w_all, experts_total, in_rows, apart):
    shards, local, piece, inner = w_all.shape
    pieces = (in_rows, piece - in_rows) if apart else (piece,)
    tokens, wide = x_all.shape
    width = in_rows * shards
    return pl.pallas_call(
        functools.partial(ffn_backward_kernel, 256, width, in_rows, experts_total),
        grid_spec=pltpu.PrefetchScalarGridSpec(
            num_scalar_prefetch=1,
            grid=(local,),
            in_specs=[
                pl.BlockSpec((tokens, wide), lambda e, f: (0, 0)),
                pl.BlockSpec((tokens, width), lambda e, f: (0, 0)),
                pl.BlockSpec((1, tokens, inner), lambda e, f: (e, 0, 0)),
                pl.BlockSpec((shards, 1, piece, inner), lambda e, f: (0, e, 0, 0)),
            ],
            out_specs=[
                pl.BlockSpec((tokens, wide), lambda e, f: (0, 0)),
            ]
            + [pl.BlockSpec((shards, 1, some, inner), lambda e, f: (0, e, 0, 0)) for some in pieces],
            scratch_shapes=[
                pltpu.VMEM((tokens, width), F32),
                pltpu.VMEM((tokens, inner), BF16),
                pltpu.VMEM((tokens, inner // 2), BF16),
                pltpu.VMEM((tokens, wide - width), F32),
            ],
        ),
        out_shape=[
            jax.ShapeDtypeStruct((tokens, wide), BF16),
        ]
        + [jax.ShapeDtypeStruct((shards, local, some, inner), BF16) for some in pieces],
        compiler_params=pltpu.CompilerParams(vmem_limit_bytes=VMEM_LIMIT),
        cost_estimate=pl.CostEstimate(
            flops=4 * local * tokens * width * (inner + inner // 2),
            bytes_accessed=2 * (2 * w_all.size + local * tokens * inner + 4 * tokens * wide),
            transcendentals=0,
        ),
        name="ffn_backward",
    )(first, x_all, g_all, gate_up, w_all)


def on_device(
    hidden_in,
    cotangent,
    doc_lengths,
    routes,
    gains,
    gains_first,
    gains_second,
    w_qkv,
    w_qkv_first,
    w_qkv_second,
    w_out,
    w_out_first,
    w_out_second,
    router,
    router_first,
    router_second,
    w_in,
    w_in_first,
    w_in_second,
    w_down,
    w_down_first,
    w_down_second,
):
    tok_rows, width = hidden_in.shape
    owners = lax.axis_size("expert")
    shards = lax.axis_size("shard")
    local_experts = w_in.shape[1]
    in_rows = w_in.shape[2]
    experts_total = local_experts * owners
    seq_len = tok_rows * SPAN
    hop_count = min(-(-WINDOW // tok_rows), SPAN - 1)
    key_count = (hop_count + 1) * tok_rows
    q_width = HEADS * HEAD
    kv_width = KV_HEADS * HEAD
    qkv_width = q_width + 2 * kv_width
    extra = -(-2 * experts_total // 128) * 128
    my_owner = lax.axis_index("expert")
    first_expert = my_owner * local_experts
    first_array = first_expert.astype(jnp.int32).reshape(1)
    row_start = (my_owner * shards + lax.axis_index("shard")) * tok_rows
    my_seq = row_start // seq_len
    doc_ends = jnp.cumsum(lax.dynamic_slice_in_dim(doc_lengths, my_seq, 1, 0)[0])
    query_rows = row_start + jnp.arange(tok_rows, dtype=jnp.int32)
    key_rows = row_start - hop_count * tok_rows + jnp.arange(key_count, dtype=jnp.int32)
    query_docs = jnp.sum(
        (query_rows[:, None] % seq_len >= doc_ends[None, :]).astype(jnp.int32), axis=1
    )
    key_docs = jnp.sum((key_rows[:, None] % seq_len >= doc_ends[None, :]).astype(jnp.int32), axis=1)
    distance = query_rows[None, :] - key_rows[:, None]
    allowed = (
        (query_rows[None, :] // seq_len == key_rows[:, None] // seq_len)
        & (query_docs[None, :] == key_docs[:, None])
        & (distance >= 0)
        & (distance < WINDOW)
    )
    bias = jnp.where(allowed, 0.0, masked_score).astype(F32)
    expert_ids = jnp.arange(experts_total, dtype=jnp.int32)
    side = 128
    layer_columns = qkv_width + width

    def dense_piece():
        rows = w_qkv.shape[1]
        parts = []
        for layer_no in range(LAYERS):
            parts += [w_qkv[layer_no].astype(BF16), w_out[layer_no].astype(BF16)]
        for layer_no in range(LAYERS):
            parts += [router[layer_no].astype(BF16), gains[layer_no].T.astype(BF16)]
        filled = LAYERS * (layer_columns + experts_total + 2)
        parts.append(jnp.zeros((rows, -filled % (128 * owners)), BF16))
        return jnp.concatenate(parts, 1)

    def expert_piece(layer_no):
        return jnp.concatenate(
            [w_in[layer_no].astype(BF16), w_down[layer_no].astype(BF16)], 1
        )

    expert_full = []
    for layer_no in range(LAYERS):
        expert_full.append(
            lax.all_gather(expert_piece(layer_no), "shard", axis=0, tiled=False)
        )
    dense = gather_dense(dense_piece(), shards, owners).reshape(width, -1)

    kept_layers = []
    stream = hidden_in
    for layer_no in range(LAYERS):
        at = layer_no * layer_columns
        w_qkv_full = dense[:, at : at + qkv_width]
        w_out_full = dense[:, at + qkv_width : at + layer_columns]
        at = LAYERS * layer_columns + layer_no * (experts_total + 2)
        small = dense[:, at : at + experts_total + 2]
        router_full = small[:, :experts_total]
        gain_pair = small[:, experts_total : experts_total + 2].astype(F32).T
        normed_one = rms_scale(stream, gain_pair[0]).astype(BF16)
        qkv_rows = jnp.dot(normed_one, w_qkv_full, preferred_element_type=F32).astype(BF16)
        ext = halo(qkv_rows[:, q_width:], shards, hop_count + 1).reshape(key_count, 2 * kv_width)
        attended, log_total = attend(qkv_rows, ext, bias)
        mixed = stream + jnp.dot(attended, w_out_full, preferred_element_type=F32)
        normed_two = rms_scale(mixed, gain_pair[1]).astype(BF16)
        logits = jnp.dot(normed_two, router_full, preferred_element_type=F32)
        named = jnp.any(routes[layer_no][:, :, None] == expert_ids[None, None, :], axis=1)
        top_logit = jnp.max(jnp.where(named, logits, -jnp.inf), axis=1, keepdims=True)
        powers = jnp.where(named, jnp.exp(jnp.where(named, logits - top_logit, 0.0)), 0.0)
        weights = powers / jnp.sum(powers, axis=1, keepdims=True)
        high = weights.astype(BF16)
        low = (weights - high.astype(F32)).astype(BF16)
        wide_rows = jnp.concatenate(
            [normed_two, high, low, jnp.zeros((tok_rows, extra - 2 * experts_total), BF16)], 1
        )
        x_all = spread(wide_rows, owners, 1).reshape(owners * tok_rows, width + extra)
        if layer_no == 0:
            g_rows, x_all = lax.optimization_barrier((cotangent.astype(BF16), x_all))
            g_all = spread(g_rows, owners, 8).reshape(owners * tok_rows, width)
            g_all, x_all = lax.optimization_barrier((g_all, x_all))
        partial, gate_up = ffn_forward(
            first_array, x_all, expert_full[layer_no], experts_total, in_rows
        )
        if layer_no + 1 == LAYERS:
            d_partial, d_experts = ffn_backward(
                first_array, x_all, g_all, gate_up, expert_full[layer_no], experts_total,
                in_rows, False,
            )
            partial, d_partial = lax.optimization_barrier((partial, d_partial))
        moe_out = collect(partial.reshape(owners, tok_rows, width), 2)
        kept_layers.append(
            (
                stream, normed_one, qkv_rows, ext, log_total, attended, mixed,
                x_all, gate_up, normed_two, weights, w_qkv_full, w_out_full, router_full,
                gain_pair,
            )
        )
        stream = mixed + moe_out
    grad_stream = cotangent
    collected = [None] * LAYERS
    dense_parts = [None] * LAYERS
    small_parts = [None] * LAYERS
    for layer_no in reversed(range(LAYERS)):
        (
            layer_input, normed_one, qkv_rows, ext, log_total, attended, mixed,
            x_all, gate_up, normed_two, weights, w_qkv_full, w_out_full, router_full,
            gain_pair,
        ) = kept_layers[layer_no]
        if layer_no + 1 < LAYERS:
            g_all = spread(grad_stream.astype(BF16), owners, 8).reshape(owners * tok_rows, width)
            d_partial, d_experts, d_down_parts = ffn_backward(
                first_array, x_all, g_all, gate_up, expert_full[layer_no], experts_total,
                in_rows, True,
            )
        d_experts = lax.psum_scatter(d_experts, "shard", scatter_dimension=0, tiled=True)[0]
        d_all = collect(d_partial.reshape(owners, tok_rows, -1), 7)
        d_weights = (
            d_all[:, width : width + experts_total]
            + d_all[:, width + experts_total : width + 2 * experts_total]
        )
        mean_d = jnp.sum(weights * d_weights, axis=1, keepdims=True)
        d_logits = (weights * (d_weights - mean_d)).astype(BF16)
        d_router = inner_rows(normed_two, d_logits)
        d_normed_two = d_all[:, :width] + outer_cols(d_logits, router_full)
        _, norm_back = jax.vjp(rms_scale, mixed, gain_pair[1])
        d_mixed_norm, d_gain_two = norm_back(d_normed_two)
        grad_mixed = grad_stream + d_mixed_norm
        d_att = grad_mixed.astype(BF16)
        d_w_out = inner_rows(attended, d_att)
        d_attended = outer_cols(d_att, w_out_full).astype(BF16)
        d_queries, d_kv = attend_back(qkv_rows, ext, bias, d_attended, log_total)
        d_qkv = halo_back(
            d_queries, d_kv.reshape(hop_count + 1, tok_rows, 2 * kv_width), shards
        )
        d_w_qkv = inner_rows(normed_one, d_qkv)
        d_normed_one = outer_cols(d_qkv, w_qkv_full)
        _, norm_back = jax.vjp(rms_scale, layer_input, gain_pair[0])
        d_input_norm, d_gain_one = norm_back(d_normed_one)
        grad_stream = grad_mixed + d_input_norm
        dense_parts[layer_no] = [d_w_qkv.astype(BF16), d_w_out.astype(BF16)]
        small_parts[layer_no] = [
            d_router.astype(BF16),
            jnp.stack([d_gain_one, d_gain_two], 1).astype(BF16),
        ]
        collected[layer_no] = (
            d_experts[:, :in_rows, :].astype(F32),
            d_experts[:, in_rows:, :].astype(F32) if layer_no + 1 == LAYERS else None,
        )
    small = sum(small_parts, [])
    small.append(jnp.zeros((width, side - LAYERS * (experts_total + 2)), BF16))
    parts = sum(dense_parts, []) + [jnp.concatenate(small, 1)]
    d_dense = [part.reshape(shards, width // shards, -1) for part in parts]
    d_dense, d_down = reduce_dense(d_dense, d_down_parts, shards, owners)
    d_dense = d_dense.astype(F32)
    collected[0] = (collected[0][0], d_down.astype(F32))
    for layer_no in range(LAYERS):
        at = layer_no * layer_columns
        d_main = d_dense[:, at : at + layer_columns]
        at = LAYERS * layer_columns + layer_no * (experts_total + 2)
        small = d_dense[:, at : at + experts_total + 2]
        collected[layer_no] = (
            small[:, experts_total:].T,
            d_main[:, :qkv_width],
            d_main[:, qkv_width:],
            small[:, :experts_total],
        ) + collected[layer_no]
    stacked = [
        jnp.stack([collected[layer_no][member] for layer_no in range(LAYERS)], 0)
        for member in range(6)
    ]
    results = [stream, grad_stream]
    results.extend(adam_update(gains, stacked[0], gains_first, gains_second))
    results.extend(adam_update(w_qkv, stacked[1], w_qkv_first, w_qkv_second))
    results.extend(adam_update(w_out, stacked[2], w_out_first, w_out_second))
    results.extend(adam_update(router, stacked[3], router_first, router_second))
    results.extend(adam_update(w_in, stacked[4], w_in_first, w_in_second))
    results.extend(adam_update(w_down, stacked[5], w_down_first, w_down_second))
    return tuple(results)


def solution(mesh):
    return jax.shard_map(
        on_device,
        mesh=mesh,
        in_specs=(
            P(("expert", "shard"), None),
            P(("expert", "shard"), None),
            P(),
            P(None, ("expert", "shard"), None),
            P(None, None, "shard"),
            P(None, None, "shard"),
            P(None, None, "shard"),
            P(None, "shard", None),
            P(None, "shard", None),
            P(None, "shard", None),
            P(None, "shard", None),
            P(None, "shard", None),
            P(None, "shard", None),
            P(None, "shard", None),
            P(None, "shard", None),
            P(None, "shard", None),
            P(None, "expert", "shard", None),
            P(None, "expert", "shard", None),
            P(None, "expert", "shard", None),
            P(None, "expert", "shard", None),
            P(None, "expert", "shard", None),
            P(None, "expert", "shard", None),
        ),
        out_specs=(
            P(("expert", "shard"), None),
            P(("expert", "shard"), None),
            P(None, None, "shard"),
            P(None, None, "shard"),
            P(None, None, "shard"),
            P(None, None, "shard"),
            P(None, "shard", None),
            P(None, "shard", None),
            P(None, "shard", None),
            P(None, "shard", None),
            P(None, "shard", None),
            P(None, "shard", None),
            P(None, "shard", None),
            P(None, "shard", None),
            P(None, "shard", None),
            P(None, "shard", None),
            P(None, "shard", None),
            P(None, "shard", None),
            P(None, "expert", "shard", None),
            P(None, "expert", "shard", None),
            P(None, "expert", "shard", None),
            P(None, "expert", "shard", None),
            P(None, "expert", "shard", None),
            P(None, "expert", "shard", None),
            P(None, "expert", "shard", None),
            P(None, "expert", "shard", None),
        ),
        check_vma=False,
    )
```
